128 devices in a mesh: rep: 1, dp: 128 (over x, y, z, core).
Axes of the slice: x: 4, y: 4, z: 4, core: 2. Of those that a mesh axis runs over, the one named last changes fastest.
Arguments:
- x: bfloat16 [128, 1024, 1024], P(('rep', 'dp'))
- dy: bfloat16 [128, 1024, 1024], P(('rep', 'dp'))
- w_gate: bfloat16 [2, 1024, 3200], replicated
- w_up: bfloat16 [2, 1024, 3200], replicated
- w_down: bfloat16 [2, 3200, 1024], replicated
- m_w_gate: float32 [2, 1024, 3200], P(None, 'dp')
- m_w_up: float32 [2, 1024, 3200], P(None, 'dp')
- m_w_down: float32 [2, 3200, 1024], P(None, 'dp')
- v_w_gate: float32 [2, 1024, 3200], P(None, 'dp')
- v_w_up: float32 [2, 1024, 3200], P(None, 'dp')
- v_w_down: float32 [2, 3200, 1024], P(None, 'dp')
Outputs:
- output 1: bfloat16 [2, 1024, 3200], P('rep')
- output 2: bfloat16 [2, 1024, 3200], P('rep')
- output 3: bfloat16 [2, 3200, 1024], P('rep')
- output 4: float32 [2, 1024, 3200], P('rep', 'dp')
- output 5: float32 [2, 1024, 3200], P('rep', 'dp')
- output 6: float32 [2, 3200, 1024], P('rep', 'dp')
- output 7: float32 [2, 1024, 3200], P('rep', 'dp')
- output 8: float32 [2, 1024, 3200], P('rep', 'dp')
- output 9: float32 [2, 3200, 1024], P('rep', 'dp')
All inputs are finite; a program needn't handle non-finite values.
Results may differ from the reference program's by a relative error of at most 0.022.
Values are sent between devices in bfloat16 or wider.
A program may use at most 1.5 GiB of HBM per device.

```python
import jax
import jax.numpy as jnp
from jax import lax

SEQUENCES = 128
TOKENS = 1024
D = 1024
FF = 3200
LAYERS = 2
NAMES = ("w_gate", "w_up", "w_down")
SHAPES = {"w_gate": (LAYERS, D, FF), "w_up": (LAYERS, D, FF), "w_down": (LAYERS, FF, D)}


def bump(key, n, height):
    away = (jnp.arange(n, dtype=jnp.int32) - jax.random.randint(key, (), 0, n, jnp.int32)) % n
    return jnp.where(away < n // 8, height, 1.0)


def together(key, own, strength):
    shared = jax.random.normal(key, own.shape[1:], jnp.float32)
    return (own + strength * shared) * lax.rsqrt(1 + strength * strength)


def setup_inputs(seed: int = 0, part: int = 0) -> dict:
    kx, kdy, ka, kb, kz, kf, kh, kl, *keys = jax.random.split(jax.random.key(seed), 8 + 3 * len(NAMES))
    kx, kdy, ka, kb = (jax.random.fold_in(k, part) for k in (kx, kdy, ka, kb))
    kw, km, kv = (keys[i::3] for i in range(3))
    shape = (SEQUENCES, TOKENS, D)
    much_x, much_dy = jax.random.uniform(kz, (2,), jnp.float32, 0.0, 1.0)
    loud = 2.0 ** jax.random.uniform(jax.random.fold_in(kz, 1), (), jnp.float32, -1.0, 2.0)
    layers = 2.0 ** jax.random.uniform(kl, (LAYERS, 1, 1), jnp.float32, -1.0, 1.0)
    x = together(ka, jax.random.normal(kx, shape, jnp.float32), much_x) * bump(kf, D, 4.0)
    dy = together(kb, jax.random.normal(kdy, shape, jnp.float32), much_dy)
    drawn = {"x": x.astype(jnp.bfloat16), "dy": (loud * dy * (SEQUENCES * TOKENS) ** -0.5).astype(jnp.bfloat16)}
    for key, name in zip(kw, NAMES, strict=True):
        w = jax.random.normal(key, SHAPES[name], jnp.float32) * SHAPES[name][1] ** -0.5
        drawn[name] = (w * {"w_gate": 1.0, "w_up": bump(kh, FF, 4.0), "w_down": layers}[name]).astype(jnp.bfloat16)
    for key, name in zip(km, NAMES, strict=True):
        drawn[f"m_{name}"] = 0.1 * jax.random.normal(key, SHAPES[name], jnp.float32)
    for key, name in zip(kv, NAMES, strict=True):
        drawn[f"v_{name}"] = loud * loud * jax.random.uniform(key, SHAPES[name], jnp.float32, 0.05, 0.15)
    return drawn


def matmul(a, w):
    return jnp.dot(a, w, preferred_element_type=jnp.float32).astype(jnp.bfloat16)


def normed(h):
    wide = h.astype(jnp.float32)
    scale = lax.rsqrt(jnp.mean(wide**2, -1, keepdims=True) + 1e-6)
    return (wide * scale).astype(jnp.bfloat16)


def layer(h, w):
    a = normed(h)
    gate = jnp.dot(a, w["w_gate"], preferred_element_type=jnp.float32)
    up = jnp.dot(a, w["w_up"], preferred_element_type=jnp.float32)
    return h + matmul((jax.nn.silu(gate) * up).astype(jnp.bfloat16), w["w_down"])


def adamw(w, m, v, g):
    m = 0.9 * m + 0.1 * g
    v = 0.95 * v + 0.05 * g * g
    step = m * lax.rsqrt(v + 1e-8) + 0.1 * w
    return (w - 0.02 * step).astype(jnp.bfloat16), m, v


def stack(weights, h):
    return lax.scan(lambda h, w: (layer(h, w), None), h, weights)[0]


def reference(x, dy, w_gate, w_up, w_down, m_w_gate, m_w_up, m_w_down, v_w_gate, v_w_up, v_w_down):
    weights = dict(zip(NAMES, (w_gate, w_up, w_down), strict=True))

    def take(so_far, sequence):
        h, by_y = sequence
        _, back = jax.vjp(lambda w: stack(w, h), weights)
        return jax.tree.map(lambda total, term: total + term.astype(jnp.float32), so_far, back(by_y)[0]), None

    none_yet = {name: jnp.zeros(w.shape, jnp.float32) for name, w in weights.items()}
    by_weights, _ = lax.scan(take, none_yet, (x, dy))
    gradients = [by_weights[name].astype(jnp.bfloat16).astype(jnp.float32) for name in NAMES]
    new = [
        adamw(w.astype(jnp.float32), m, v, g)
        for w, m, v, g in zip((w_gate, w_up, w_down), (m_w_gate, m_w_up, m_w_down), (v_w_gate, v_w_up, v_w_down), gradients, strict=True)
    ]
    return tuple(one[which] for which in range(3) for one in new)
```

```python
import functools

import jax
import jax.numpy as jnp
from jax import lax
from jax.experimental import pallas as pl
from jax.experimental.pallas import tpu as pltpu
from jax.sharding import PartitionSpec as P

MESH = pl.DeviceIdType.MESH
TWO = 2
BF, F32 = jnp.bfloat16, jnp.float32
LAYERS, D, FF, TOK = 2, 1024, 3200, 1024
LANES, ROWS, OCT = 128, 16, 8
PARTS, CHIPS, HALF = 6, 64, 32
TILE, TILES = 256, 13
TB = 2 * CHIPS
ORDER = ("x1", "y1", "z1", "x0", "y0", "z0")
GROUP, GROUPS, ROWS_GROUP = 8, 16, 200
PAIR = 2 * ROWS_GROUP
UNITS = ROWS_GROUP // ROWS
OWN_ROWS = ROWS_GROUP // GROUP
WIN = 32

G1, D1, D0, G0, NW = 0, 4, 6, 8, 12
SHORT = (0, 3)
NS = 2
OWN_SLOT = (0, 1, 2, 0, 1, 2, 0, 3, 2, 0, 1, 2)
OWN_SLOTS = 4
NRS, NDD, NX = 4, 2, 4

T_F, T_FN, T_L1, T_DOWN1, T_NORM, T_DOWN0, T_B0, T_TAIL = 0, 13, 14, 40, 44, 45, 49, 62
START = (21, 27, 33, 39, 43, 44, 48, 49, 52, 55, 58, 61)
SHORT_START = (50, 45)
OFF = (0, 2, 4, 6, 7, 8, 9, 10, 11, 12)
DX = ((61, 63, 65), (56, 58, 60))
AGS = (33, 39, 45, 51, 60, 61, 65, 66, 64, 67, 70, 73)
SHORT_AGS = (65, 60)
AGO = (0, 2, 4, 6, 8, 10, 13, 16)
TICKS = 90


def div(a, b):
    return a // b if isinstance(a, int) else lax.div(a, jnp.int32(b))


def mod(a, b):
    return a % b if isinstance(a, int) else lax.rem(a, jnp.int32(b))


def base_of(x, y, z):
    r = 0
    for d in ORDER:
        v = {"x": x, "y": y, "z": z}[d[0]]
        r = TWO * r + gray(v, d)
    return r


def gray(v, d):
    h, l = div(v, 2), mod(v, 2)
    return h if d.endswith("1") else h + l - TWO * h * l


CHIP_AT = [None] * CHIPS
for _n in range(CHIPS):
    CHIP_AT[base_of(_n // 16, _n // 4 % 4, _n % 4)] = _n


def rotl(u, p):
    return mod(u * TWO**p, CHIPS) + div(u * TWO**p, CHIPS)


def rotr(u, p):
    return rotl(u, (PARTS - p) % PARTS)


def off_of(i):
    return pl.multiple_of(jnp.maximum(TILE * i - LANES, 0), LANES)


def aligned(start, size, to=None):
    return pl.ds(pl.multiple_of(start, to or size), size)


def dot(a, b, cb=0):
    return lax.dot_general(a, b, (((1,), (cb,)), ((), ())), preferred_element_type=F32)


def pick(w, values):
    r = values[0]
    for q, v in enumerate(values):
        if q:
            r = jnp.where(w == q, v, r)
    return r


def adam(w, m, v, g):
    m = 0.9 * m + 0.1 * g
    v = 0.95 * v + 0.05 * g * g
    step = m * lax.rsqrt(v + 1e-8) + 0.1 * w
    return (w - 0.02 * step).astype(BF).astype(F32), m, v


def rms_scale(squares):
    return lax.rsqrt(squares * (1.0 / D) + 1e-6)


def lanes(q):
    return slice(LANES * q, LANES * q + LANES)


def step_kernel(
    x, dy, w_gate, w_up, w_down, m_g, m_u, m_d, v_g, v_u, v_d,
    ag, agm, hidt, a0t, gu0, om_g, om_u, om_d, ov_g, ov_u, ov_d,
    acts, at, da, wgu, wdb, dgb, dub, hidb, hts, htb, wr_g, wr_u, wr_d,
    own, d2d, acc, r1, r2, r3, r4, r5, r6, s1, s2, s3, s4, s5, s6,
    d2dm, accm, q1, q2, q3, q4, q5, q6, t1, t2, t3, t4, t5, t6,
    gfin, xg, wsend, wrecv, fin, g_d, gx, ws_d, wx,
    lsem, wsem, gsem, hsem, htsem, d2s, d2r, ssem, rsem, xs, xr, wsm, wrm, agl, ags, agr, dags, dagr, dxs, dxr, d2c, rcred,
):
    dp = lax.axis_index("dp")
    c = mod(dp, 2)
    pos = {"x": div(dp, 32), "y": mod(div(dp, 8), 4), "z": mod(div(dp, 2), 4)}
    other = dp + 1 - TWO * c
    j_me = pos["z"] * TWO + c

    def device(x, y, z, core):
        return ((x * 4 + y) * 4 + z) * TWO + core

    def partner(d):
        o = pos[d[0]]
        return device(**(pos | {d[0]: 3 - o if d.endswith("1") else o + 1 - TWO * mod(o, 2)}), core=c)

    bits = [gray(pos[d[0]], d) for d in ORDER]
    partners = [partner(d) for d in ORDER]
    rot = [rotl(base_of(**pos), p) for p in range(PARTS)]

    def group_dev(j):
        return device(pos["x"], pos["y"], div(j, 2), mod(j, 2))

    def rcopy(src, dst, ss, rs, dev):
        return pltpu.make_async_remote_copy(src_ref=src, dst_ref=dst, send_sem=ss, recv_sem=rs, device_id={"dp": dev}, device_id_type=MESH)

    def signal(sem, dev):
        pl.semaphore_signal(sem, inc=1, device_id={"dp": dev}, device_id_type=MESH)

    copy = pltpu.make_async_copy

    barrier = pltpu.get_barrier_semaphore()
    for r in range(1, GROUP):
        signal(barrier, group_dev(mod(j_me + r, GROUP)))
    far = [q for d, q in zip(ORDER, partners) if d[0] != "z"]
    for q in far:
        signal(barrier, q)

    def weights(layer, i, b, gate_up=True):
        o = pl.ds(off_of(i), TILE)
        down = [copy(w_down.at[layer, o], wdb.at[b], wsem.at[b, 2])]
        if not gate_up:
            return down
        return down + [copy(w.at[layer, :, o], wgu.at[TWO * b + k], wsem.at[b, k]) for k, w in enumerate((w_gate, w_up))]

    def saved(i, b):
        return weights(0, i, b, False) + [copy(gu0.at[i], da.at[pl.ds(b * TWO * TB, TWO * TB)], gsem.at[b])]

    def stream(make, i, b):
        for cp in make(i, b):
            cp.wait()

        @pl.when(i + 1 < TILES)
        def _():
            for cp in make(i + 1, 1 - b):
                cp.start()

    def halves(fn):
        def chunk(k, _):
            fn(k, aligned(k * (TOK // TWO), TOK // TWO))
            return 0

        lax.fori_loop(0, 2, chunk, 0)

    def as_blocks(v):
        return v.reshape(v.shape[0] // ROWS, ROWS, LANES)

    def get_da(q, rows, n):
        return da[pl.ds(q * CHIPS + div(rows, ROWS), n // ROWS)].reshape(n, LANES)

    def sigmoid(v):
        return 1.0 / (1.0 + jnp.exp(-v))

    def through_act(gate, up, dhid):
        sg = sigmoid(gate)
        s = gate * sg
        return s, dhid * up * (sg * (1.0 + gate * (1.0 - sg))), dhid * s

    def counts(i):
        return (lax.broadcasted_iota(jnp.int32, (TOK // TWO, TILE), 1) < LANES) | (i > 0)

    def add_products(terms):
        def part(n, _):
            total = sum(dot(a[...], *rhs(n)) for a, rhs in terms)
            for q in range(TWO):
                o = pl.ds((TWO * n + q) * CHIPS, CHIPS)
                da[o] = da[o] + as_blocks(total[:, lanes(q)])
            return 0

        lax.fori_loop(0, D // TILE, part, 0)

    def hid_write(layer, i, b, q):
        o = pl.multiple_of(off_of(i) + LANES * q, LANES)
        return copy(hts.at[b, lanes(q)], hidt.at[layer, pl.ds(o, LANES)], hsem.at[b, q])

    def put_hidden(layer, i, b):
        for q in range(TWO):

            @pl.when(i >= 2 + q)
            def _():
                hid_write(layer, i - 2, b, q).wait()

        hts[b] = hidb[...].T
        for q in range(TWO):

            @pl.when(i >= q)
            def _():
                hid_write(layer, i, b, q).start()

    def hidden_out(layer):
        for i in (TILES - 2, TILES - 1):
            for q in range(TWO):
                hid_write(layer, i, i % TWO, q).wait()

    def gu_out(i, b):
        return copy(acc.at[pl.ds(b * TWO * TB, TWO * TB)], gu0.at[i], gsem.at[b])

    def tick_f(i):
        b = mod(i, 2)
        stream(functools.partial(weights, 0), i, b)

        @pl.when(i >= 2)
        def _():
            gu_out(i - 2, b).wait()

        def chunk(k, rows):
            gate = dot(acts[1, rows], wgu[TWO * b])
            up = dot(acts[1, rows], wgu[TWO * b + 1])
            hidb[rows] = jnp.where(counts(i), gate * sigmoid(gate) * up, 0.0).astype(BF)
            for m, t in enumerate((gate, up)):
                for q in range(TWO):
                    acc[pl.ds((TWO * b + m) * TB + q * CHIPS + k * HALF, HALF)] = as_blocks(t[:, lanes(q)])

        halves(chunk)
        gu_out(i, b).start()
        add_products([(hidb, lambda n: (wdb[b, :, aligned(n * TILE, TILE)],))])
        put_hidden(0, i, b)

    def transpose_in():
        def part(k, _):
            t = acts[1, :, aligned(k * LANES, LANES)].T
            for q in range(OCT):
                n = k * OCT + q
                at[aligned(base_of(div(n, 16), mod(div(n, 4), 4), mod(n, 4)) * ROWS, ROWS)] = t[q * ROWS : (q + 1) * ROWS]
            return 0

        lax.fori_loop(0, D // LANES, part, 0)

    def by_rows(fn):
        def chunk(k, _):
            fn(k * LANES, aligned(k * LANES, LANES))
            return 0

        lax.fori_loop(0, TOK // LANES, chunk, 0)

    def norm_in(_, rows):
        h = acts[2, rows].astype(F32)
        acts[1, rows] = (h * rms_scale(jnp.sum(h * h, -1, keepdims=True))).astype(BF)

    def tick_fn():
        for b in range(TWO):
            gu_out(TILES - 2 + (b + TILES) % TWO, b).wait()

        def chunk(r, rows):
            o = jnp.concatenate([get_da(q, r, LANES) for q in range(OCT)], 1).astype(BF).astype(F32)
            acts[2, rows] = (acts[2, rows].astype(F32) + o).astype(BF)
            for q in range(OCT):
                da[pl.ds(q * CHIPS + div(r, ROWS), OCT)] = jnp.zeros((OCT, ROWS, LANES), F32)
            norm_in(r, rows)

        by_rows(chunk)
        a0t_out.wait()
        transpose_in()
        hidden_out(0)

    def tick_a(i):
        b = mod(i, 2)
        stream(functools.partial(weights, 1), i, b)

        def chunk(_, rows):
            gate = dot(acts[1, rows], wgu[TWO * b])
            up = dot(acts[1, rows], wgu[TWO * b + 1])
            dhid = dot(acts[0, rows], wdb[b], 1).astype(BF).astype(F32)
            s, dgate, dup = through_act(gate, up, dhid)
            hidb[rows] = (s * up).astype(BF)
            dgb[rows] = jnp.where(counts(i), dgate, 0.0).astype(BF)
            dub[rows] = jnp.where(counts(i), dup, 0.0).astype(BF)

        halves(chunk)

    def grads_gate_up(i, slot, layer):
        first = i == 0
        part = slot * PARTS + TWO * mod(i + 2, 3)
        pa = jnp.where(first, OWN_SLOTS * PARTS + TWO * layer, part)
        pb = jnp.where(first, slot * PARTS, part + 1)

        def chunk(k, rows):
            blocks = pl.ds(k * HALF, HALF)
            lhs = at[rows]
            for mat, src in enumerate((dgb, dub)):
                r = dot(lhs, src[...]).astype(BF)
                for q, p in enumerate((pa, pb)):
                    own[mat, p, blocks] = as_blocks(r[:, lanes(q)])

        halves(chunk)

    def wave_in_layer(i):
        return div(jnp.maximum(i - 1, 0), 3)

    def tick_b(i):
        b = mod(i, 2)
        grads_gate_up(i, mod(wave_in_layer(i), 3), 1)
        add_products([(t, lambda n, m=m: (wgu[TWO * b + m, aligned(n * TILE, TILE)], 1)) for m, t in enumerate((dgb, dub))])
        put_hidden(1, i, b)

    def hid_load(layer, r):
        return copy(hidt.at[layer, aligned(PAIR * r, PAIR, ROWS)], htb.at[mod(r, 2)], htsem.at[mod(r, 2)])

    def tick_down(k, layer):
        def iteration(r, _):
            hid_load(layer, r).wait()

            @pl.when(r + 1 < OCT)
            def _():
                hid_load(layer, r + 1).start()

            slots = [jnp.where(layer == 1, OWN_SLOT[D1 + q], OWN_SLOT[D0 + q]) * PARTS for q in range(TWO)]
            res = dot(htb[mod(r, 2)], acts[1 - layer])
            for gg in range(TWO):
                g = TWO * r + gg
                at_xy = base_of(div(g, 4), mod(g, 4), 0)
                for lt in range(OCT):
                    place = at_xy + base_of(0, 0, lt % 4)
                    mine = res[gg * ROWS_GROUP : (gg + 1) * ROWS_GROUP, lanes(lt)]
                    for u in range(UNITS):
                        own[lt // 4, slots[u // PARTS] + u % PARTS, place] = mine[ROWS * u : ROWS * u + ROWS].astype(BF)
                    last = jnp.concatenate([mine[ROWS * UNITS :], jnp.zeros((OCT, LANES), F32)], 0)
                    own[lt // 4, OWN_SLOTS * PARTS + TWO * layer + 1, place] = last.astype(BF)
            return 0

        lax.fori_loop(TWO * k, TWO * k + 2, iteration, 0)

    def tick_norm():
        def chunk(r, rows):
            h = acts[2, rows].astype(F32)
            g = jnp.concatenate([get_da(q, r, LANES) for q in range(OCT)], 1).astype(BF).astype(F32)
            scale = rms_scale(jnp.sum(h * h, -1, keepdims=True))
            back = scale * scale * scale * jnp.sum(h * g, -1, keepdims=True) * (1.0 / D)
            dh = (g * scale - h * back).astype(BF).astype(F32)
            acts[1, rows] = (acts[0, rows].astype(F32) + dh).astype(BF)

        by_rows(chunk)

    def tick_back0(i):
        b = mod(i, 2)
        stream(saved, i, b)

        def chunk(k, rows):
            dhid = dot(acts[1, rows], wdb[b], 1).astype(BF).astype(F32)
            gate, up = (
                jnp.concatenate([get_da(4 * b + TWO * m + q, k * (TOK // TWO), TOK // TWO) for q in range(TWO)], 1) for m in range(TWO)
            )
            _, dgate, dup = through_act(gate, up, dhid)
            dgb[rows] = dgate.astype(BF)
            dub[rows] = dup.astype(BF)

        halves(chunk)
        grads_gate_up(i, pick(wave_in_layer(i), OWN_SLOT[G0:]), 0)

    a0t_out = copy(at, a0t, lsem.at[0])
    a0t_in = copy(a0t, at, lsem.at[0])

    def compute(t):
        def between(lo, hi, fn):
            @pl.when((t >= lo) & (t < hi))
            def _():
                fn(t - lo)

        between(T_F, T_FN, tick_f)

        @pl.when(t == T_FN)
        def _():
            for cp in weights(1, 0, 0):
                cp.start()
            tick_fn()
            loads[1].wait()

        @pl.when((t >= T_L1) & (t < T_DOWN1) & (mod(t, 2) == T_L1 % TWO))
        def _():
            tick_a(div(t - T_L1, 2))

        @pl.when((t >= T_L1) & (t < T_DOWN1) & (mod(t, 2) != T_L1 % TWO))
        def _():
            tick_b(div(t - T_L1, 2))

        @pl.when(t == T_DOWN1 - 1)
        def _():
            hid_load(1, 0).start()
            a0t_in.start()

        @pl.when(t == T_DOWN1)
        def _():
            hidden_out(1)

        @pl.when(((t >= T_DOWN1) & (t < T_NORM)) | ((t >= T_DOWN0) & (t < T_B0)))
        def _():
            layer = jnp.where(t < T_NORM, 1, 0)
            tick_down(t - jnp.where(t < T_NORM, T_DOWN1, T_DOWN0), layer)

        @pl.when(t == T_NORM)
        def _():
            hid_load(0, 0).start()
            tick_norm()
            for cp in saved(0, 0):
                cp.start()
            a0t_in.wait()

        between(T_B0, T_TAIL, tick_back0)

    def L(j):
        return 2 ** (PARTS - j)

    starts = [[div(r, L(j)) * L(j) for j in range(PARTS + 1)] for r in rot]

    def kept(p, j):
        return starts[p][j]

    def lag_start(makers):
        last = None
        for make in makers:
            cp = make()
            if last is not None:
                last.start()
            last = cp
        last.start()

    class Full:
        parts = tuple(range(PARTS))
        accumulated, received, sent, crossed, ag_ref = acc, (None, r1, r2, r3, r4, r5, r6), (None, s1, s2, s3, s4, s5, s6), d2d, ag

        def __init__(self, w):
            self.w, self.id, self.r, self.s, self.f = w, w, mod(w, NRS), mod(w, NDD), mod(w, NX)
            self.own = pick(w, OWN_SLOT) * PARTS

    class Short:
        parts = SHORT
        accumulated, received, sent, crossed, ag_ref = accm, (None, q1, q2, q3, q4, q5, q6), (None, t1, t2, t3, t4, t5, t6), d2dm, agm

        def __init__(self, w):
            self.w, self.id, self.r, self.s, self.f = w, NW + w, w, w, NX + w
            self.own = OWN_SLOTS * PARTS + TWO * w

    def sems(v):
        return (v.r, v.s) if isinstance(v, Full) else (NRS + v.r, NDD + v.s)

    def crossing(v):
        s = sems(v)[1]
        return rcopy(own.at[1 - c, pl.ds(v.own, len(v.parts))], v.crossed.at[v.s], d2s.at[s], d2r.at[s], other)

    def stage_all(v, j):
        s = sems(v)[0]
        return rcopy(v.sent[j].at[v.r], v.received[j].at[v.r], ssem.at[s, j - 1], rsem.at[s, j - 1], other)

    def stage_one(v, j, k):
        s = sems(v)[0]
        to = partners[(v.parts[k] + j - 1) % PARTS]
        return rcopy(v.sent[j].at[v.r, k], v.received[j].at[v.r, k], ssem.at[s, j - 1], rsem.at[s, j - 1], to)

    def acc_at(v, k):
        return (v.r * len(v.parts) + k) * HALF

    def rs0(v):
        if isinstance(v, Full):

            @pl.when(v.w >= NDD)
            def _():
                pl.semaphore_wait(d2c.at[v.s], 1)

        crossing(v).start()

    def rs1(v):
        crossing(v).wait_recv()
        if isinstance(v, Full):

            @pl.when(v.w >= NRS)
            def _():
                pl.semaphore_wait(rcred.at[v.r], len(partners))

        def make(k):
            p = v.parts[k]
            b = bits[p]
            lv, kp = (1 - b) * TWO ** (PARTS - 1 - p), b * TWO ** (PARTS - 1 - p)
            def some(g, _):
                at_g = rotr(g * OCT, p)
                for i in range(OCT):
                    u = at_g + rotr(i, p)
                    both = [own[c, v.own + k, o + u].astype(F32) + v.crossed[v.s, k, o + u].astype(F32) for o in (lv, kp)]
                    v.sent[1][v.r, k, g * OCT + i] = both[0].astype(BF)
                    v.accumulated[acc_at(v, k) + g * OCT + i] = both[1]
                return 0

            lax.fori_loop(0, HALF // OCT, some, 0)
            return stage_one(v, 1, k)

        lag_start([functools.partial(make, k) for k in range(len(v.parts))])
        crossing(v).wait_send()
        if isinstance(v, Full):

            @pl.when(v.w + NDD < NW)
            def _():
                signal(d2c.at[v.s], other)

    def rsj(j, v):
        stage_all(v, j - 1).wait_recv()
        n = L(j)
        ch = min(n, OCT)

        def make(k):
            p = v.parts[k]
            b = bits[(p + j - 1) % PARTS]
            o = acc_at(v, k) + kept(p, j - 1) - kept(p, 1)
            for i in range(0, n, ch):
                lv, kp = (1 - b) * n + i, b * n + i
                both = [v.accumulated[pl.ds(o + h, ch)] + v.received[j - 1][v.r, k, pl.ds(h, ch)].astype(F32) for h in (lv, kp)]
                v.sent[j][v.r, k, pl.ds(i, ch)] = both[0].astype(BF)
                v.accumulated[pl.ds(o + kp, ch)] = both[1]
            return stage_one(v, j, k)

        lag_start([functools.partial(make, k) for k in range(len(v.parts))])

    def is_down(w):
        return (w >= D1) & (w < G0)

    def exchange(v):
        return rcopy(gfin.at[v.f, 1 - c], xg.at[v.id], xs.at[v.f], xr.at[v.id], other)

    def rs7(v):
        stage_all(v, PARTS).wait_recv()
        for k, p in enumerate(v.parts):
            g = v.accumulated[acc_at(v, k) + rot[p] - kept(p, 1)] + v.received[PARTS][v.r, k, 0].astype(F32)
            g = g.astype(BF).astype(F32)
            for h in range(TWO):
                gfin[v.f, h, k] = g[OCT * h : OCT * h + OCT]
        for j in range(1, PARTS + 1):
            stage_all(v, j).wait_send()
        if isinstance(v, Short):
            g_d[v.w, ROWS * UNITS : ROWS * UNITS + OCT] = gfin[v.f, 0, 1]
            exchange(v).start()
            return

        @pl.when(v.w + NRS < NW)
        def _():
            for q in partners:
                signal(rcred.at[v.r], q)

        @pl.when(is_down(v.w))
        def _():
            for p in range(PARTS):
                for h in range(TWO):
                    g_d[jnp.where(v.w < D0, 1, 0), aligned((mod(v.w, 2) * PARTS + p) * ROWS + OCT * h, OCT)] = gfin[v.f, h, p]

        @pl.when(~is_down(v.w))
        def _():
            exchange(v).start()

    def adam_tile(layer, col, v, k):
        cols = aligned(col, LANES)
        mine, theirs = gfin[v.f, c, k], xg[v.id, k]
        for mat, (wr, om, ov) in enumerate(((wr_g, om_g, ov_g), (wr_u, om_u, ov_u))):
            g = jnp.where(c == mat, mine, theirs)
            wn, mn, vn = adam(wr[layer, :, cols].astype(F32), om[layer, :, cols], ov[layer, :, cols], g)
            om[layer, :, cols] = mn
            ov[layer, :, cols] = vn
            wsend[v.f, mat, k] = wn

    def w_exchange(v):
        return rcopy(wsend.at[v.f, 1 - c], wrecv.at[v.id], wsm.at[v.f], wrm.at[v.id], other)

    def unless_down(fn):
        def run(v):
            if isinstance(v, Short):
                fn(v)
            else:

                @pl.when(~is_down(v.w))
                def _():
                    fn(v)

        run.__name__ = fn.__name__
        return run

    @unless_down
    def rs8(v):
        exchange(v).wait_recv()
        if isinstance(v, Short):
            adam_tile(v.w, 0, v, 0)
            for mat in range(TWO):
                for k in range(1, PARTS):
                    wsend[v.f, mat, k] = jnp.zeros((OCT, LANES), F32)
        else:
            layer = jnp.where(v.w < G0, 1, 0)
            for k in range(PARTS):
                adam_tile(layer, LANES + PARTS * LANES * (v.w - jnp.where(v.w < G0, 0, G0)) + LANES * k, v, k)
        exchange(v).wait_send()
        w_exchange(v).start()

    @unless_down
    def rs9(v):
        w_exchange(v).wait_recv()
        for k in range(PARTS if isinstance(v, Full) else 1):
            mine, theirs = wsend[v.f, c, k], wrecv[v.id, k]
            fin[v.id, k] = jnp.concatenate([jnp.where(c == 0, mine, theirs), jnp.where(c == 0, theirs, mine)], 0).astype(BF)
        w_exchange(v).wait_send()

    def window(j):
        return div(OWN_ROWS * j, OCT) * OCT

    def to_group(k, layer, src, dst):
        for r in range(1, GROUP):
            j = mod(j_me + r, GROUP)
            rcopy(src(j), dst.at[layer, j_me], dxs.at[k, layer], dxr.at[k, layer], group_dev(j)).start()

    def from_group(k, layer, dst):
        seven = dst.at[layer, pl.ds(0, GROUP - 1)]
        cp = rcopy(seven, seven, dxs.at[k, layer], dxr.at[k, layer], other)
        cp.wait_recv()
        cp.wait_send()

    def dx1(layer):
        def src(j):
            return g_d.at[layer, aligned(window(j), WIN, OCT)]

        to_group(0, layer, src, gx)
        gx[layer, j_me] = g_d[layer, aligned(window(j_me), WIN, OCT)]

    def dx2(layer):
        from_group(0, layer, gx)
        shift = mod(OWN_ROWS * j_me, OCT)
        row = lax.broadcasted_iota(jnp.int32, (WIN, LANES), 0)
        valid = (row >= shift) & (row < shift + OWN_ROWS)
        def tile(lt, _):
            cols = aligned(lt * LANES, LANES)
            m, s = (pltpu.roll(t[layer, :, cols], shift, 0) for t in (om_d, ov_d))
            wn, mn, vn = adam(wr_d[layer, :, cols].astype(F32), m, s, gx[layer, TWO * mod(lt, 4) + div(lt, 4)])
            for o, t in ((om_d, mn), (ov_d, vn)):
                o[layer, :, cols] = pltpu.roll(t, mod(WIN - shift, WIN), 0)
            ws_d[layer, lt] = jnp.where(valid, wn, 0.0)
            return 0

        lax.fori_loop(0, OCT, tile, 0)

        def src(j):
            return ws_d.at[layer, 4 * mod(j, 2) + div(j, 2)]

        to_group(1, layer, src, wx)
        wx[layer, j_me] = ws_d[layer, 4 * c + pos["z"]]

    def dx3(layer):
        from_group(1, layer, wx)
        octets = [None] * (TWO * UNITS + 2)
        for j in range(GROUP):
            for k in range(WIN // OCT):
                o, t = window(j) // OCT + k, wx[layer, j, OCT * k : OCT * k + OCT]
                octets[o] = t if octets[o] is None else octets[o] + t
        octets[-1] = jnp.zeros((OCT, LANES), F32)
        for u in range(UNITS + 1):
            block = jnp.concatenate(octets[TWO * u : TWO * u + 2], 0).astype(BF)
            if u < UNITS:
                fin[jnp.where(layer == 1, D1, D0) + u // PARTS, u % PARTS] = block
            else:
                fin[NW + layer, 1] = block

    def part_of(v):
        return v.ag_ref.at[v.w, c]

    def ag1(v):
        for k, p in enumerate(v.parts):
            src, dst = fin.at[v.id, k], part_of(v).at[k, rot[p]]
            copy(src, dst, agl.at[v.id]).start()
            rcopy(src, dst, ags.at[v.id], agr.at[v.id, 0], partners[(p + PARTS - 1) % PARTS]).start()
            rcopy(src, dst, dags.at[v.id], dagr.at[v.id], other).start()

    def agk(k, v):
        n = 2 ** (k - 2)
        mine = part_of(v)
        if k == 2:
            copy(fin.at[v.id, pl.ds(0, len(v.parts))], mine.at[:, 0], agl.at[v.id]).wait()
        came = mine.at[:, pl.ds(0, n)]
        rcopy(came, came, ags.at[v.id], agr.at[v.id, k - 2], other).wait_recv()
        j = PARTS + 1 - k
        for q, p in enumerate(v.parts):
            if k <= PARTS:
                h = mine.at[q, pl.ds(kept(p, j), TWO * n)]
                rcopy(h, h, ags.at[v.id], agr.at[v.id, k - 1], partners[(p + j - 1) % PARTS]).start()
            g = mine.at[q, pl.ds(kept(p, j) + (1 - bits[(p + j) % PARTS]) * n, n)]
            rcopy(g, g, dags.at[v.id], dagr.at[v.id], other).start()

    def ag_end(v):
        most = part_of(v).at[:, pl.ds(0, CHIPS - 1)]
        rcopy(most, most, ags.at[v.id], agr.at[v.id, 0], other).wait_send()
        cp = rcopy(part_of(v), part_of(v), dags.at[v.id], dagr.at[v.id], other)
        cp.wait_send()
        cp.wait_recv()

    rs_stages = [rs0, rs1] + [functools.partial(rsj, j) for j in range(TWO, PARTS + 1)] + [rs7, rs8, rs9]
    ag_stages = [ag1] + [functools.partial(agk, k) for k in range(TWO, PARTS + 2)] + [ag_end]

    def stage(fn, t, tables):
        for kind, table in zip((Full, Short), tables):
            w = NW
            for q, s in enumerate(table):
                w = jnp.where(t == s, q, w)

            @pl.when(w < NW)
            def _():
                fn(kind(w))

    def moves(t):
        for s in reversed(range(len(OFF))):
            stage(rs_stages[s], t - OFF[s], (START, SHORT_START))
        for q, fn in enumerate((dx1, dx2, dx3)):

            @pl.when((t == DX[0][q]) | (t == DX[1][q]))
            def _():
                fn(jnp.where(t == DX[1][q], 1, 0))

        for s in reversed(range(len(AGO))):
            stage(ag_stages[s], t - AGO[s], (AGS, SHORT_AGS))

    loads = [copy(x, acts.at[2], lsem.at[1]), copy(dy, acts.at[0], lsem.at[2])]
    rows_in = [copy(w.at[:, aligned(dp * OCT, OCT)], o, lsem.at[3 + k]) for k, (w, o) in enumerate(((w_gate, wr_g), (w_up, wr_u)))]
    rows_in.append(copy(w_down.at[:, aligned(div(OWN_ROWS * dp, OCT) * OCT, WIN, OCT)], wr_d, lsem.at[5]))
    moments = ((m_g, om_g), (m_u, om_u), (m_d, om_d), (v_g, ov_g), (v_u, ov_u), (v_d, ov_d))
    rows_in += [copy(m, o, lsem.at[6 + k]) for k, (m, o) in enumerate(moments)]
    for cp in loads + weights(0, 0, 0) + rows_in:
        cp.start()
    for q in range(OCT):
        da[pl.ds(q * CHIPS, CHIPS)] = jnp.zeros((CHIPS, ROWS, LANES), F32)
    loads[0].wait()
    by_rows(norm_in)
    transpose_in()
    a0t_out.start()
    for cp in rows_in:
        cp.wait()
    pl.semaphore_wait(barrier, GROUP - 1 + len(far))

    def tick(t, _):
        compute(t)
        moves(t)
        return 0

    lax.fori_loop(0, TICKS, tick, 0)


def step_call(args):
    B = (ROWS, LANES)
    V, R, S = pltpu.VMEM, pltpu.SemaphoreType.REGULAR, pltpu.SemaphoreType.DMA
    sizes = [TWO**k for k in reversed(range(PARTS))]
    n, ns = NW + NS, len(SHORT)
    own_parts = OWN_SLOTS * PARTS + NS * ns
    E = (PARTS, OCT, LANES)
    scratch = [
        V((3, TOK, D), BF), V((D, TOK), BF), V((4 * TB, *B), F32), V((4, D, TILE), BF), V((TWO, TILE, D), BF),
        *[V((TOK, TILE), BF)] * 3, V((TWO, TILE, TOK), BF), V((TWO, PAIR, TOK), BF), *[V((LAYERS, OCT, FF), BF)] * TWO, V((LAYERS, WIN, D), BF),
        V((TWO, own_parts, CHIPS, *B), BF), V((NDD, PARTS, CHIPS, *B), BF), V((NRS * PARTS * HALF, *B), F32),
        *[V((NRS, PARTS, k, *B), BF) for k in sizes * TWO],
        V((NS, ns, CHIPS, *B), BF), V((NS * ns * HALF, *B), F32),
        *[V((NS, ns, k, *B), BF) for k in sizes * TWO],
        V((NX + NS, TWO, *E), F32), V((n, *E), F32), V((NX + NS, TWO, *E), F32), V((n, *E), F32), V((n, PARTS, *B), BF),
        V((LAYERS, ROWS * (UNITS + 1), LANES), F32), *[V((LAYERS, GROUP, WIN, LANES), F32)] * 3,
        S((12,)), S((TWO, 3)), S((TWO,)), S((TWO, 2)), S((TWO,)), S((NDD + NS,)), S((NDD + NS,)), S((NRS + NS, PARTS)), S((NRS + NS, PARTS)),
        S((NX + NS,)), S((n,)), S((NX + NS,)), S((n,)), S((n,)), S((n,)), S((n, PARTS)), S((n,)), S((n,)), S((TWO, LAYERS)), S((TWO, LAYERS)),
        R((NDD,)), R((NRS,)),
    ]
    hbm, vmem = pl.BlockSpec(memory_space=pl.ANY), pl.BlockSpec(memory_space=pltpu.VMEM)
    out = [((NW, TWO, PARTS, CHIPS, *B), BF), ((NS, 2, ns, CHIPS, *B), BF), ((LAYERS, FF, TOK), BF), ((D, TOK), BF), ((TILES, TWO * TB, *B), F32)]
    out += [(s, F32) for s in ((LAYERS, OCT, FF), (LAYERS, OCT, FF), (LAYERS, WIN, D))] * TWO
    return pl.pallas_call(
        step_kernel,
        out_shape=[jax.ShapeDtypeStruct(*o) for o in out],
        in_specs=[hbm] * 11,
        out_specs=[hbm] * 5 + [vmem] * 6,
        scratch_shapes=scratch,
        compiler_params=pltpu.CompilerParams(collective_id=0, has_side_effects=True, vmem_limit_bytes=67043328),
        name="step",
    )(*args)


def place_kernel(
    ag, agm, om_g, om_u, om_d, ov_g, ov_u, ov_d, gate, up, down, pm_g, pm_u, pm_d, pv_g, pv_u, pv_d, buf, dbuf, mbuf, stage, mstage, dstage,
    isem, dsem, msem, osem, mosem, dosem,
):
    copy = pltpu.make_async_copy
    jobs = G0
    outs = (gate, up)

    def load(k):
        return copy(ag.at[jnp.where(k < D1, k, k + D1)], buf.at[mod(k, 2)], isem.at[mod(k, 2)])

    def stores(k):
        cols = aligned(LANES + PARTS * LANES * (mod(k, 4)), PARTS * LANES, LANES)
        return [copy(stage.at[mod(k, 2), m], o.at[jnp.where(k < D1, 1, 0), :, cols], osem.at[mod(k, 2), m]) for m, o in enumerate(outs)]

    def load_down(layer):
        return copy(ag.at[pl.ds(pick(layer, (D0, D1)), 2)], dbuf.at[layer], dsem.at[layer])

    def store_down(k):
        rows = aligned(mod(k, 4) * TWO * PAIR, TWO * PAIR, ROWS)
        return copy(dstage.at[mod(k, 2)], down.at[jnp.where(k < D1, 1, 0), rows], dosem.at[mod(k, 2)])

    def store_short(layer, m):
        return copy(mstage.at[layer, m], outs[m].at[layer, :, lanes(0)], mosem.at[layer, m])

    mini = copy(agm, mbuf, msem.at[0])
    for cp in (load_down(1), mini, load(0), load_down(0)):
        cp.start()
    for o, t in ((pm_g, om_g), (pm_u, om_u), (pv_g, ov_g), (pv_u, ov_u)):
        o[...] = t[...]
    for o, t in ((pm_d, om_d), (pv_d, ov_d)):
        o[...] = t[:, :OWN_ROWS]
    mini.wait()

    def by_chip(dst, cols, src, p):
        for u in range(CHIPS):
            n = CHIP_AT[u]
            dst[ROWS * n : ROWS * n + ROWS, cols] = src[rotl(u, p)]

    for layer in range(LAYERS):
        for m in range(TWO):
            by_chip(mstage.at[layer, m], lanes(0), mbuf.at[layer, m, 0], SHORT[0])
            store_short(layer, m).start()

    def body(k, _):
        layer = jnp.where(k < D1, 1, 0)

        @pl.when(mod(k, 4) == 0)
        def _():
            load_down(layer).wait()

        load(k).wait()

        @pl.when(k + 1 < jobs)
        def _():
            load(k + 1).start()

        @pl.when(k >= 2)
        def _():
            for cp in stores(k - 2) + [store_down(k - 2)]:
                cp.wait()

        for m in range(TWO):
            for p in range(PARTS):
                by_chip(stage.at[mod(k, 2), m], lanes(p), buf.at[mod(k, 2), m, p], p)
        for cp in stores(k):
            cp.start()

        def pair(q, _):
            for lt in range(OCT):
                h = lt // 4
                octets = []
                for gg in range(TWO):
                    g = (mod(k, 4) * TWO + q) * TWO + gg
                    spot = base_of(div(g, 4), mod(g, 4), 0) + base_of(0, 0, lt % 4)
                    for u in range(UNITS + 1):
                        if u < UNITS:
                            t = dbuf[layer, u // PARTS, h, u % PARTS, rotl(spot, u % PARTS)].astype(F32)
                        else:
                            t = mbuf[layer, h, 1, rotl(spot, SHORT[1])].astype(F32)[:OCT]
                        octets.append(t)
                dstage[mod(k, 2), aligned(PAIR * q, PAIR, ROWS), lanes(lt)] = jnp.concatenate(octets, 0).astype(BF)
            return 0

        lax.fori_loop(0, 2, pair, 0)
        store_down(k).start()
        return 0

    lax.fori_loop(0, jobs, body, 0)
    for k in (jobs - 2, jobs - 1):
        for cp in stores(k) + [store_down(k)]:
            cp.wait()
    for layer in range(LAYERS):
        for m in range(TWO):
            store_short(layer, m).wait()


def place_call(args):
    hbm, vmem = pl.BlockSpec(memory_space=pl.ANY), pl.BlockSpec(memory_space=pltpu.VMEM)
    V, S = pltpu.VMEM, pltpu.SemaphoreType.DMA
    whole = (TWO, PARTS, CHIPS, ROWS, LANES)
    out = [(s, BF) for s in ((LAYERS, D, FF), (LAYERS, D, FF), (LAYERS, FF, D))]
    out += [(s, F32) for s in ((LAYERS, OCT, FF), (LAYERS, OCT, FF), (LAYERS, OWN_ROWS, D))] * TWO
    return pl.pallas_call(
        place_kernel,
        out_shape=[jax.ShapeDtypeStruct(*o) for o in out],
        in_specs=[hbm] * TWO + [vmem] * 6,
        out_specs=[hbm] * 3 + [vmem] * 6,
        scratch_shapes=[
            V((TWO, *whole), BF), V((LAYERS, TWO, *whole), BF), V((NS, 2, len(SHORT), CHIPS, ROWS, LANES), BF),
            V((TWO, TWO, D, PARTS * LANES), BF), V((LAYERS, TWO, D, LANES), BF), V((TWO, TWO * PAIR, D), BF),
            S((TWO,)), S((TWO,)), S((1,)), S((TWO, 2)), S((TWO, 2)), S((TWO,)),
        ],
        compiler_params=pltpu.CompilerParams(vmem_limit_bytes=60 * TWO**20),
        name="place",
    )(*args)


def local_step(x, dy, w_gate, w_up, w_down, m_g, m_u, m_d, v_g, v_u, v_d):
    m_d, v_d = (jnp.pad(t, ((0, 0), (0, WIN - OWN_ROWS), (0, 0))) for t in (m_d, v_d))
    ag, agm, _, _, _, *moments = step_call((x[0], dy[0], w_gate, w_up, w_down, m_g, m_u, m_d, v_g, v_u, v_d))
    return tuple(place_call((ag, agm, *moments)))


def solution(mesh):
    moment = P(None, "dp", None)
    return jax.shard_map(
        local_step,
        mesh=mesh,
        in_specs=(P(("rep", "dp")), P(("rep", "dp")), P(), P(), P(), *[moment] * 6),
        out_specs=(P("rep"), P("rep"), P("rep"), *[P("rep", "dp", None)] * 6),
        check_vma=False,
    )
```

```python
import functools

import jax
import jax.numpy as jnp
from jax import lax
from jax.experimental import pallas as pl
from jax.experimental.pallas import tpu as pltpu
from jax.sharding import PartitionSpec as P

MESH = pl.DeviceIdType.MESH
TWO = 2
BF, F32 = jnp.bfloat16, jnp.float32
LAYERS, D, FF, TOK = 2, 1024, 3200, 1024
LANES, ROWS, OCT = 128, 16, 8
PARTS, CHIPS, HALF = 6, 64, 32
TILE, TILES = 256, 13
TB = 2 * CHIPS
ORDER = ("x1", "y1", "z1", "x0", "y0", "z0")
GROUP, GROUPS, ROWS_GROUP = 8, 16, 200
PAIR = 2 * ROWS_GROUP
UNITS = ROWS_GROUP // ROWS
OWN_ROWS = ROWS_GROUP // GROUP
WIN = 32

G1, D1, D0, G0, NW = 0, 4, 6, 8, 12
SHORT = (0, 3)
NS = 2
OWN_SLOT = (0, 1, 2, 0, 1, 2, 0, 3, 2, 0, 1, 2)
OWN_SLOTS = 4
NRS, NDD, NX = 3, 2, 4

T_F, T_FN, T_L1, T_DOWN1, T_NORM, T_DOWN0, T_B0, T_TAIL = 0, 13, 14, 40, 44, 45, 49, 62
START = (21, 27, 33, 39, 43, 45, 49, 51, 53, 57, 59, 61)
SHORT_START = (50, 45)
OFF = (0, 2, 4, 6, 7, 8, 9, 10, 11, 12)
DX = ((62, 64, 66), (56, 58, 60))
AGS = (33, 39, 45, 51, 61, 63, 67, 69, 65, 71, 73, 75)
SHORT_AGS = (67, 61)
AGO = (0, 2, 4, 6, 8, 10, 13, 16)
TICKS = 92


def div(a, b):
    return a // b if isinstance(a, int) else lax.div(a, jnp.int32(b))


def mod(a, b):
    return a % b if isinstance(a, int) else lax.rem(a, jnp.int32(b))


def loop(n, fn):
    lax.fori_loop(0, n, fn, 0)


def base_of(x, y, z):
    r = 0
    for d in ORDER:
        v = {"x": x, "y": y, "z": z}[d[0]]
        r = TWO * r + gray(v, d)
    return r


def gray(v, d):
    h, l = div(v, 2), mod(v, 2)
    return h if d.endswith("1") else h + l - TWO * h * l


CHIP_AT = [None] * CHIPS
for _n in range(CHIPS):
    CHIP_AT[base_of(_n // 16, _n // 4 % 4, _n % 4)] = _n


def rotl(u, p):
    return mod(u * TWO**p, CHIPS) + div(u * TWO**p, CHIPS)


def rotr(u, p):
    return rotl(u, (PARTS - p) % PARTS)


def off_of(i):
    return pl.multiple_of(jnp.maximum(TILE * i - LANES, 0), LANES)


def aligned(start, size, to=None):
    return pl.ds(pl.multiple_of(start, to or size), size)


def dot(a, b, cb=0):
    return lax.dot_general(a, b, (((1,), (cb,)), ((), ())), preferred_element_type=F32)


def pick(w, values):
    r = values[0]
    for q, v in enumerate(values):
        if q:
            r = jnp.where(w == q, v, r)
    return r


def adam(w, m, v, g):
    m = 0.9 * m + 0.1 * g
    v = 0.95 * v + 0.05 * g * g
    step = m * lax.rsqrt(v + 1e-8) + 0.1 * w
    return (w - 0.02 * step).astype(BF).astype(F32), m, v


def rms_scale(squares):
    return lax.rsqrt(squares * (1.0 / D) + 1e-6)


def lanes(q):
    return slice(LANES * q, LANES * q + LANES)


def step_kernel(
    x, dy, w_gate, w_up, w_down, m_g, m_u, m_d, v_g, v_u, v_d,
    ag, agm, hidt, a0t, gu0, om_g, om_u, om_d, ov_g, ov_u, ov_d,
    acts, at, da, wgu, wdb, dgu, hidb, hts, htb, wr_g, wr_u, wr_d, md, vd,
    own, d2d, acc, r1, r2, r3, r4, r5, r6, s1, s2, s3, s4, s5, s6,
    d2dm, accm, q1, q2, q3, q4, q5, q6, t1, t2, t3, t4, t5, t6,
    gfin, xg, wsend, wrecv, fin, g_d, gx, ws_d, wx,
    lsem, wsem, gsem, hsem, htsem, d2s, d2r, ssem, rsem, xs, xr, wsm, wrm, agl, ags, agr, dags, dagr, dxs, dxr, d2c, rcred,
):
    dp = lax.axis_index("dp")
    c = mod(dp, 2)
    pos = {"x": div(dp, 32), "y": mod(div(dp, 8), 4), "z": mod(div(dp, 2), 4)}
    other = dp + 1 - TWO * c
    j_me = pos["z"] * TWO + c

    def device(x, y, z, core):
        return ((x * 4 + y) * 4 + z) * TWO + core

    def partner(d):
        o = pos[d[0]]
        return device(**(pos | {d[0]: 3 - o if d.endswith("1") else o + 1 - TWO * mod(o, 2)}), core=c)

    bits = [gray(pos[d[0]], d) for d in ORDER]
    partners = [partner(d) for d in ORDER]
    rot = [rotl(base_of(**pos), p) for p in range(PARTS)]

    def group_dev(j):
        return device(pos["x"], pos["y"], div(j, 2), mod(j, 2))

    def rcopy(src, dst, ss, rs, dev):
        return pltpu.make_async_remote_copy(src_ref=src, dst_ref=dst, send_sem=ss, recv_sem=rs, device_id={"dp": dev}, device_id_type=MESH)

    def signal(sem, dev):
        pl.semaphore_signal(sem, inc=1, device_id={"dp": dev}, device_id_type=MESH)

    copy = pltpu.make_async_copy

    barrier = pltpu.get_barrier_semaphore()
    for r in range(1, GROUP):
        signal(barrier, group_dev(mod(j_me + r, GROUP)))
    far = [q for d, q in zip(ORDER, partners) if d[0] != "z"]
    for q in far:
        signal(barrier, q)

    def weights(layer, i, b, gate_up=True):
        o = pl.ds(off_of(i), TILE)
        down = [copy(w_down.at[layer, o], wdb.at[b], wsem.at[b, 2])]
        if not gate_up:
            return down
        return down + [copy(w.at[layer, :, o], wgu.at[b, :, pl.ds(TILE * k, TILE)], wsem.at[b, k]) for k, w in enumerate((w_gate, w_up))]

    def saved(i, b):
        return weights(0, i, b, False) + [copy(gu0.at[i], da.at[pl.ds(b * TWO * TB, TWO * TB)], gsem.at[b])]

    def stream(make, i, b):
        for cp in make(i, b):
            cp.wait()

        @pl.when(i + 1 < TILES)
        def _():
            for cp in make(i + 1, 1 - b):
                cp.start()

    def as_blocks(v):
        return v.reshape(v.shape[0] // ROWS, ROWS, LANES)

    def get_da(q, rows, n):
        at_row = rows // ROWS if isinstance(rows, int) else div(rows, ROWS)
        return da[pl.ds(q * CHIPS + at_row, n // ROWS)].reshape(n, LANES)

    def sigmoid(v):
        return 1.0 / (1.0 + jnp.exp(-v))

    def through_act(gate, up, dhid):
        sg = sigmoid(gate)
        s = gate * sg
        return s, dhid * up * (sg * (1.0 + gate * (1.0 - sg))), dhid * s

    def counts(i):
        return (lax.broadcasted_iota(jnp.int32, (TOK, TILE), 1) < LANES) | (i > 0)

    def add_product(t):
        for q in range(OCT):
            o = pl.ds(q * CHIPS, CHIPS)
            da[o] = da[o] + as_blocks(t[:, lanes(q)])

    def hid_write(layer, i, b, q):
        o = pl.multiple_of(off_of(i) + LANES * q, LANES)
        return copy(hts.at[b, lanes(q)], hidt.at[layer, pl.ds(o, LANES)], hsem.at[b, q])

    def put_hidden(layer, i, b):
        for q in range(TWO):

            @pl.when(i >= 2 + q)
            def _():
                hid_write(layer, i - 2, b, q).wait()

        hts[b] = hidb[...].T
        for q in range(TWO):

            @pl.when(i >= q)
            def _():
                hid_write(layer, i, b, q).start()

    def hidden_out(layer):
        for i in (TILES - 2, TILES - 1):
            for q in range(TWO):
                hid_write(layer, i, i % TWO, q).wait()

    def gu_out(i, b):
        return copy(acc.at[pl.ds(b * TWO * TB, TWO * TB)], gu0.at[i], gsem.at[b])

    def tick_f(i):
        b = mod(i, 2)
        stream(functools.partial(weights, 0), i, b)

        @pl.when(i >= 2)
        def _():
            gu_out(i - 2, b).wait()

        gu = dot(acts[1], wgu[b])
        gate, up = gu[:, :TILE], gu[:, TILE:]
        hidb[...] = jnp.where(counts(i), gate * sigmoid(gate) * up, 0.0).astype(BF)
        for q in range(4):
            acc[pl.ds(TWO * b * TB + q * CHIPS, CHIPS)] = as_blocks(gu[:, lanes(q)])
        gu_out(i, b).start()
        add_product(dot(hidb[...], wdb[b]))
        put_hidden(0, i, b)

    def transpose_in():
        def part(k, _):
            t = acts[1, :, aligned(k * LANES, LANES)].T
            for q in range(OCT):
                n = k * OCT + q
                at[aligned(base_of(div(n, 16), mod(div(n, 4), 4), mod(n, 4)) * ROWS, ROWS)] = t[q * ROWS : (q + 1) * ROWS]
            return 0

        loop(D // LANES, part)

    def by_rows(fn):
        def chunk(k, _):
            fn(k * LANES, aligned(k * LANES, LANES))
            return 0

        loop(TOK // LANES, chunk)

    def norm_in(_, rows):
        h = acts[2, rows].astype(F32)
        acts[1, rows] = (h * rms_scale(jnp.sum(h * h, -1, keepdims=True))).astype(BF)

    def tick_fn():
        for b in range(TWO):
            gu_out(TILES - 2 + (b + TILES) % TWO, b).wait()

        def chunk(r, rows):
            o = jnp.concatenate([get_da(q, r, LANES) for q in range(OCT)], 1).astype(BF).astype(F32)
            acts[2, rows] = (acts[2, rows].astype(F32) + o).astype(BF)
            for q in range(OCT):
                da[pl.ds(q * CHIPS + div(r, ROWS), OCT)] = jnp.zeros((OCT, ROWS, LANES), F32)
            norm_in(r, rows)

        by_rows(chunk)
        a0t_out.wait()
        transpose_in()
        hidden_out(0)

    def tick_a(i):
        b = mod(i, 2)
        stream(functools.partial(weights, 1), i, b)

        gu = dot(acts[1], wgu[b])
        gate, up = gu[:, :TILE], gu[:, TILE:]
        dhid = dot(acts[0], wdb[b], 1).astype(BF).astype(F32)
        s, dgate, dup = through_act(gate, up, dhid)
        hidb[...] = (s * up).astype(BF)
        dgu[:, :TILE] = jnp.where(counts(i), dgate, 0.0).astype(BF)
        dgu[:, TILE:] = jnp.where(counts(i), dup, 0.0).astype(BF)

    def grads_gate_up(i, slot, layer):
        first = i == 0
        part = slot * PARTS + TWO * mod(i + 2, 3)
        pa = jnp.where(first, OWN_SLOTS * PARTS + TWO * layer, part)
        pb = jnp.where(first, slot * PARTS, part + 1)
        r = dot(at[...], dgu[...]).astype(BF)
        for q in range(4):
            own[q // TWO, pb if q % TWO else pa] = as_blocks(r[:, lanes(q)])

    def wave_in_layer(i):
        return div(jnp.maximum(i - 1, 0), 3)

    def tick_b(i):
        b = mod(i, 2)
        grads_gate_up(i, mod(wave_in_layer(i), 3), 1)
        add_product(dot(dgu[...], wgu[b], 1))
        put_hidden(1, i, b)

    def hid_load(layer, r):
        return copy(hidt.at[layer, aligned(PAIR * r, PAIR, ROWS)], htb.at[mod(r, 2)], htsem.at[mod(r, 2)])

    def tick_down(k, layer):
        def iteration(r, _):
            hid_load(layer, r).wait()

            @pl.when(r + 1 < OCT)
            def _():
                hid_load(layer, r + 1).start()

            slots = [jnp.where(layer == 1, OWN_SLOT[D1 + q], OWN_SLOT[D0 + q]) * PARTS for q in range(TWO)]
            res = dot(htb[mod(r, 2)], acts[1 - layer])
            for gg in range(TWO):
                g = TWO * r + gg
                at_xy = base_of(div(g, 4), mod(g, 4), 0)
                for lt in range(OCT):
                    place = at_xy + base_of(0, 0, lt % 4)
                    mine = res[gg * ROWS_GROUP : (gg + 1) * ROWS_GROUP, lanes(lt)]
                    for u in range(UNITS):
                        own[lt // 4, slots[u // PARTS] + u % PARTS, place] = mine[ROWS * u : ROWS * u + ROWS].astype(BF)
                    last = jnp.concatenate([mine[ROWS * UNITS :], jnp.zeros((OCT, LANES), F32)], 0)
                    own[lt // 4, OWN_SLOTS * PARTS + TWO * layer + 1, place] = last.astype(BF)
            return 0

        lax.fori_loop(TWO * k, TWO * k + 2, iteration, 0)

    def tick_norm():
        def chunk(r, rows):
            h = acts[2, rows].astype(F32)
            g = jnp.concatenate([get_da(q, r, LANES) for q in range(OCT)], 1).astype(BF).astype(F32)
            scale = rms_scale(jnp.sum(h * h, -1, keepdims=True))
            back = scale * scale * scale * jnp.sum(h * g, -1, keepdims=True) * (1.0 / D)
            dh = (g * scale - h * back).astype(BF).astype(F32)
            acts[1, rows] = (acts[0, rows].astype(F32) + dh).astype(BF)

        by_rows(chunk)

    def tick_back0(i):
        b = mod(i, 2)
        stream(saved, i, b)

        dhid = dot(acts[1], wdb[b], 1).astype(BF).astype(F32)
        gate, up = (jnp.concatenate([get_da(4 * b + TWO * m + q, 0, TOK) for q in range(TWO)], 1) for m in range(TWO))
        _, dgate, dup = through_act(gate, up, dhid)
        dgu[:, :TILE] = dgate.astype(BF)
        dgu[:, TILE:] = dup.astype(BF)
        grads_gate_up(i, pick(wave_in_layer(i), OWN_SLOT[G0:]), 0)

    a0t_out = copy(at, a0t, lsem.at[0])
    a0t_in = copy(a0t, at, lsem.at[0])

    def compute(t):
        def between(lo, hi, fn):
            @pl.when((t >= lo) & (t < hi))
            def _():
                fn(t - lo)

        between(T_F, T_FN, tick_f)

        @pl.when(t == T_FN)
        def _():
            for cp in weights(1, 0, 0):
                cp.start()
            tick_fn()
            loads[1].wait()

        @pl.when((t >= T_L1) & (t < T_DOWN1) & (mod(t, 2) == T_L1 % TWO))
        def _():
            tick_a(div(t - T_L1, 2))

        @pl.when((t >= T_L1) & (t < T_DOWN1) & (mod(t, 2) != T_L1 % TWO))
        def _():
            tick_b(div(t - T_L1, 2))

        @pl.when(t == T_DOWN1 - 1)
        def _():
            hid_load(1, 0).start()
            a0t_in.start()

        @pl.when(t == T_DOWN1)
        def _():
            hidden_out(1)

        @pl.when(((t >= T_DOWN1) & (t < T_NORM)) | ((t >= T_DOWN0) & (t < T_B0)))
        def _():
            layer = jnp.where(t < T_NORM, 1, 0)
            tick_down(t - jnp.where(t < T_NORM, T_DOWN1, T_DOWN0), layer)

        @pl.when(t == T_NORM)
        def _():
            hid_load(0, 0).start()
            tick_norm()
            for cp in saved(0, 0):
                cp.start()
            a0t_in.wait()

        between(T_B0, T_TAIL, tick_back0)

    def L(j):
        return 2 ** (PARTS - j)

    starts = [[div(r, L(j)) * L(j) for j in range(PARTS + 1)] for r in rot]

    def kept(p, j):
        return starts[p][j]

    def lag_start(makers):
        last = None
        for make in makers:
            cp = make()
            if last is not None:
                last.start()
            last = cp
        last.start()

    class Full:
        parts = tuple(range(PARTS))
        accumulated, received, sent, crossed, ag_ref = acc, (None, r1, r2, r3, r4, r5, r6), (None, s1, s2, s3, s4, s5, s6), d2d, ag

        def __init__(self, w):
            self.w, self.id, self.r, self.s, self.f = w, w, mod(w, NRS), mod(w, NDD), mod(w, NX)
            self.own = pick(w, OWN_SLOT) * PARTS

    class Short:
        parts = SHORT
        accumulated, received, sent, crossed, ag_ref = accm, (None, q1, q2, q3, q4, q5, q6), (None, t1, t2, t3, t4, t5, t6), d2dm, agm

        def __init__(self, w):
            self.w, self.id, self.r, self.s, self.f = w, NW + w, w, w, NX + w
            self.own = OWN_SLOTS * PARTS + TWO * w

    def sems(v):
        return (v.r, v.s) if isinstance(v, Full) else (NRS + v.r, NDD + v.s)

    def crossing(v):
        s = sems(v)[1]
        return rcopy(own.at[1 - c, pl.ds(v.own, len(v.parts))], v.crossed.at[v.s], d2s.at[s], d2r.at[s], other)

    def stage_all(v, j):
        s = sems(v)[0]
        return rcopy(v.sent[j].at[v.r], v.received[j].at[v.r], ssem.at[s, j - 1], rsem.at[s, j - 1], other)

    def stage_one(v, j, k):
        s = sems(v)[0]
        to = partners[(v.parts[k] + j - 1) % PARTS]
        return rcopy(v.sent[j].at[v.r, k], v.received[j].at[v.r, k], ssem.at[s, j - 1], rsem.at[s, j - 1], to)

    def acc_at(v, k):
        return (v.r * len(v.parts) + k) * HALF

    def rs0(v):
        if isinstance(v, Full):

            @pl.when(v.w >= NDD)
            def _():
                pl.semaphore_wait(d2c.at[v.s], 1)

        crossing(v).start()

    def rs1(v):
        crossing(v).wait_recv()
        if isinstance(v, Full):

            @pl.when(v.w >= NRS)
            def _():
                pl.semaphore_wait(rcred.at[v.r], len(partners))

        def make(k):
            p = v.parts[k]
            b = bits[p]
            lv, kp = (1 - b) * TWO ** (PARTS - 1 - p), b * TWO ** (PARTS - 1 - p)
            def some(g, _):
                at_g = rotr(g * OCT, p)
                for i in range(OCT):
                    u = at_g + rotr(i, p)
                    both = [own[c, v.own + k, o + u].astype(F32) + v.crossed[v.s, k, o + u].astype(F32) for o in (lv, kp)]
                    v.sent[1][v.r, k, g * OCT + i] = both[0].astype(BF)
                    v.accumulated[acc_at(v, k) + g * OCT + i] = both[1]
                return 0

            loop(HALF // OCT, some)
            return stage_one(v, 1, k)

        lag_start([functools.partial(make, k) for k in range(len(v.parts))])
        crossing(v).wait_send()
        if isinstance(v, Full):

            @pl.when(v.w + NDD < NW)
            def _():
                signal(d2c.at[v.s], other)

    def rsj(j, v):
        stage_all(v, j - 1).wait_recv()
        n = L(j)
        ch = min(n, OCT)

        def make(k):
            p = v.parts[k]
            b = bits[(p + j - 1) % PARTS]
            o = acc_at(v, k) + kept(p, j - 1) - kept(p, 1)
            for i in range(0, n, ch):
                lv, kp = (1 - b) * n + i, b * n + i
                both = [v.accumulated[pl.ds(o + h, ch)] + v.received[j - 1][v.r, k, pl.ds(h, ch)].astype(F32) for h in (lv, kp)]
                v.sent[j][v.r, k, pl.ds(i, ch)] = both[0].astype(BF)
                v.accumulated[pl.ds(o + kp, ch)] = both[1]
            return stage_one(v, j, k)

        lag_start([functools.partial(make, k) for k in range(len(v.parts))])

    def is_down(w):
        return (w >= D1) & (w < G0)

    def exchange(v):
        return rcopy(gfin.at[v.f, 1 - c], xg.at[v.id], xs.at[v.f], xr.at[v.id], other)

    def rs7(v):
        stage_all(v, PARTS).wait_recv()
        for k, p in enumerate(v.parts):
            g = v.accumulated[acc_at(v, k) + rot[p] - kept(p, 1)] + v.received[PARTS][v.r, k, 0].astype(F32)
            g = g.astype(BF).astype(F32)
            for h in range(TWO):
                gfin[v.f, h, k] = g[OCT * h : OCT * h + OCT]
        for j in range(1, PARTS + 1):
            stage_all(v, j).wait_send()
        if isinstance(v, Short):
            g_d[v.w, ROWS * UNITS : ROWS * UNITS + OCT] = gfin[v.f, 0, 1]
            exchange(v).start()
            return

        @pl.when(v.w + NRS < NW)
        def _():
            for q in partners:
                signal(rcred.at[v.r], q)

        @pl.when(is_down(v.w))
        def _():
            for p in range(PARTS):
                for h in range(TWO):
                    g_d[jnp.where(v.w < D0, 1, 0), aligned((mod(v.w, 2) * PARTS + p) * ROWS + OCT * h, OCT)] = gfin[v.f, h, p]

        @pl.when(~is_down(v.w))
        def _():
            exchange(v).start()

    def adam_tile(layer, col, v, k):
        cols = aligned(col, LANES)
        mine, theirs = gfin[v.f, c, k], xg[v.id, k]
        for mat, (wr, om, ov) in enumerate(((wr_g, om_g, ov_g), (wr_u, om_u, ov_u))):
            g = jnp.where(c == mat, mine, theirs)
            wn, mn, vn = adam(wr[layer, :, cols].astype(F32), om[layer, :, cols], ov[layer, :, cols], g)
            om[layer, :, cols] = mn
            ov[layer, :, cols] = vn
            wsend[v.f, mat, k] = wn

    def w_exchange(v):
        return rcopy(wsend.at[v.f, 1 - c], wrecv.at[v.id], wsm.at[v.f], wrm.at[v.id], other)

    def unless_down(fn):
        def run(v):
            if isinstance(v, Short):
                fn(v)
            else:

                @pl.when(~is_down(v.w))
                def _():
                    fn(v)

        run.__name__ = fn.__name__
        return run

    @unless_down
    def rs8(v):
        exchange(v).wait_recv()
        if isinstance(v, Short):
            adam_tile(v.w, 0, v, 0)
            for mat in range(TWO):
                for k in range(1, PARTS):
                    wsend[v.f, mat, k] = jnp.zeros((OCT, LANES), F32)
        else:
            layer = jnp.where(v.w < G0, 1, 0)
            for k in range(PARTS):
                adam_tile(layer, LANES + PARTS * LANES * (v.w - jnp.where(v.w < G0, 0, G0)) + LANES * k, v, k)
        exchange(v).wait_send()
        w_exchange(v).start()

    @unless_down
    def rs9(v):
        w_exchange(v).wait_recv()
        for k in range(PARTS if isinstance(v, Full) else 1):
            mine, theirs = wsend[v.f, c, k], wrecv[v.id, k]
            fin[v.id, k] = jnp.concatenate([jnp.where(c == 0, mine, theirs), jnp.where(c == 0, theirs, mine)], 0).astype(BF)
        w_exchange(v).wait_send()

    def window(j):
        return div(OWN_ROWS * j, OCT) * OCT

    def to_group(k, layer, src, dst):
        for r in range(1, GROUP):
            j = mod(j_me + r, GROUP)
            rcopy(src(j), dst.at[layer, j_me], dxs.at[k, layer], dxr.at[k, layer], group_dev(j)).start()

    def from_group(k, layer, dst):
        seven = dst.at[layer, pl.ds(0, GROUP - 1)]
        cp = rcopy(seven, seven, dxs.at[k, layer], dxr.at[k, layer], other)
        cp.wait_recv()
        cp.wait_send()

    def dx1(layer):
        def src(j):
            return g_d.at[layer, aligned(window(j), WIN, OCT)]

        to_group(0, layer, src, gx)

        def row(r, _):
            for o, t in ((om_d, md), (ov_d, vd)):
                o[layer, pl.ds(r, 1)] = t[r, pl.ds(layer, 1)]
            return 0

        loop(OWN_ROWS, row)
        gx[layer, j_me] = g_d[layer, aligned(window(j_me), WIN, OCT)]

    def dx2(layer):
        from_group(0, layer, gx)
        shift = mod(OWN_ROWS * j_me, OCT)
        row = lax.broadcasted_iota(jnp.int32, (WIN, LANES), 0)
        valid = (row >= shift) & (row < shift + OWN_ROWS)
        def tile(lt, _):
            cols = aligned(lt * LANES, LANES)
            m, s = (pltpu.roll(t[layer, :, cols], shift, 0) for t in (om_d, ov_d))
            wn, mn, vn = adam(wr_d[layer, :, cols].astype(F32), m, s, gx[layer, TWO * mod(lt, 4) + div(lt, 4)])
            for o, t in ((om_d, mn), (ov_d, vn)):
                o[layer, :, cols] = pltpu.roll(t, mod(WIN - shift, WIN), 0)
            ws_d[layer, lt] = jnp.where(valid, wn, 0.0)
            return 0

        loop(OCT, tile)

        def src(j):
            return ws_d.at[layer, 4 * mod(j, 2) + div(j, 2)]

        to_group(1, layer, src, wx)
        wx[layer, j_me] = ws_d[layer, 4 * c + pos["z"]]

    def dx3(layer):
        from_group(1, layer, wx)
        octets = [None] * (TWO * UNITS + 2)
        for j in range(GROUP):
            for k in range(WIN // OCT):
                o, t = window(j) // OCT + k, wx[layer, j, OCT * k : OCT * k + OCT]
                octets[o] = t if octets[o] is None else octets[o] + t
        octets[-1] = jnp.zeros((OCT, LANES), F32)
        for u in range(UNITS + 1):
            block = jnp.concatenate(octets[TWO * u : TWO * u + 2], 0).astype(BF)
            if u < UNITS:
                fin[jnp.where(layer == 1, D1, D0) + u // PARTS, u % PARTS] = block
            else:
                fin[NW + layer, 1] = block

    def part_of(v):
        return v.ag_ref.at[v.w, c]

    def ag1(v):
        for k, p in enumerate(v.parts):
            src, dst = fin.at[v.id, k], part_of(v).at[k, rot[p]]
            copy(src, dst, agl.at[v.id]).start()
            rcopy(src, dst, ags.at[v.id], agr.at[v.id, 0], partners[(p + PARTS - 1) % PARTS]).start()
            rcopy(src, dst, dags.at[v.id], dagr.at[v.id], other).start()

    def agk(k, v):
        n = 2 ** (k - 2)
        mine = part_of(v)
        if k == 2:
            copy(fin.at[v.id, pl.ds(0, len(v.parts))], mine.at[:, 0], agl.at[v.id]).wait()
        came = mine.at[:, pl.ds(0, n)]
        rcopy(came, came, ags.at[v.id], agr.at[v.id, k - 2], other).wait_recv()
        j = PARTS + 1 - k
        for q, p in enumerate(v.parts):
            if k <= PARTS:
                h = mine.at[q, pl.ds(kept(p, j), TWO * n)]
                rcopy(h, h, ags.at[v.id], agr.at[v.id, k - 1], partners[(p + j - 1) % PARTS]).start()
            g = mine.at[q, pl.ds(kept(p, j) + (1 - bits[(p + j) % PARTS]) * n, n)]
            rcopy(g, g, dags.at[v.id], dagr.at[v.id], other).start()

    def ag_end(v):
        most = part_of(v).at[:, pl.ds(0, CHIPS - 1)]
        rcopy(most, most, ags.at[v.id], agr.at[v.id, 0], other).wait_send()
        cp = rcopy(part_of(v), part_of(v), dags.at[v.id], dagr.at[v.id], other)
        cp.wait_send()
        cp.wait_recv()

    rs_stages = [rs0, rs1] + [functools.partial(rsj, j) for j in range(TWO, PARTS + 1)] + [rs7, rs8, rs9]
    ag_stages = [ag1] + [functools.partial(agk, k) for k in range(TWO, PARTS + 2)] + [ag_end]

    def find(t, table):
        terms = [jnp.where(t == s, q + 1, 0) for q, s in enumerate(table)]
        while len(terms) > 1:
            terms = [sum(terms[q : q + 2]) for q in range(0, len(terms), 2)]
        return terms[0]

    def run(fns, offs, s, t, kind, table):
        w = find(t - offs[s], table)

        @pl.when(w > 0)
        def _():
            fns[s](kind(w - 1))

    def stages(fns, offs, t, table, short_table):
        @pl.when((t >= min(table)) & (t <= max(table) + offs[-1]))
        def _():
            for odd in range(TWO):

                @pl.when(mod(t, 2) == odd)
                def _():
                    for s in reversed(range(len(offs))):
                        if (offs[s] + 1) % TWO == odd:
                            run(fns, offs, s, t, Full, table)

        @pl.when((t >= min(short_table)) & (t <= max(short_table) + offs[-1]))
        def _():
            for s in reversed(range(len(offs))):
                run(fns, offs, s, t, Short, short_table)

    def moves(t):
        stages(rs_stages, OFF, t, START, SHORT_START)
        for q, fn in enumerate((dx1, dx2, dx3)):

            @pl.when((t == DX[0][q]) | (t == DX[1][q]))
            def _():
                fn(jnp.where(t == DX[1][q], 1, 0))

        stages(ag_stages, AGO, t, AGS, SHORT_AGS)

    loads = [copy(x, acts.at[2], lsem.at[1]), copy(dy, acts.at[0], lsem.at[2])]
    rows_in = [copy(w.at[:, aligned(dp * OCT, OCT)], o, lsem.at[3 + k]) for k, (w, o) in enumerate(((w_gate, wr_g), (w_up, wr_u)))]
    rows_in.append(copy(w_down.at[:, aligned(div(OWN_ROWS * dp, OCT) * OCT, WIN, OCT)], wr_d, lsem.at[5]))
    moments = ((m_g, om_g), (m_u, om_u), (m_d, md), (v_g, ov_g), (v_u, ov_u), (v_d, vd))
    rows_in += [copy(m, o, lsem.at[6 + k]) for k, (m, o) in enumerate(moments)]
    for cp in loads + weights(0, 0, 0) + rows_in:
        cp.start()
    for q in range(OCT):
        da[pl.ds(q * CHIPS, CHIPS)] = jnp.zeros((CHIPS, ROWS, LANES), F32)
    loads[0].wait()
    by_rows(norm_in)
    transpose_in()
    a0t_out.start()
    for cp in rows_in:
        cp.wait()
    pl.semaphore_wait(barrier, GROUP - 1 + len(far))

    def tick(t, _):
        compute(t)
        moves(t)
        return 0

    loop(TICKS, tick)


def step_call(args):
    B = (ROWS, LANES)
    V, R, S = pltpu.VMEM, pltpu.SemaphoreType.REGULAR, pltpu.SemaphoreType.DMA
    sizes = [TWO**k for k in reversed(range(PARTS))]
    n, ns = NW + NS, len(SHORT)
    own_parts = OWN_SLOTS * PARTS + NS * ns
    E = (PARTS, OCT, LANES)
    scratch = [
        V((3, TOK, D), BF), V((D, TOK), BF), V((4 * TB, *B), F32), V((TWO, D, TWO * TILE), BF), V((TWO, TILE, D), BF),
        V((TOK, TWO * TILE), BF), V((TOK, TILE), BF), V((TWO, TILE, TOK), BF), V((TWO, PAIR, TOK), BF),
        *[V((LAYERS, OCT, FF), BF)] * TWO, V((LAYERS, WIN, D), BF), *[V((OWN_ROWS, LAYERS, D), F32)] * TWO,
        V((TWO, own_parts, CHIPS, *B), BF), V((NDD, PARTS, CHIPS, *B), BF), V((NRS * PARTS * HALF, *B), F32),
        *[V((NRS, PARTS, k, *B), BF) for k in sizes * TWO],
        V((NS, ns, CHIPS, *B), BF), V((NS * ns * HALF, *B), F32),
        *[V((NS, ns, k, *B), BF) for k in sizes * TWO],
        V((NX + NS, TWO, *E), F32), V((n, *E), F32), V((NX + NS, TWO, *E), F32), V((n, *E), F32), V((n, PARTS, *B), BF),
        V((LAYERS, ROWS * (UNITS + 1), LANES), F32), *[V((LAYERS, GROUP, WIN, LANES), F32)] * 3,
        S((12,)), S((TWO, 3)), S((TWO,)), S((TWO, 2)), S((TWO,)), S((NDD + NS,)), S((NDD + NS,)), S((NRS + NS, PARTS)), S((NRS + NS, PARTS)),
        S((NX + NS,)), S((n,)), S((NX + NS,)), S((n,)), S((n,)), S((n,)), S((n, PARTS)), S((n,)), S((n,)), S((TWO, LAYERS)), S((TWO, LAYERS)),
        R((NDD,)), R((NRS,)),
    ]
    hbm, vmem = pl.BlockSpec(memory_space=pl.ANY), pl.BlockSpec(memory_space=pltpu.VMEM)
    out = [((NW, TWO, PARTS, CHIPS, *B), BF), ((NS, 2, ns, CHIPS, *B), BF), ((LAYERS, FF, TOK), BF), ((D, TOK), BF), ((TILES, TWO * TB, *B), F32)]
    out += [(s, F32) for s in ((LAYERS, OCT, FF), (LAYERS, OCT, FF), (LAYERS, WIN, D))] * TWO
    return pl.pallas_call(
        step_kernel,
        out_shape=[jax.ShapeDtypeStruct(*o) for o in out],
        in_specs=[hbm] * 11,
        out_specs=[hbm] * 5 + [vmem] * 6,
        scratch_shapes=scratch,
        compiler_params=pltpu.CompilerParams(collective_id=0, has_side_effects=True, vmem_limit_bytes=67043328),
        name="step",
    )(*args)


def place_kernel(
    ag, agm, om_g, om_u, om_d, ov_g, ov_u, ov_d, gate, up, down, pm_g, pm_u, pm_d, pv_g, pv_u, pv_d, buf, dbuf, mbuf, stage, mstage, dstage,
    isem, dsem, msem, osem, mosem, dosem,
):
    copy = pltpu.make_async_copy
    jobs = G0
    outs = (gate, up)

    def load(k):
        return copy(ag.at[jnp.where(k < D1, k, k + D1)], buf.at[mod(k, 2)], isem.at[mod(k, 2)])

    def stores(k):
        cols = aligned(LANES + PARTS * LANES * (mod(k, 4)), PARTS * LANES, LANES)
        return [copy(stage.at[mod(k, 2), m], o.at[jnp.where(k < D1, 1, 0), :, cols], osem.at[mod(k, 2), m]) for m, o in enumerate(outs)]

    def load_down(layer):
        return copy(ag.at[pl.ds(pick(layer, (D0, D1)), 2)], dbuf.at[layer], dsem.at[layer])

    def store_down(k):
        rows = aligned(mod(k, 4) * TWO * PAIR, TWO * PAIR, ROWS)
        return copy(dstage.at[mod(k, 2)], down.at[jnp.where(k < D1, 1, 0), rows], dosem.at[mod(k, 2)])

    def store_short(layer, m):
        return copy(mstage.at[layer, m], outs[m].at[layer, :, lanes(0)], mosem.at[layer, m])

    mini = copy(agm, mbuf, msem.at[0])
    for cp in (load_down(1), mini, load(0), load_down(0)):
        cp.start()
    for o, t in ((pm_g, om_g), (pm_u, om_u), (pv_g, ov_g), (pv_u, ov_u)):
        o[...] = t[...]
    for o, t in ((pm_d, om_d), (pv_d, ov_d)):
        for layer in range(LAYERS):
            for r in range(OWN_ROWS):
                o[r, layer : layer + 1] = t[layer, r : r + 1]
    mini.wait()

    def by_chip(dst, cols, src, p):
        for u in range(CHIPS):
            n = CHIP_AT[u]
            dst[ROWS * n : ROWS * n + ROWS, cols] = src[rotl(u, p)]

    for layer in range(LAYERS):
        for m in range(TWO):
            by_chip(mstage.at[layer, m], lanes(0), mbuf.at[layer, m, 0], SHORT[0])
            store_short(layer, m).start()

    def body(k, _):
        layer = jnp.where(k < D1, 1, 0)

        @pl.when(mod(k, 4) == 0)
        def _():
            load_down(layer).wait()

        load(k).wait()

        @pl.when(k + 1 < jobs)
        def _():
            load(k + 1).start()

        @pl.when(k >= 2)
        def _():
            for cp in stores(k - 2) + [store_down(k - 2)]:
                cp.wait()

        for m in range(TWO):
            for p in range(PARTS):
                by_chip(stage.at[mod(k, 2), m], lanes(p), buf.at[mod(k, 2), m, p], p)
        for cp in stores(k):
            cp.start()

        def pair(q, _):
            for lt in range(OCT):
                h = lt // 4
                octets = []
                for gg in range(TWO):
                    g = (mod(k, 4) * TWO + q) * TWO + gg
                    spot = base_of(div(g, 4), mod(g, 4), 0) + base_of(0, 0, lt % 4)
                    for u in range(UNITS + 1):
                        if u < UNITS:
                            t = dbuf[layer, u // PARTS, h, u % PARTS, rotl(spot, u % PARTS)].astype(F32)
                        else:
                            t = mbuf[layer, h, 1, rotl(spot, SHORT[1])].astype(F32)[:OCT]
                        octets.append(t)
                dstage[mod(k, 2), aligned(PAIR * q, PAIR, ROWS), lanes(lt)] = jnp.concatenate(octets, 0).astype(BF)
            return 0

        loop(2, pair)
        store_down(k).start()
        return 0

    loop(jobs, body)
    for k in (jobs - 2, jobs - 1):
        for cp in stores(k) + [store_down(k)]:
            cp.wait()
    for layer in range(LAYERS):
        for m in range(TWO):
            store_short(layer, m).wait()


def place_call(args):
    hbm, vmem = pl.BlockSpec(memory_space=pl.ANY), pl.BlockSpec(memory_space=pltpu.VMEM)
    V, S = pltpu.VMEM, pltpu.SemaphoreType.DMA
    whole = (TWO, PARTS, CHIPS, ROWS, LANES)
    out = [(s, BF) for s in ((LAYERS, D, FF), (LAYERS, D, FF), (LAYERS, FF, D))]
    out += [(s, F32) for s in ((LAYERS, OCT, FF), (LAYERS, OCT, FF), (OWN_ROWS, LAYERS, D))] * TWO
    return pl.pallas_call(
        place_kernel,
        out_shape=[jax.ShapeDtypeStruct(*o) for o in out],
        in_specs=[hbm] * TWO + [vmem] * 6,
        out_specs=[hbm] * 3 + [vmem] * 6,
        scratch_shapes=[
            V((TWO, *whole), BF), V((LAYERS, TWO, *whole), BF), V((NS, 2, len(SHORT), CHIPS, ROWS, LANES), BF),
            V((TWO, TWO, D, PARTS * LANES), BF), V((LAYERS, TWO, D, LANES), BF), V((TWO, TWO * PAIR, D), BF),
            S((TWO,)), S((TWO,)), S((1,)), S((TWO, 2)), S((TWO, 2)), S((TWO,)),
        ],
        compiler_params=pltpu.CompilerParams(vmem_limit_bytes=60 * TWO**20),
        name="place",
    )(*args)


def local_step(x, dy, w_gate, w_up, w_down, m_g, m_u, m_d, v_g, v_u, v_d):
    m_d, v_d = (jnp.transpose(t, (1, 0, 2)) for t in (m_d, v_d))
    ag, agm, _, _, _, *moments = step_call((x[0], dy[0], w_gate, w_up, w_down, m_g, m_u, m_d, v_g, v_u, v_d))
    gate, up, down, om_g, om_u, om_d, ov_g, ov_u, ov_d = place_call((ag, agm, *moments))
    om_d, ov_d = (jnp.transpose(t, (1, 0, 2)) for t in (om_d, ov_d))
    return gate, up, down, om_g, om_u, om_d, ov_g, ov_u, ov_d


def solution(mesh):
    moment = P(None, "dp", None)
    return jax.shard_map(
        local_step,
        mesh=mesh,
        in_specs=(P(("rep", "dp")), P(("rep", "dp")), P(), P(), P(), *[moment] * 6),
        out_specs=(P("rep"), P("rep"), P("rep"), *[P("rep", "dp", None)] * 6),
        check_vma=False,
    )
```

```python
import functools
from itertools import accumulate

import jax
import jax.numpy as jnp
from jax import lax
from jax.experimental import pallas as pl
from jax.experimental.pallas import tpu as pltpu
from jax.sharding import PartitionSpec as P

MESH = pl.DeviceIdType.MESH
ONE, TWO = 1, 2
BF, F32 = jnp.bfloat16, jnp.float32
LAYERS, D, FF, TOK = 2, 1024, 3200, 1024
LANES, ROWS, OCT = 128, 16, 8
PARTS, CHIPS, HALF = 6, 64, 32
TILE, TILES = 256, 13
TB = 2 * CHIPS
ORDER = ("x1", "y1", "z1", "x0", "y0", "z0")
GROUP, GROUPS, ROWS_GROUP = 8, 16, 200
PAIR = 2 * ROWS_GROUP
UNITS = ROWS_GROUP // ROWS
OWN_ROWS = ROWS_GROUP // GROUP
WIN = 32
RUN = 16
DEEP = 3

G1, D1, D0, G0, NW = 0, 4, 6, 8, 12
SHORT = (0, 3)
NS = 2
OWN_SLOT = (0, 1, 2, 0, 1, 2, 0, 3, 2, 0, 1, 2)
OWN_SLOTS = 4
NRS, NDD, NX = 3, 2, 4

T_F, T_FN, T_L1, T_DOWN1, T_DA, T_NORM, T_DOWN0, T_B0, T_TAIL = 0, 13, 14, 40, 44, 51, 52, 56, 69


def ticks(codes):
    return tuple(tuple(accumulate((ord(ch) - ord("0") for ch in code), initial=20))[1:] for code in codes)


RS_TICKS = ticks(('34427211', '74623257', '=4421211', 'C4223211', 'G2241417', 'K422521=', 'S2221271', 'U422143;', 'W4223433', '[2243473', ']6421831', 'a6263411'))
SHORT_RS_TICKS = ticks(('T2221693', 'I1242751'))
AG_TICKS = ticks(('J34;>A', 'Z96SP7', 'L343TE', 'T56=DM', '^A49>7', '`7:3JA', 'h;D9:C', 'p9:A@A', 'l;8?:3', 't9F?85', 'vC6I:9', 'x=L5:9'))
SHORT_AG_TICKS = ticks(('q6@@G9', 't=E>;;'))
DX = ticks(('e12', 'Z12'))
TICKS = max(max(t) for t in AG_TICKS + SHORT_AG_TICKS) + 1


def div(a, b):
    return a // b if isinstance(a, int) else lax.div(a, jnp.int32(b))


def mod(a, b):
    return a % b if isinstance(a, int) else lax.rem(a, jnp.int32(b))


def loop(n, fn):
    lax.fori_loop(0, n, fn, 0)


def base_of(x, y, z):
    r = 0
    for d in ORDER:
        v = {"x": x, "y": y, "z": z}[d[0]]
        r = TWO * r + gray(v, d)
    return r


def gray(v, d):
    h, l = div(v, 2), mod(v, 2)
    return h if d.endswith("1") else h + l - TWO * h * l


CHIP_AT = [None] * CHIPS
for _n in range(CHIPS):
    CHIP_AT[base_of(_n // 16, _n // 4 % 4, _n % 4)] = _n


def rotl(u, p):
    return mod(u * TWO**p, CHIPS) + div(u * TWO**p, CHIPS)


def rotr(u, p):
    return rotl(u, (PARTS - p) % PARTS)


def _flips(p):
    dims = [ORDER[(p + j) % PARTS] for j in (3, 4, 5)]
    return [tuple(d for d, bit in zip(dims, (4, 2, 1)) if e & bit) for e in range(1, OCT)]


def off_of(i):
    return pl.multiple_of(jnp.maximum(TILE * i - LANES, 0), LANES)


def aligned(start, size, to=None):
    return pl.ds(pl.multiple_of(start, to or size), size)


def dot(a, b, cb=0):
    return lax.dot_general(a, b, (((1,), (cb,)), ((), ())), preferred_element_type=F32)


def pick(w, values):
    r = values[0]
    for q, v in enumerate(values):
        if q:
            r = jnp.where(w == q, v, r)
    return r


def adam(w, m, v, g):
    m = 0.9 * m + 0.1 * g
    v = 0.95 * v + 0.05 * g * g
    step = m * lax.rsqrt(v + 1e-8) + 0.1 * w
    return (w - 0.02 * step).astype(BF).astype(F32), m, v


def rms_scale(squares):
    return lax.rsqrt(squares * (1.0 / D) + 1e-6)


def lanes(q):
    return slice(LANES * q, LANES * q + LANES)


def step_kernel(
    x, dy, w_gate, w_up, w_down, m_g, m_u, m_d, v_g, v_u, v_d,
    ag, agm, hidt, a0t, gu0, dgh, om_g, om_u, om_d, ov_g, ov_u, ov_d,
    acts, at, da, wgu, wdb, dgu, hidb, hts, htb, wr_g, wr_u, wr_d, md, vd,
    own, d2d, acc, r1, r2, r3, r4, s1, s2, s3, s4,
    d2dm, accm, q1, q2, q3, q4, t1, t2, t3, t4,
    gfin, xg, wsend, wrecv, fin, g_d, gx, ws_d, wx,
    lsem, wsem, gsem, dsem, hsem, htsem, d2s, d2r, ssem, rsem, xs, xr, wsm, wrm, agl, ags, agr, dags, dagr, dxs, dxr, d2c, rcred,
):
    dp = lax.axis_index("dp")
    c = mod(dp, 2)
    pos = {"x": div(dp, 32), "y": mod(div(dp, 8), 4), "z": mod(div(dp, 2), 4)}
    other = dp + 1 - TWO * c
    j_me = pos["z"] * TWO + c

    def device(x, y, z, core):
        return ((x * 4 + y) * 4 + z) * TWO + core

    def flipped(*dims):
        at = dict(pos)
        for d in dims:
            o = pos[d[0]]
            at[d[0]] = 3 - o if d.endswith("1") else o + 1 - TWO * mod(o, 2)
        return device(**at, core=c)

    bits = [gray(pos[d[0]], d) for d in ORDER]
    partners = [flipped(d) for d in ORDER]
    near = [_flips(p) for p in range(PARTS)]
    across = {dims: flipped(*dims) for dims in dict.fromkeys(d for ds in near for d in ds)}
    rot = [rotl(base_of(**pos), p) for p in range(PARTS)]

    def group_dev(j):
        return device(pos["x"], pos["y"], div(j, 2), mod(j, 2))

    def rcopy(src, dst, ss, rs, dev):
        return pltpu.make_async_remote_copy(src_ref=src, dst_ref=dst, send_sem=ss, recv_sem=rs, device_id={"dp": dev}, device_id_type=MESH)

    def signal(sem, dev):
        pl.semaphore_signal(sem, inc=1, device_id={"dp": dev}, device_id_type=MESH)

    copy = pltpu.make_async_copy

    barrier = pltpu.get_barrier_semaphore()
    for r in range(1, GROUP):
        signal(barrier, group_dev(mod(j_me + r, GROUP)))
    far = [q for dims, q in across.items() if dims not in (("z1",), ("z0",))]
    for q in far:
        signal(barrier, q)

    def weights(layer, i, b, gate_up=True, down=True):
        o = pl.ds(off_of(i), TILE)
        some = [copy(w_down.at[layer, o], wdb.at[b], wsem.at[b, 2])] if down else []
        if not gate_up:
            return some
        return some + [copy(w.at[layer, :, o], wgu.at[b, :, pl.ds(TILE * k, TILE)], wsem.at[b, k]) for k, w in enumerate((w_gate, w_up))]

    def saved(i, b):
        return weights(0, i, b, False) + [copy(gu0.at[i], da.at[pl.ds(b * TWO * TB, TWO * TB)], gsem.at[b])]

    def stream(make, i, b):
        for cp in make(i, b):
            cp.wait()

        @pl.when(i + 1 < TILES)
        def _():
            for cp in make(i + 1, ONE - b):
                cp.start()

    def as_blocks(v):
        return v.reshape(v.shape[0] // ROWS, ROWS, LANES)

    def get_da(q, rows, n):
        at_row = rows // ROWS if isinstance(rows, int) else div(rows, ROWS)
        return da[pl.ds(q * CHIPS + at_row, n // ROWS)].reshape(n, LANES)

    def sigmoid(v):
        return 1.0 / (1.0 + jnp.exp(-v))

    def through_act(gate, up, dhid):
        sg = sigmoid(gate)
        s = gate * sg
        return s, dhid * up * (sg * (1.0 + gate * (1.0 - sg))), dhid * s

    def counts(i):
        return (lax.broadcasted_iota(jnp.int32, (TOK, TILE), 1) < LANES) | (i > 0)

    def add_product(t):
        for q in range(OCT):
            o = pl.ds(q * CHIPS, CHIPS)
            da[o] = da[o] + as_blocks(t[:, lanes(q)])

    def hid_write(layer, i, b, q):
        o = pl.multiple_of(off_of(i) + LANES * q, LANES)
        return copy(hts.at[b, lanes(q)], hidt.at[layer, pl.ds(o, LANES)], hsem.at[b, q])

    def put_hidden(layer, i, b):
        for q in range(TWO):

            @pl.when(i >= 2 + q)
            def _():
                hid_write(layer, i - 2, b, q).wait()

        hts[b] = hidb[...].T
        for q in range(TWO):

            @pl.when(i >= q)
            def _():
                hid_write(layer, i, b, q).start()

    def hidden_out(layer):
        for i in (TILES - 2, TILES - 1):
            for q in range(TWO):
                hid_write(layer, i, i % TWO, q).wait()

    def gu_out(i, b):
        return copy(acc.at[pl.ds(b * TWO * TB, TWO * TB)], gu0.at[i], gsem.at[b])

    def tick_f(i):
        b = mod(i, 2)
        stream(functools.partial(weights, 0), i, b)

        @pl.when(i >= 2)
        def _():
            gu_out(i - 2, b).wait()

        gu = dot(acts[1], wgu[b])
        gate, up = gu[:, :TILE], gu[:, TILE:]
        hidb[...] = jnp.where(counts(i), gate * sigmoid(gate) * up, 0.0).astype(BF)
        for q in range(4):
            acc[pl.ds(TWO * b * TB + q * CHIPS, CHIPS)] = as_blocks(gu[:, lanes(q)])
        gu_out(i, b).start()
        add_product(dot(hidb[...], wdb[b]))
        put_hidden(0, i, b)

    def transpose_in():
        def part(k, _):
            t = acts[1, :, aligned(k * LANES, LANES)].T
            for q in range(OCT):
                n = k * OCT + q
                at[aligned(base_of(div(n, 16), mod(div(n, 4), 4), mod(n, 4)) * ROWS, ROWS)] = t[q * ROWS : (q + 1) * ROWS]
            return 0

        loop(D // LANES, part)

    def by_rows(fn):
        def chunk(k, _):
            fn(k * LANES, aligned(k * LANES, LANES))
            return 0

        loop(TOK // LANES, chunk)

    def norm_in(_, rows):
        h = acts[2, rows].astype(F32)
        acts[1, rows] = (h * rms_scale(jnp.sum(h * h, -1, keepdims=True))).astype(BF)

    def tick_fn():
        for b in range(TWO):
            gu_out(TILES - 2 + (b + TILES) % TWO, b).wait()

        def chunk(r, rows):
            o = jnp.concatenate([get_da(q, r, LANES) for q in range(OCT)], 1).astype(BF).astype(F32)
            acts[2, rows] = (acts[2, rows].astype(F32) + o).astype(BF)
            for q in range(OCT):
                da[pl.ds(q * CHIPS + div(r, ROWS), OCT)] = jnp.zeros((OCT, ROWS, LANES), F32)
            norm_in(r, rows)

        by_rows(chunk)
        a0t_out.wait()
        transpose_in()
        hidden_out(0)

    def dgu_out(i, b):
        return copy(dgu.at[b], dgh.at[i], dsem.at[b])

    def tick_a(i):
        b = mod(i, 2)
        stream(functools.partial(weights, 1), i, b)

        @pl.when(i >= 2)
        def _():
            dgu_out(i - 2, b).wait()


        gu = dot(acts[1], wgu[b])
        gate, up = gu[:, :TILE], gu[:, TILE:]
        dhid = dot(acts[0], wdb[b], 1).astype(BF).astype(F32)
        s, dgate, dup = through_act(gate, up, dhid)
        hidb[...] = (s * up).astype(BF)
        dgu[b, :, :TILE] = jnp.where(counts(i), dgate, 0.0).astype(BF)
        dgu[b, :, TILE:] = jnp.where(counts(i), dup, 0.0).astype(BF)

    def grads_gate_up(i, slot, layer, cuts):
        first = i == 0
        part = slot * PARTS + TWO * mod(i + 2, 3)
        pa = jnp.where(first, OWN_SLOTS * PARTS + TWO * layer, part)
        pb = jnp.where(first, slot * PARTS, part + 1)
        n = D // cuts

        def chunk(k, _):
            r = dot(at[aligned(k * n, n)], dgu[mod(i, 2)]).astype(BF)
            for q in range(4):
                own[q // TWO, pb if q % TWO else pa, pl.ds(k * (n // ROWS), n // ROWS)] = as_blocks(r[:, lanes(q)])
            return 0

        if cuts == 1:
            chunk(0, 0)
        else:
            loop(cuts, chunk)

    def wave_in_layer(i):
        return div(jnp.maximum(i - 1, 0), 3)

    def tick_b(i):
        b = mod(i, 2)
        grads_gate_up(i, mod(wave_in_layer(i), 3), 1, 1)
        dgu_out(i, b).start()
        put_hidden(1, i, b)

    def da_loads(i, b):
        return weights(1, i, b, down=False) + [copy(dgh.at[i], dgu.at[b], dsem.at[b])]

    def tick_da(k):
        def iteration(i, _):
            b = mod(i, 2)
            stream(da_loads, i, b)
            add_product(dot(dgu[b], wgu[b], 1))
            return 0

        lax.fori_loop(TWO * k, jnp.minimum(TWO * k + 2, TILES), iteration, 0)

    def hid_load(layer, r):
        return copy(hidt.at[layer, aligned(PAIR * r, PAIR, ROWS)], htb.at[mod(r, 2)], htsem.at[mod(r, 2)])

    def tick_down(k, layer):
        def iteration(r, _):
            hid_load(layer, r).wait()

            @pl.when(r + 1 < OCT)
            def _():
                hid_load(layer, r + 1).start()

            slots = [jnp.where(layer == 1, OWN_SLOT[D1 + q], OWN_SLOT[D0 + q]) * PARTS for q in range(TWO)]
            res = dot(htb[mod(r, 2)], acts[ONE - layer])
            for gg in range(TWO):
                g = TWO * r + gg
                at_xy = base_of(div(g, 4), mod(g, 4), 0)
                for lt in range(OCT):
                    place = at_xy + base_of(0, 0, lt % 4)
                    mine = res[gg * ROWS_GROUP : (gg + 1) * ROWS_GROUP, lanes(lt)]
                    for u in range(UNITS):
                        own[lt // 4, slots[u // PARTS] + u % PARTS, place] = mine[ROWS * u : ROWS * u + ROWS].astype(BF)
                    last = jnp.concatenate([mine[ROWS * UNITS :], jnp.zeros((OCT, LANES), F32)], 0)
                    own[lt // 4, OWN_SLOTS * PARTS + TWO * layer + 1, place] = last.astype(BF)
            return 0

        lax.fori_loop(TWO * k, TWO * k + 2, iteration, 0)

    def tick_norm():
        def chunk(r, rows):
            h = acts[2, rows].astype(F32)
            g = jnp.concatenate([get_da(q, r, LANES) for q in range(OCT)], 1).astype(BF).astype(F32)
            scale = rms_scale(jnp.sum(h * h, -1, keepdims=True))
            back = scale * scale * scale * jnp.sum(h * g, -1, keepdims=True) * (1.0 / D)
            dh = (g * scale - h * back).astype(BF).astype(F32)
            acts[1, rows] = (acts[0, rows].astype(F32) + dh).astype(BF)

        by_rows(chunk)

    def tick_back0(i):
        b = mod(i, 2)
        stream(saved, i, b)

        def chunk(k, _):
            n = TOK // TWO
            rows = aligned(k * n, n)
            dhid = dot(acts[1, rows], wdb[b], 1).astype(BF).astype(F32)
            gate, up = (jnp.concatenate([get_da(4 * b + TWO * m + q, k * n, n) for q in range(TWO)], 1) for m in range(TWO))
            _, dgate, dup = through_act(gate, up, dhid)
            dgu[b, rows, :TILE] = dgate.astype(BF)
            dgu[b, rows, TILE:] = dup.astype(BF)
            return 0

        loop(2, chunk)
        grads_gate_up(i, pick(wave_in_layer(i), OWN_SLOT[G0:]), 0, 2)

    a0t_out = copy(at, a0t, lsem.at[0])
    a0t_in = copy(a0t, at, lsem.at[0])

    def compute(t):
        def between(lo, hi, fn):
            @pl.when((t >= lo) & (t < hi))
            def _():
                fn(t - lo)

        between(T_F, T_FN, tick_f)

        @pl.when(t == T_FN)
        def _():
            for cp in weights(1, 0, 0):
                cp.start()
            tick_fn()
            loads[1].wait()

        @pl.when((t >= T_L1) & (t < T_DOWN1) & (mod(t, 2) == T_L1 % TWO))
        def _():
            tick_a(div(t - T_L1, 2))

        @pl.when((t >= T_L1) & (t < T_DOWN1) & (mod(t, 2) != T_L1 % TWO))
        def _():
            tick_b(div(t - T_L1, 2))

        @pl.when(t == T_DOWN1 - 1)
        def _():
            hid_load(1, 0).start()
            a0t_in.start()

        @pl.when(t == T_DOWN1)
        def _():
            hidden_out(1)
            for i in (TILES - 2, TILES - 1):
                dgu_out(i, i % TWO).wait()
            for cp in da_loads(0, 0):
                cp.start()

        @pl.when(((t >= T_DOWN1) & (t < T_DA)) | ((t >= T_DOWN0) & (t < T_B0)))
        def _():
            layer = jnp.where(t < T_NORM, 1, 0)
            tick_down(t - jnp.where(t < T_NORM, T_DOWN1, T_DOWN0), layer)

        between(T_DA, T_NORM, tick_da)

        @pl.when(t == T_NORM)
        def _():
            hid_load(0, 0).start()
            tick_norm()
            for cp in saved(0, 0):
                cp.start()
            a0t_in.wait()

        between(T_B0, T_TAIL, tick_back0)

    def L(j):
        return 2 ** (PARTS - j)

    starts = [[div(r, L(j)) * L(j) for j in range(PARTS + 1)] for r in rot]

    def kept(p, j):
        return starts[p][j]

    def lag_start(makers):
        last = None
        for make in makers:
            cp = make()
            if last is not None:
                last.start()
            last = cp
        last.start()

    class Full:
        parts = tuple(range(PARTS))
        accumulated, received, sent, crossed, ag_ref = acc, (None, r1, r2, r3, r4), (None, s1, s2, s3, s4), d2d, ag

        def __init__(self, w):
            self.w, self.id, self.r, self.s, self.f = w, w, mod(w, NRS), mod(w, NDD), mod(w, NX)
            self.own = pick(w, OWN_SLOT) * PARTS

    class Short:
        parts = SHORT
        accumulated, received, sent, crossed, ag_ref = accm, (None, q1, q2, q3, q4), (None, t1, t2, t3, t4), d2dm, agm

        def __init__(self, w):
            self.w, self.id, self.r, self.s, self.f = w, NW + w, w, w, NX + w
            self.own = OWN_SLOTS * PARTS + TWO * w

    def sems(v):
        return (v.r, v.s) if isinstance(v, Full) else (NRS + v.r, NDD + v.s)

    def crossing(v):
        s = sems(v)[1]
        return rcopy(own.at[ONE - c, pl.ds(v.own, len(v.parts))], v.crossed.at[v.s], d2s.at[s], d2r.at[s], other)

    def stage_all(v, j):
        s = sems(v)[0]
        return rcopy(v.sent[j].at[v.r], v.received[j].at[v.r], ssem.at[s, j - ONE], rsem.at[s, j - ONE], other)

    def stage_one(v, j, k):
        s = sems(v)[0]
        to = partners[(v.parts[k] + j - ONE) % PARTS]
        return rcopy(v.sent[j].at[v.r, k], v.received[j].at[v.r, k], ssem.at[s, j - ONE], rsem.at[s, j - ONE], to)

    def acc_at(v, k):
        return (v.r * len(v.parts) + k) * HALF

    def rs0(v):
        if isinstance(v, Full):

            @pl.when(v.w >= NDD)
            def _():
                pl.semaphore_wait(d2c.at[v.s], 1)

        crossing(v).start()

    def rs1(v):
        crossing(v).wait_recv()
        if isinstance(v, Full):

            @pl.when(v.w >= NRS)
            def _():
                pl.semaphore_wait(rcred.at[v.r], len(partners))

        def make(k):
            p = v.parts[k]
            b = bits[p]
            lv, kp = (ONE - b) * TWO ** (PARTS - ONE - p), b * TWO ** (PARTS - ONE - p)
            def some(g, _):
                at_g = rotr(g * RUN, p)
                for i in range(RUN):
                    u = at_g + rotr(i, p)
                    both = [own[c, v.own + k, o + u].astype(F32) + v.crossed[v.s, k, o + u].astype(F32) for o in (lv, kp)]
                    v.sent[1][v.r, k, g * RUN + i] = both[0].astype(BF)
                    v.accumulated[acc_at(v, k) + g * RUN + i] = both[1]
                return 0

            loop(HALF // RUN, some)
            return stage_one(v, 1, k)

        lag_start([functools.partial(make, k) for k in range(len(v.parts))])
        crossing(v).wait_send()
        if isinstance(v, Full):

            @pl.when(v.w + NDD < NW)
            def _():
                signal(d2c.at[v.s], other)

    def peer_block(p, e):
        r = 0
        for j, bit in zip((3, 4, 5), (4, 2, 1)):
            own_bit = bits[(p + j) % PARTS]
            r = TWO * r + (ONE - own_bit if e & bit else own_bit)
        return r

    def seven(v, ref):
        s = sems(v)[0]
        view = ref.at[v.r, :, pl.ds(0, OCT - 1)]
        return rcopy(view, view, ssem.at[s, 3], rsem.at[s, 3], other)

    def rs4(v):
        stage_all(v, 3).wait_recv()

        def make(k):
            p = v.parts[k]
            o = pl.ds(acc_at(v, k) + kept(p, 3) - kept(p, 1), OCT)
            total = v.accumulated[o] + v.received[3][v.r, k].astype(F32)
            v.accumulated[o] = total
            v.sent[4][v.r, k] = total.astype(BF)
            s = sems(v)[0]
            return [
                rcopy(v.sent[4].at[v.r, k, peer_block(p, e)], v.received[4].at[v.r, k, e - 1], ssem.at[s, 3], rsem.at[s, 3], across[near[p][e - 1]])
                for e in range(1, OCT)
            ]

        last = []
        for k in range(len(v.parts) + 1):
            made = make(k) if k < len(v.parts) else []
            for cp in last:
                cp.start()
            last = made

    def rsj(j, v):
        stage_all(v, j - ONE).wait_recv()
        n = L(j)
        ch = min(n, OCT)

        def make(k):
            p = v.parts[k]
            b = bits[(p + j - ONE) % PARTS]
            o = acc_at(v, k) + kept(p, j - ONE) - kept(p, 1)
            for i in range(0, n, ch):
                lv, kp = (ONE - b) * n + i, b * n + i
                both = [v.accumulated[pl.ds(o + h, ch)] + v.received[j - ONE][v.r, k, pl.ds(h, ch)].astype(F32) for h in (lv, kp)]
                v.sent[j][v.r, k, pl.ds(i, ch)] = both[0].astype(BF)
                v.accumulated[pl.ds(o + kp, ch)] = both[1]
            return stage_one(v, j, k)

        lag_start([functools.partial(make, k) for k in range(len(v.parts))])

    def is_down(w):
        return (w >= D1) & (w < G0)

    def exchange(v):
        return rcopy(gfin.at[v.f, ONE - c], xg.at[v.id], xs.at[v.f], xr.at[v.id], other)

    def rs5(v):
        seven(v, v.received[4]).wait_recv()
        for k, p in enumerate(v.parts):
            g = v.accumulated[acc_at(v, k) + rot[p] - kept(p, 1)]
            for e in range(OCT - 1):
                g = g + v.received[4][v.r, k, e].astype(F32)
            g = g.astype(BF).astype(F32)
            for h in range(TWO):
                gfin[v.f, h, k] = g[OCT * h : OCT * h + OCT]
        for j in range(1, 4):
            stage_all(v, j).wait_send()
        seven(v, v.sent[4]).wait_send()
        if isinstance(v, Short):
            g_d[v.w, ROWS * UNITS : ROWS * UNITS + OCT] = gfin[v.f, 0, 1]
            exchange(v).start()
            return

        @pl.when(v.w + NRS < NW)
        def _():
            for q in partners:
                signal(rcred.at[v.r], q)

        @pl.when(is_down(v.w))
        def _():
            for p in range(PARTS):
                for h in range(TWO):
                    g_d[jnp.where(v.w < D0, 1, 0), aligned((mod(v.w, 2) * PARTS + p) * ROWS + OCT * h, OCT)] = gfin[v.f, h, p]

        @pl.when(~is_down(v.w))
        def _():
            exchange(v).start()

    def adam_tile(layer, col, v, k):
        cols = aligned(col, LANES)
        mine, theirs = gfin[v.f, c, k], xg[v.id, k]
        for mat, (wr, om, ov) in enumerate(((wr_g, om_g, ov_g), (wr_u, om_u, ov_u))):
            g = jnp.where(c == mat, mine, theirs)
            wn, mn, vn = adam(wr[layer, :, cols].astype(F32), om[layer, :, cols], ov[layer, :, cols], g)
            om[layer, :, cols] = mn
            ov[layer, :, cols] = vn
            wsend[v.f, mat, k] = wn

    def w_exchange(v):
        return rcopy(wsend.at[v.f, ONE - c], wrecv.at[v.id], wsm.at[v.f], wrm.at[v.id], other)

    def unless_down(fn):
        def run(v):
            if isinstance(v, Short):
                fn(v)
            else:

                @pl.when(~is_down(v.w))
                def _():
                    fn(v)

        run.__name__ = fn.__name__
        return run

    @unless_down
    def rs6(v):
        exchange(v).wait_recv()
        if isinstance(v, Short):
            adam_tile(v.w, 0, v, 0)
            for mat in range(TWO):
                for k in range(1, PARTS):
                    wsend[v.f, mat, k] = jnp.zeros((OCT, LANES), F32)
        else:
            layer = jnp.where(v.w < G0, 1, 0)
            for k in range(PARTS):
                adam_tile(layer, LANES + PARTS * LANES * (v.w - jnp.where(v.w < G0, 0, G0)) + LANES * k, v, k)
        exchange(v).wait_send()
        w_exchange(v).start()

    @unless_down
    def rs7(v):
        w_exchange(v).wait_recv()
        for k in range(PARTS if isinstance(v, Full) else 1):
            mine, theirs = wsend[v.f, c, k], wrecv[v.id, k]
            fin[v.id, k] = jnp.concatenate([jnp.where(c == 0, mine, theirs), jnp.where(c == 0, theirs, mine)], 0).astype(BF)
        w_exchange(v).wait_send()

    def window(j):
        return div(OWN_ROWS * j, OCT) * OCT

    def to_group(k, layer, src, dst):
        for r in range(1, GROUP):
            j = mod(j_me + r, GROUP)
            rcopy(src(j), dst.at[layer, j_me], dxs.at[k, layer], dxr.at[k, layer], group_dev(j)).start()

    def from_group(k, layer, dst):
        seven = dst.at[layer, pl.ds(0, GROUP - 1)]
        cp = rcopy(seven, seven, dxs.at[k, layer], dxr.at[k, layer], other)
        cp.wait_recv()
        cp.wait_send()

    def dx1(layer):
        def src(j):
            return g_d.at[layer, aligned(window(j), WIN, OCT)]

        to_group(0, layer, src, gx)

        def row(r, _):
            for o, t in ((om_d, md), (ov_d, vd)):
                o[layer, pl.ds(r, 1)] = t[r, pl.ds(layer, 1)]
            return 0

        loop(OWN_ROWS, row)
        gx[layer, j_me] = g_d[layer, aligned(window(j_me), WIN, OCT)]

    def dx2(layer):
        from_group(0, layer, gx)
        shift = mod(OWN_ROWS * j_me, OCT)
        row = lax.broadcasted_iota(jnp.int32, (WIN, LANES), 0)
        valid = (row >= shift) & (row < shift + OWN_ROWS)
        def tile(lt, _):
            cols = aligned(lt * LANES, LANES)
            m, s = (pltpu.roll(t[layer, :, cols], shift, 0) for t in (om_d, ov_d))
            wn, mn, vn = adam(wr_d[layer, :, cols].astype(F32), m, s, gx[layer, TWO * mod(lt, 4) + div(lt, 4)])
            for o, t in ((om_d, mn), (ov_d, vn)):
                o[layer, :, cols] = pltpu.roll(t, mod(WIN - shift, WIN), 0)
            ws_d[layer, lt] = jnp.where(valid, wn, 0.0)
            return 0

        loop(OCT, tile)

        def src(j):
            return ws_d.at[layer, 4 * mod(j, 2) + div(j, 2)]

        to_group(1, layer, src, wx)
        wx[layer, j_me] = ws_d[layer, 4 * c + pos["z"]]

    def dx3(layer):
        from_group(1, layer, wx)
        octets = [None] * (TWO * UNITS + 2)
        for j in range(GROUP):
            for k in range(WIN // OCT):
                o, t = window(j) // OCT + k, wx[layer, j, OCT * k : OCT * k + OCT]
                octets[o] = t if octets[o] is None else octets[o] + t
        octets[-1] = jnp.zeros((OCT, LANES), F32)
        for u in range(UNITS + 1):
            block = jnp.concatenate(octets[TWO * u : TWO * u + 2], 0).astype(BF)
            if u < UNITS:
                fin[jnp.where(layer == 1, D1, D0) + u // PARTS, u % PARTS] = block
            else:
                fin[NW + layer, 1] = block

    def part_of(v):
        return v.ag_ref.at[v.w, c]

    def ag1(v):
        for k, p in enumerate(v.parts):
            src, dst = fin.at[v.id, k], part_of(v).at[k, rot[p]]
            copy(src, dst, agl.at[v.id]).start()
            for dims in near[p]:
                rcopy(src, dst, ags.at[v.id], agr.at[v.id, 0], across[dims]).start()

    def agk(k, v):
        n = 2 ** (k - 2)
        mine = part_of(v)
        first = k == 4
        if first:
            copy(fin.at[v.id, pl.ds(0, len(v.parts))], mine.at[:, 0], agl.at[v.id]).wait()
        came = mine.at[:, pl.ds(0, OCT - 1 if first else n)]
        rcopy(came, came, ags.at[v.id], agr.at[v.id, 0 if first else k - 4], other).wait_recv()
        j = PARTS + ONE - k
        for q, p in enumerate(v.parts):
            if k <= PARTS:
                h = mine.at[q, pl.ds(kept(p, j), TWO * n)]
                rcopy(h, h, ags.at[v.id], agr.at[v.id, k - 3], partners[(p + j - ONE) % PARTS]).start()
            g = mine.at[q, pl.ds(kept(p, j), OCT) if first else pl.ds(kept(p, j) + (ONE - bits[(p + j) % PARTS]) * n, n)]
            rcopy(g, g, dags.at[v.id], dagr.at[v.id], other).start()

    def ag_end(v):
        most = part_of(v).at[:, pl.ds(0, CHIPS - 1)]
        rcopy(most, most, ags.at[v.id], agr.at[v.id, 0], other).wait_send()
        cp = rcopy(part_of(v), part_of(v), dags.at[v.id], dagr.at[v.id], other)
        cp.wait_send()
        cp.wait_recv()

    rs_stages = [rs0, rs1, functools.partial(rsj, 2), functools.partial(rsj, 3), rs4, rs5, rs6, rs7]
    ag_stages = [ag1] + [functools.partial(agk, k) for k in range(4, PARTS + 2)] + [ag_end]

    def find(t, table):
        terms = [jnp.where(t == s, q + 1, 0) for q, s in enumerate(table)]
        while len(terms) > 1:
            terms = [sum(terms[q : q + 2]) for q in range(0, len(terms), 2)]
        return terms[0]

    def run(fn, t, kind, ticks):
        w = find(t, ticks)

        @pl.when(w > 0)
        def _():
            fn(kind(w - 1))

    def within(t, ticks, fn):
        pl.when((t >= min(min(ticks))) & (t <= max(max(ticks))))(fn)

    def stages(fns, t, full, short):
        full, short = tuple(zip(*full)), tuple(zip(*short))

        def full_ones():
            for odd in range(TWO):

                @pl.when(mod(t, 2) == odd)
                def _():
                    for fn, due in zip(reversed(fns), reversed(full)):
                        if due[0] % TWO == odd:
                            run(fn, t, Full, due)

        def short_ones():
            for fn, due in zip(reversed(fns), reversed(short)):
                run(fn, t, Short, due)

        within(t, full, full_ones)
        within(t, short, short_ones)

    def moves(t):
        stages(rs_stages, t, RS_TICKS, SHORT_RS_TICKS)
        for q, fn in enumerate((dx1, dx2, dx3)):

            @pl.when((t == DX[0][q]) | (t == DX[1][q]))
            def _():
                fn(jnp.where(t == DX[1][q], 1, 0))

        stages(ag_stages, t, AG_TICKS, SHORT_AG_TICKS)

    loads = [copy(x, acts.at[2], lsem.at[1]), copy(dy, acts.at[0], lsem.at[2])]
    rows_in = [copy(w.at[:, aligned(dp * OCT, OCT)], o, lsem.at[3 + k]) for k, (w, o) in enumerate(((w_gate, wr_g), (w_up, wr_u)))]
    rows_in.append(copy(w_down.at[:, aligned(div(OWN_ROWS * dp, OCT) * OCT, WIN, OCT)], wr_d, lsem.at[5]))
    moments = ((m_g, om_g), (m_u, om_u), (m_d, md), (v_g, ov_g), (v_u, ov_u), (v_d, vd))
    rows_in += [copy(m, o, lsem.at[6 + k]) for k, (m, o) in enumerate(moments)]
    for cp in loads + weights(0, 0, 0) + rows_in:
        cp.start()
    for q in range(OCT):
        da[pl.ds(q * CHIPS, CHIPS)] = jnp.zeros((CHIPS, ROWS, LANES), F32)
    loads[0].wait()
    by_rows(norm_in)
    transpose_in()
    a0t_out.start()
    for cp in rows_in:
        cp.wait()
    pl.semaphore_wait(barrier, GROUP - 1 + len(far))

    def tick(t, _):
        compute(t)
        moves(t)
        return 0

    loop(TICKS, tick)


def step_call(args):
    B = (ROWS, LANES)
    V, R, S = pltpu.VMEM, pltpu.SemaphoreType.REGULAR, pltpu.SemaphoreType.DMA
    sizes = [HALF, HALF // TWO, OCT, OCT]
    n, ns = NW + NS, len(SHORT)
    own_parts = OWN_SLOTS * PARTS + NS * ns
    E = (PARTS, OCT, LANES)
    scratch = [
        V((3, TOK, D), BF), V((D, TOK), BF), V((4 * TB, *B), F32), V((TWO, D, TWO * TILE), BF), V((TWO, TILE, D), BF),
        V((TWO, TOK, TWO * TILE), BF), V((TOK, TILE), BF), V((TWO, TILE, TOK), BF), V((TWO, PAIR, TOK), BF),
        *[V((LAYERS, OCT, FF), BF)] * TWO, V((LAYERS, WIN, D), BF), *[V((OWN_ROWS, LAYERS, D), F32)] * TWO,
        V((TWO, own_parts, CHIPS, *B), BF), V((NDD, PARTS, CHIPS, *B), BF), V((NRS * PARTS * HALF, *B), F32),
        *[V((NRS, PARTS, k, *B), BF) for k in sizes * TWO],
        V((NS, ns, CHIPS, *B), BF), V((NS * ns * HALF, *B), F32),
        *[V((NS, ns, k, *B), BF) for k in sizes * TWO],
        V((NX + NS, TWO, *E), F32), V((n, *E), F32), V((NX + NS, TWO, *E), F32), V((n, *E), F32), V((n, PARTS, *B), BF),
        V((LAYERS, ROWS * (UNITS + 1), LANES), F32), *[V((LAYERS, GROUP, WIN, LANES), F32)] * 3,
        S((12,)), S((TWO, 3)), S((TWO,)), S((TWO,)), S((TWO, 2)), S((TWO,)), S((NDD + NS,)), S((NDD + NS,)), S((NRS + NS, PARTS)), S((NRS + NS, PARTS)),
        S((NX + NS,)), S((n,)), S((NX + NS,)), S((n,)), S((n,)), S((n,)), S((n, PARTS)), S((n,)), S((n,)), S((TWO, LAYERS)), S((TWO, LAYERS)),
        R((NDD,)), R((NRS,)),
    ]
    hbm, vmem = pl.BlockSpec(memory_space=pl.ANY), pl.BlockSpec(memory_space=pltpu.VMEM)
    out = [((NW, TWO, PARTS, CHIPS, *B), BF), ((NS, 2, ns, CHIPS, *B), BF), ((LAYERS, FF, TOK), BF), ((D, TOK), BF), ((TILES, TWO * TB, *B), F32), ((TILES, TOK, TWO * TILE), BF)]
    out += [(s, F32) for s in ((LAYERS, OCT, FF), (LAYERS, OCT, FF), (LAYERS, WIN, D))] * TWO
    return pl.pallas_call(
        step_kernel,
        out_shape=[jax.ShapeDtypeStruct(*o) for o in out],
        in_specs=[hbm] * 11,
        out_specs=[hbm] * 6 + [vmem] * 6,
        scratch_shapes=scratch,
        compiler_params=pltpu.CompilerParams(collective_id=0, has_side_effects=True, vmem_limit_bytes=67043328),
        name="step",
    )(*args)


def place_kernel(
    ag, agm, om_g, om_u, om_d, ov_g, ov_u, ov_d, gate, up, down, pm_g, pm_u, pm_d, pv_g, pv_u, pv_d, buf, dbuf, mbuf, stage, mstage, dstage,
    isem, dsem, msem, osem, mosem, dosem,
):
    copy = pltpu.make_async_copy
    jobs = G0
    outs = (gate, up)

    def load(k):
        return copy(ag.at[jnp.where(k < D1, k, k + D1)], buf.at[mod(k, DEEP)], isem.at[mod(k, DEEP)])

    def stores(k):
        cols = aligned(LANES + PARTS * LANES * mod(k, 4), PARTS * LANES, LANES)
        return [copy(stage.at[mod(k, 2), m], o.at[jnp.where(k < D1, 1, 0), :, cols], osem.at[mod(k, 2), m]) for m, o in enumerate(outs)]

    def load_down(layer):
        return copy(ag.at[pl.ds(pick(layer, (D0, D1)), 2)], dbuf.at[layer], dsem.at[layer])

    def store_down(k):
        rows = aligned(mod(k, 4) * TWO * PAIR, TWO * PAIR, ROWS)
        return copy(dstage.at[mod(k, 2)], down.at[jnp.where(k < D1, 1, 0), rows], dosem.at[mod(k, 2)])

    def store_short(layer, m):
        return copy(mstage.at[layer, m], outs[m].at[layer, :, lanes(0)], mosem.at[layer, m])

    mini = copy(agm, mbuf, msem.at[0])
    for cp in (load(0), load(1), load_down(1), mini, load(2), load_down(0)):
        cp.start()

    def by_chip(dst, cols, src, p):
        for u in range(CHIPS):
            n = CHIP_AT[u]
            dst[ROWS * n : ROWS * n + ROWS, cols] = src[rotl(u, p)]

    def body(k, _):
        @pl.when(k < jobs)
        def _():
            load(k).wait()

            @pl.when(k >= 2)
            def _():
                for cp in stores(k - 2):
                    cp.wait()

            for m in range(TWO):
                for p in range(PARTS):
                    by_chip(stage.at[mod(k, 2), m], lanes(p), buf.at[mod(k, DEEP), m, p], p)
            for cp in stores(k):
                cp.start()

            @pl.when(k + DEEP < jobs)
            def _():
                load(k + DEEP).start()

        @pl.when(k >= 1)
        def _():
            down_job(k - ONE)

        return 0

    def down_job(k):
        layer = jnp.where(k < D1, 1, 0)

        @pl.when(k == 0)
        def _():
            mini.wait()
            for layer in range(LAYERS):
                for m in range(TWO):
                    by_chip(mstage.at[layer, m], lanes(0), mbuf.at[layer, m, 0], SHORT[0])
                    store_short(layer, m).start()

        @pl.when(mod(k, 4) == 0)
        def _():
            load_down(layer).wait()

        @pl.when(k >= 2)
        def _():
            store_down(k - 2).wait()

        def pair(q, _):
            for lt in range(OCT):
                h = lt // 4
                octets = []
                for gg in range(TWO):
                    g = (mod(k, 4) * TWO + q) * TWO + gg
                    spot = base_of(div(g, 4), mod(g, 4), 0) + base_of(0, 0, lt % 4)
                    for u in range(UNITS + 1):
                        if u < UNITS:
                            t = dbuf[layer, u // PARTS, h, u % PARTS, rotl(spot, u % PARTS)].astype(F32)
                        else:
                            t = mbuf[layer, h, 1, rotl(spot, SHORT[1])].astype(F32)[:OCT]
                        octets.append(t)
                dstage[mod(k, 2), aligned(PAIR * q, PAIR, ROWS), lanes(lt)] = jnp.concatenate(octets, 0).astype(BF)
            return 0

        loop(2, pair)
        store_down(k).start()

        @pl.when(k == jobs - 1)
        def _():
            for o, t in ((pm_g, om_g), (pm_u, om_u), (pv_g, ov_g), (pv_u, ov_u)):
                o[...] = t[...]
            for o, t in ((pm_d, om_d), (pv_d, ov_d)):
                for layer in range(LAYERS):
                    for r in range(OWN_ROWS):
                        o[r, layer : layer + 1] = t[layer, r : r + 1]

    loop(jobs + 1, body)
    for k in (jobs - 2, jobs - 1):
        for cp in stores(k) + [store_down(k)]:
            cp.wait()
    for layer in range(LAYERS):
        for m in range(TWO):
            store_short(layer, m).wait()


def place_call(args):
    hbm, vmem = pl.BlockSpec(memory_space=pl.ANY), pl.BlockSpec(memory_space=pltpu.VMEM)
    V, S = pltpu.VMEM, pltpu.SemaphoreType.DMA
    whole = (TWO, PARTS, CHIPS, ROWS, LANES)
    out = [(s, BF) for s in ((LAYERS, D, FF), (LAYERS, D, FF), (LAYERS, FF, D))]
    out += [(s, F32) for s in ((LAYERS, OCT, FF), (LAYERS, OCT, FF), (OWN_ROWS, LAYERS, D))] * TWO
    return pl.pallas_call(
        place_kernel,
        out_shape=[jax.ShapeDtypeStruct(*o) for o in out],
        in_specs=[hbm] * TWO + [vmem] * 6,
        out_specs=[hbm] * 3 + [vmem] * 6,
        scratch_shapes=[
            V((DEEP, *whole), BF), V((LAYERS, TWO, *whole), BF), V((NS, 2, len(SHORT), CHIPS, ROWS, LANES), BF),
            V((TWO, TWO, D, PARTS * LANES), BF), V((LAYERS, TWO, D, LANES), BF), V((TWO, TWO * PAIR, D), BF),
            S((DEEP,)), S((TWO,)), S((1,)), S((TWO, 2)), S((TWO, 2)), S((TWO,)),
        ],
        compiler_params=pltpu.CompilerParams(vmem_limit_bytes=60 * TWO**20),
        name="place",
    )(*args)


def local_step(x, dy, w_gate, w_up, w_down, m_g, m_u, m_d, v_g, v_u, v_d):
    m_d, v_d = (jnp.transpose(t, (1, 0, 2)) for t in (m_d, v_d))
    ag, agm, _, _, _, _, *moments = step_call((x[0], dy[0], w_gate, w_up, w_down, m_g, m_u, m_d, v_g, v_u, v_d))
    gate, up, down, om_g, om_u, om_d, ov_g, ov_u, ov_d = place_call((ag, agm, *moments))
    om_d, ov_d = (jnp.transpose(t, (1, 0, 2)) for t in (om_d, ov_d))
    return gate, up, down, om_g, om_u, om_d, ov_g, ov_u, ov_d


def solution(mesh):
    moment = P(None, "dp", None)
    return jax.shard_map(
        local_step,
        mesh=mesh,
        in_specs=(P(("rep", "dp")), P(("rep", "dp")), P(), P(), P(), *[moment] * 6),
        out_specs=(P("rep"), P("rep"), P("rep"), *[P("rep", "dp", None)] * 6),
        check_vma=False,
    )
```

```python
import functools
from itertools import accumulate

import jax
import jax.numpy as jnp
from jax import lax
from jax.experimental import pallas as pl
from jax.experimental.pallas import tpu as pltpu
from jax.sharding import PartitionSpec as P

MESH = pl.DeviceIdType.MESH
ONE, TWO = 1, 2
BF, F32 = jnp.bfloat16, jnp.float32
LAYERS, D, FF, TOK = 2, 1024, 3200, 1024
LANES, ROWS, OCT = 128, 16, 8
PARTS, CHIPS, HALF = 6, 64, 32
TILE, TILES = 256, 13
TB = 2 * CHIPS
ORDER = ("x1", "y1", "z1", "x0", "y0", "z0")
GROUP, GROUPS, ROWS_GROUP = 8, 16, 200
PAIR = 2 * ROWS_GROUP
UNITS = ROWS_GROUP // ROWS
OWN_ROWS = ROWS_GROUP // GROUP
WIN = 32
RUN = 16
DEEP = 3

G1, D1, D0, G0, NW = 0, 4, 6, 8, 12
SHORT = (0, 3)
NS = 2
OWN_SLOT = (0, 1, 2, 0, 1, 2, 0, 3, 2, 0, 1, 2)
OWN_SLOTS = 4
NRS, NDD, NX = 3, 2, 4

T_F, T_FN, T_L1, T_DOWN1, T_DA, T_NORM, T_DOWN0, T_B0, T_TAIL = 0, 13, 14, 40, 44, 51, 52, 56, 69


def ticks(codes):
    return tuple(tuple(accumulate((ord(ch) - ord("0") for ch in code), initial=20))[1:] for code in codes)


RS_TICKS = ticks(('14322411', '74322211', '=4322211', 'C2322411', 'G2322211', 'I2322211', 'S2322211', 'U2322211', 'W2322611', '[4344411', ']4544411', 'a6362411'))
SHORT_RS_TICKS = ticks(('T2321211', 'G2322212'))
AG_TICKS = ticks(('B23234', 'F23432', 'L43254', 'R23432', 'Z23472', '\\45654', 'n47674', 'j63652', 'h63454', 'p43654', 't45656', 'x45474'))
SHORT_AG_TICKS = ticks(('j43441', 'Z23731'))
DX = ticks(('`64', 'T33'))
TICKS = max(max(t) for t in AG_TICKS + SHORT_AG_TICKS) + 1


def div(a, b):
    return a // b if isinstance(a, int) else lax.div(a, jnp.int32(b))


def mod(a, b):
    return a % b if isinstance(a, int) else lax.rem(a, jnp.int32(b))


def loop(n, fn):
    lax.fori_loop(0, n, fn, 0)


def base_of(x, y, z):
    r = 0
    for d in ORDER:
        v = {"x": x, "y": y, "z": z}[d[0]]
        r = TWO * r + gray(v, d)
    return r


def gray(v, d):
    h, l = div(v, 2), mod(v, 2)
    return h if d.endswith("1") else h + l - TWO * h * l


CHIP_AT = [None] * CHIPS
for _n in range(CHIPS):
    CHIP_AT[base_of(_n // 16, _n // 4 % 4, _n % 4)] = _n


def rotl(u, p):
    return mod(u * TWO**p, CHIPS) + div(u * TWO**p, CHIPS)


def rotr(u, p):
    return rotl(u, (PARTS - p) % PARTS)


def _flips(p):
    dims = [ORDER[(p + j) % PARTS] for j in (3, 4, 5)]
    return [tuple(d for d, bit in zip(dims, (4, 2, 1)) if e & bit) for e in range(1, OCT)]


def off_of(i):
    return pl.multiple_of(jnp.maximum(TILE * i - LANES, 0), LANES)


def aligned(start, size, to=None):
    return pl.ds(pl.multiple_of(start, to or size), size)


def dot(a, b, cb=0):
    return lax.dot_general(a, b, (((1,), (cb,)), ((), ())), preferred_element_type=F32)


def pick(w, values):
    r = values[0]
    for q, v in enumerate(values):
        if q:
            r = jnp.where(w == q, v, r)
    return r


def adam(w, m, v, g):
    m = 0.9 * m + 0.1 * g
    v = 0.95 * v + 0.05 * g * g
    step = m * lax.rsqrt(v + 1e-8) + 0.1 * w
    return (w - 0.02 * step).astype(BF).astype(F32), m, v


def rms_scale(squares):
    return lax.rsqrt(squares * (1.0 / D) + 1e-6)


def lanes(q):
    return slice(LANES * q, LANES * q + LANES)


def step_kernel(
    x, dy, w_gate, w_up, w_down, m_g, m_u, m_d, v_g, v_u, v_d,
    ag, agm, hidt, a0t, gu0, dgh, om_g, om_u, om_d, ov_g, ov_u, ov_d,
    acts, at, da, wgu, wdb, dgu, hidb, hts, htb, wr_g, wr_u, wr_d, md, vd,
    own, d2d, acc, r1, r2, r3, r4, s1, s2, s3, s4,
    d2dm, accm, q1, q2, q3, q4, t1, t2, t3, t4,
    gfin, xg, wsend, wrecv, fin, g_d, gx, ws_d, wx,
    lsem, wsem, gsem, dsem, hsem, htsem, d2s, d2r, ssem, rsem, xs, xr, wsm, wrm, agl, ags, agr, dags, dagr, dxs, dxr, d2c, rcred,
):
    dp = lax.axis_index("dp")
    c = mod(dp, 2)
    pos = {"x": div(dp, 32), "y": mod(div(dp, 8), 4), "z": mod(div(dp, 2), 4)}
    other = dp + 1 - TWO * c
    j_me = pos["z"] * TWO + c

    def device(x, y, z, core):
        return ((x * 4 + y) * 4 + z) * TWO + core

    def flipped(*dims):
        at = dict(pos)
        for d in dims:
            o = pos[d[0]]
            at[d[0]] = 3 - o if d.endswith("1") else o + 1 - TWO * mod(o, 2)
        return device(**at, core=c)

    bits = [gray(pos[d[0]], d) for d in ORDER]
    partners = [flipped(d) for d in ORDER]
    near = [_flips(p) for p in range(PARTS)]
    across = {dims: flipped(*dims) for dims in dict.fromkeys(d for ds in near for d in ds)}
    rot = [rotl(base_of(**pos), p) for p in range(PARTS)]

    def group_dev(j):
        return device(pos["x"], pos["y"], div(j, 2), mod(j, 2))

    def rcopy(src, dst, ss, rs, dev):
        return pltpu.make_async_remote_copy(src_ref=src, dst_ref=dst, send_sem=ss, recv_sem=rs, device_id={"dp": dev}, device_id_type=MESH)

    def signal(sem, dev):
        pl.semaphore_signal(sem, inc=1, device_id={"dp": dev}, device_id_type=MESH)

    copy = pltpu.make_async_copy

    barrier = pltpu.get_barrier_semaphore()
    for r in range(1, GROUP):
        signal(barrier, group_dev(mod(j_me + r, GROUP)))
    far = [q for dims, q in across.items() if dims not in (("z1",), ("z0",))]
    for q in far:
        signal(barrier, q)

    def weights(layer, i, b, gate_up=True, down=True):
        o = pl.ds(off_of(i), TILE)
        some = [copy(w_down.at[layer, o], wdb.at[b], wsem.at[b, 2])] if down else []
        if not gate_up:
            return some
        return some + [copy(w.at[layer, :, o], wgu.at[b, :, pl.ds(TILE * k, TILE)], wsem.at[b, k]) for k, w in enumerate((w_gate, w_up))]

    def saved(i, b):
        return weights(0, i, b, False) + [copy(gu0.at[i], da.at[pl.ds(b * TWO * TB, TWO * TB)], gsem.at[b])]

    def stream(make, i, b):
        for cp in make(i, b):
            cp.wait()

        @pl.when(i + 1 < TILES)
        def _():
            for cp in make(i + 1, ONE - b):
                cp.start()

    def as_blocks(v):
        return v.reshape(v.shape[0] // ROWS, ROWS, LANES)

    def get_da(q, rows, n):
        at_row = rows // ROWS if isinstance(rows, int) else div(rows, ROWS)
        return da[pl.ds(q * CHIPS + at_row, n // ROWS)].reshape(n, LANES)

    def sigmoid(v):
        return 1.0 / (1.0 + jnp.exp(-v))

    def through_act(gate, up, dhid):
        sg = sigmoid(gate)
        s = gate * sg
        return s, dhid * up * (sg * (1.0 + gate * (1.0 - sg))), dhid * s

    def counts(i):
        return (lax.broadcasted_iota(jnp.int32, (TOK, TILE), 1) < LANES) | (i > 0)

    def add_product(t):
        for q in range(OCT):
            o = pl.ds(q * CHIPS, CHIPS)
            da[o] = da[o] + as_blocks(t[:, lanes(q)])

    def hid_write(layer, i, b, q):
        o = pl.multiple_of(off_of(i) + LANES * q, LANES)
        return copy(hts.at[b, lanes(q)], hidt.at[layer, pl.ds(o, LANES)], hsem.at[b, q])

    def put_hidden(layer, i, b):
        for q in range(TWO):

            @pl.when(i >= 2 + q)
            def _():
                hid_write(layer, i - 2, b, q).wait()

        hts[b] = hidb[...].T
        for q in range(TWO):

            @pl.when(i >= q)
            def _():
                hid_write(layer, i, b, q).start()

    def hidden_out(layer):
        for i in (TILES - 2, TILES - 1):
            for q in range(TWO):
                hid_write(layer, i, i % TWO, q).wait()

    def gu_out(i, b):
        return copy(acc.at[pl.ds(b * TWO * TB, TWO * TB)], gu0.at[i], gsem.at[b])

    def tick_f(i):
        b = mod(i, 2)
        stream(functools.partial(weights, 0), i, b)

        @pl.when(i >= 2)
        def _():
            gu_out(i - 2, b).wait()

        gu = dot(acts[1], wgu[b])
        gate, up = gu[:, :TILE], gu[:, TILE:]
        hidb[...] = jnp.where(counts(i), gate * sigmoid(gate) * up, 0.0).astype(BF)
        for q in range(4):
            acc[pl.ds(TWO * b * TB + q * CHIPS, CHIPS)] = as_blocks(gu[:, lanes(q)])
        gu_out(i, b).start()
        add_product(dot(hidb[...], wdb[b]))
        put_hidden(0, i, b)

    def transpose_in():
        def part(k, _):
            t = acts[1, :, aligned(k * LANES, LANES)].T
            for q in range(OCT):
                n = k * OCT + q
                at[aligned(base_of(div(n, 16), mod(div(n, 4), 4), mod(n, 4)) * ROWS, ROWS)] = t[q * ROWS : (q + 1) * ROWS]
            return 0

        loop(D // LANES, part)

    def by_rows(fn):
        def chunk(k, _):
            fn(k * LANES, aligned(k * LANES, LANES))
            return 0

        loop(TOK // LANES, chunk)

    def norm_in(_, rows):
        h = acts[2, rows].astype(F32)
        acts[1, rows] = (h * rms_scale(jnp.sum(h * h, -1, keepdims=True))).astype(BF)

    def tick_fn():
        for b in range(TWO):
            gu_out(TILES - 2 + (b + TILES) % TWO, b).wait()

        def chunk(r, rows):
            o = jnp.concatenate([get_da(q, r, LANES) for q in range(OCT)], 1).astype(BF).astype(F32)
            acts[2, rows] = (acts[2, rows].astype(F32) + o).astype(BF)
            for q in range(OCT):
                da[pl.ds(q * CHIPS + div(r, ROWS), OCT)] = jnp.zeros((OCT, ROWS, LANES), F32)
            norm_in(r, rows)

        by_rows(chunk)
        a0t_out.wait()
        transpose_in()
        hidden_out(0)

    def dgu_out(i, b):
        return copy(dgu.at[b], dgh.at[i], dsem.at[b])

    def tick_a(i):
        b = mod(i, 2)
        stream(functools.partial(weights, 1), i, b)

        @pl.when(i >= 2)
        def _():
            dgu_out(i - 2, b).wait()


        gu = dot(acts[1], wgu[b])
        gate, up = gu[:, :TILE], gu[:, TILE:]
        dhid = dot(acts[0], wdb[b], 1).astype(BF).astype(F32)
        s, dgate, dup = through_act(gate, up, dhid)
        hidb[...] = (s * up).astype(BF)
        dgu[b, :, :TILE] = jnp.where(counts(i), dgate, 0.0).astype(BF)
        dgu[b, :, TILE:] = jnp.where(counts(i), dup, 0.0).astype(BF)

    def grads_gate_up(i, slot, layer, cuts):
        first = i == 0
        part = slot * PARTS + TWO * mod(i + 2, 3)
        pa = jnp.where(first, OWN_SLOTS * PARTS + TWO * layer, part)
        pb = jnp.where(first, slot * PARTS, part + 1)
        n = D // cuts

        def chunk(k, _):
            r = dot(at[aligned(k * n, n)], dgu[mod(i, 2)]).astype(BF)
            for q in range(4):
                own[q // TWO, pb if q % TWO else pa, pl.ds(k * (n // ROWS), n // ROWS)] = as_blocks(r[:, lanes(q)])
            return 0

        if cuts == 1:
            chunk(0, 0)
        else:
            loop(cuts, chunk)

    def wave_in_layer(i):
        return div(jnp.maximum(i - 1, 0), 3)

    def tick_b(i):
        b = mod(i, 2)
        grads_gate_up(i, mod(wave_in_layer(i), 3), 1, 1)
        dgu_out(i, b).start()
        put_hidden(1, i, b)

    def da_loads(i, b):
        return weights(1, i, b, down=False) + [copy(dgh.at[i], dgu.at[b], dsem.at[b])]

    def tick_da(k):
        def iteration(i, _):
            b = mod(i, 2)
            stream(da_loads, i, b)
            add_product(dot(dgu[b], wgu[b], 1))
            return 0

        lax.fori_loop(TWO * k, jnp.minimum(TWO * k + 2, TILES), iteration, 0)

    def hid_load(layer, r):
        return copy(hidt.at[layer, aligned(PAIR * r, PAIR, ROWS)], htb.at[mod(r, 2)], htsem.at[mod(r, 2)])

    def tick_down(k, layer):
        def iteration(r, _):
            hid_load(layer, r).wait()

            @pl.when(r + 1 < OCT)
            def _():
                hid_load(layer, r + 1).start()

            slots = [jnp.where(layer == 1, OWN_SLOT[D1 + q], OWN_SLOT[D0 + q]) * PARTS for q in range(TWO)]
            res = dot(htb[mod(r, 2)], acts[ONE - layer])
            for gg in range(TWO):
                g = TWO * r + gg
                at_xy = base_of(div(g, 4), mod(g, 4), 0)
                for lt in range(OCT):
                    place = at_xy + base_of(0, 0, lt % 4)
                    mine = res[gg * ROWS_GROUP : (gg + 1) * ROWS_GROUP, lanes(lt)]
                    for u in range(UNITS):
                        own[lt // 4, slots[u // PARTS] + u % PARTS, place] = mine[ROWS * u : ROWS * u + ROWS].astype(BF)
                    last = jnp.concatenate([mine[ROWS * UNITS :], jnp.zeros((OCT, LANES), F32)], 0)
                    own[lt // 4, OWN_SLOTS * PARTS + TWO * layer + 1, place] = last.astype(BF)
            return 0

        lax.fori_loop(TWO * k, TWO * k + 2, iteration, 0)

    def tick_norm():
        def chunk(r, rows):
            h = acts[2, rows].astype(F32)
            g = jnp.concatenate([get_da(q, r, LANES) for q in range(OCT)], 1).astype(BF).astype(F32)
            scale = rms_scale(jnp.sum(h * h, -1, keepdims=True))
            back = scale * scale * scale * jnp.sum(h * g, -1, keepdims=True) * (1.0 / D)
            dh = (g * scale - h * back).astype(BF).astype(F32)
            acts[1, rows] = (acts[0, rows].astype(F32) + dh).astype(BF)

        by_rows(chunk)

    def tick_back0(i):
        b = mod(i, 2)
        stream(saved, i, b)

        def chunk(k, _):
            n = TOK // TWO
            rows = aligned(k * n, n)
            dhid = dot(acts[1, rows], wdb[b], 1).astype(BF).astype(F32)
            gate, up = (jnp.concatenate([get_da(4 * b + TWO * m + q, k * n, n) for q in range(TWO)], 1) for m in range(TWO))
            _, dgate, dup = through_act(gate, up, dhid)
            dgu[b, rows, :TILE] = dgate.astype(BF)
            dgu[b, rows, TILE:] = dup.astype(BF)
            return 0

        loop(2, chunk)
        grads_gate_up(i, pick(wave_in_layer(i), OWN_SLOT[G0:]), 0, 2)

    a0t_out = copy(at, a0t, lsem.at[0])
    a0t_in = copy(a0t, at, lsem.at[0])

    def compute(t):
        def between(lo, hi, fn):
            @pl.when((t >= lo) & (t < hi))
            def _():
                fn(t - lo)

        between(T_F, T_FN, tick_f)

        @pl.when(t == T_FN)
        def _():
            for cp in weights(1, 0, 0):
                cp.start()
            tick_fn()
            loads[1].wait()

        @pl.when((t >= T_L1) & (t < T_DOWN1) & (mod(t, 2) == T_L1 % TWO))
        def _():
            tick_a(div(t - T_L1, 2))

        @pl.when((t >= T_L1) & (t < T_DOWN1) & (mod(t, 2) != T_L1 % TWO))
        def _():
            tick_b(div(t - T_L1, 2))

        @pl.when(t == T_DOWN1 - 1)
        def _():
            hid_load(1, 0).start()
            a0t_in.start()

        @pl.when(t == T_DOWN1)
        def _():
            hidden_out(1)
            for i in (TILES - 2, TILES - 1):
                dgu_out(i, i % TWO).wait()
            for cp in da_loads(0, 0):
                cp.start()

        @pl.when(((t >= T_DOWN1) & (t < T_DA)) | ((t >= T_DOWN0) & (t < T_B0)))
        def _():
            layer = jnp.where(t < T_NORM, 1, 0)
            tick_down(t - jnp.where(t < T_NORM, T_DOWN1, T_DOWN0), layer)

        between(T_DA, T_NORM, tick_da)

        @pl.when(t == T_NORM)
        def _():
            hid_load(0, 0).start()
            tick_norm()
            for cp in saved(0, 0):
                cp.start()
            a0t_in.wait()

        between(T_B0, T_TAIL, tick_back0)

    def L(j):
        return 2 ** (PARTS - j)

    starts = [[div(r, L(j)) * L(j) for j in range(PARTS + 1)] for r in rot]

    def kept(p, j):
        return starts[p][j]

    def lag_start(makers):
        last = None
        for make in makers:
            cp = make()
            if last is not None:
                last.start()
            last = cp
        last.start()

    class Full:
        parts = tuple(range(PARTS))
        accumulated, received, sent, crossed, ag_ref = acc, (None, r1, r2, r3, r4), (None, s1, s2, s3, s4), d2d, ag

        def __init__(self, w):
            self.w, self.id, self.r, self.s, self.f = w, w, mod(w, NRS), mod(w, NDD), mod(w, NX)
            self.own = pick(w, OWN_SLOT) * PARTS

    class Short:
        parts = SHORT
        accumulated, received, sent, crossed, ag_ref = accm, (None, q1, q2, q3, q4), (None, t1, t2, t3, t4), d2dm, agm

        def __init__(self, w):
            self.w, self.id, self.r, self.s, self.f = w, NW + w, w, w, NX + w
            self.own = OWN_SLOTS * PARTS + TWO * w

    def sems(v):
        return (v.r, v.s) if isinstance(v, Full) else (NRS + v.r, NDD + v.s)

    def crossing(v):
        s = sems(v)[1]
        return rcopy(own.at[ONE - c, pl.ds(v.own, len(v.parts))], v.crossed.at[v.s], d2s.at[s], d2r.at[s], other)

    def stage_all(v, j):
        s = sems(v)[0]
        return rcopy(v.sent[j].at[v.r], v.received[j].at[v.r], ssem.at[s, j - ONE], rsem.at[s, j - ONE], other)

    def stage_one(v, j, k):
        s = sems(v)[0]
        to = partners[(v.parts[k] + j - ONE) % PARTS]
        return rcopy(v.sent[j].at[v.r, k], v.received[j].at[v.r, k], ssem.at[s, j - ONE], rsem.at[s, j - ONE], to)

    def acc_at(v, k):
        return (v.r * len(v.parts) + k) * HALF

    def rs0(v):
        if isinstance(v, Full):

            @pl.when(v.w >= NDD)
            def _():
                pl.semaphore_wait(d2c.at[v.s], 1)

        crossing(v).start()

    def rs1(v):
        crossing(v).wait_recv()
        if isinstance(v, Full):

            @pl.when(v.w >= NRS)
            def _():
                pl.semaphore_wait(rcred.at[v.r], len(partners))

        def make(k):
            p = v.parts[k]
            b = bits[p]
            lv, kp = (ONE - b) * TWO ** (PARTS - ONE - p), b * TWO ** (PARTS - ONE - p)
            def some(g, _):
                at_g = rotr(g * RUN, p)
                for i in range(RUN):
                    u = at_g + rotr(i, p)
                    both = [own[c, v.own + k, o + u].astype(F32) + v.crossed[v.s, k, o + u].astype(F32) for o in (lv, kp)]
                    v.sent[1][v.r, k, g * RUN + i] = both[0].astype(BF)
                    v.accumulated[acc_at(v, k) + g * RUN + i] = both[1]
                return 0

            loop(HALF // RUN, some)
            return stage_one(v, 1, k)

        lag_start([functools.partial(make, k) for k in range(len(v.parts))])
        crossing(v).wait_send()
        if isinstance(v, Full):

            @pl.when(v.w + NDD < NW)
            def _():
                signal(d2c.at[v.s], other)

    def peer_block(p, e):
        r = 0
        for j, bit in zip((3, 4, 5), (4, 2, 1)):
            own_bit = bits[(p + j) % PARTS]
            r = TWO * r + (ONE - own_bit if e & bit else own_bit)
        return r

    def seven(v, ref):
        s = sems(v)[0]
        view = ref.at[v.r, :, pl.ds(0, OCT - 1)]
        return rcopy(view, view, ssem.at[s, 3], rsem.at[s, 3], other)

    def rs4(v):
        stage_all(v, 3).wait_recv()

        def make(k):
            p = v.parts[k]
            o = pl.ds(acc_at(v, k) + kept(p, 3) - kept(p, 1), OCT)
            total = v.accumulated[o] + v.received[3][v.r, k].astype(F32)
            v.accumulated[o] = total
            v.sent[4][v.r, k] = total.astype(BF)
            s = sems(v)[0]
            return [
                rcopy(v.sent[4].at[v.r, k, peer_block(p, e)], v.received[4].at[v.r, k, e - 1], ssem.at[s, 3], rsem.at[s, 3], across[near[p][e - 1]])
                for e in range(1, OCT)
            ]

        last = []
        for k in range(len(v.parts) + 1):
            made = make(k) if k < len(v.parts) else []
            for cp in last:
                cp.start()
            last = made

    def rsj(j, v):
        stage_all(v, j - ONE).wait_recv()
        n = L(j)
        ch = min(n, OCT)

        def make(k):
            p = v.parts[k]
            b = bits[(p + j - ONE) % PARTS]
            o = acc_at(v, k) + kept(p, j - ONE) - kept(p, 1)
            for i in range(0, n, ch):
                lv, kp = (ONE - b) * n + i, b * n + i
                both = [v.accumulated[pl.ds(o + h, ch)] + v.received[j - ONE][v.r, k, pl.ds(h, ch)].astype(F32) for h in (lv, kp)]
                v.sent[j][v.r, k, pl.ds(i, ch)] = both[0].astype(BF)
                v.accumulated[pl.ds(o + kp, ch)] = both[1]
            return stage_one(v, j, k)

        lag_start([functools.partial(make, k) for k in range(len(v.parts))])

    def is_down(w):
        return (w >= D1) & (w < G0)

    def exchange(v):
        return rcopy(gfin.at[v.f, ONE - c], xg.at[v.id], xs.at[v.f], xr.at[v.id], other)

    def rs5(v):
        seven(v, v.received[4]).wait_recv()
        for k, p in enumerate(v.parts):
            g = v.accumulated[acc_at(v, k) + rot[p] - kept(p, 1)]
            for e in range(OCT - 1):
                g = g + v.received[4][v.r, k, e].astype(F32)
            g = g.astype(BF).astype(F32)
            for h in range(TWO):
                gfin[v.f, h, k] = g[OCT * h : OCT * h + OCT]
        for j in range(1, 4):
            stage_all(v, j).wait_send()
        seven(v, v.sent[4]).wait_send()
        if isinstance(v, Short):
            g_d[v.w, ROWS * UNITS : ROWS * UNITS + OCT] = gfin[v.f, 0, 1]
            exchange(v).start()
            return

        @pl.when(v.w + NRS < NW)
        def _():
            for q in partners:
                signal(rcred.at[v.r], q)

        @pl.when(is_down(v.w))
        def _():
            for p in range(PARTS):
                for h in range(TWO):
                    g_d[jnp.where(v.w < D0, 1, 0), aligned((mod(v.w, 2) * PARTS + p) * ROWS + OCT * h, OCT)] = gfin[v.f, h, p]

        @pl.when(~is_down(v.w))
        def _():
            exchange(v).start()

    def adam_tile(layer, col, v, k):
        cols = aligned(col, LANES)
        mine, theirs = gfin[v.f, c, k], xg[v.id, k]
        for mat, (wr, om, ov) in enumerate(((wr_g, om_g, ov_g), (wr_u, om_u, ov_u))):
            g = jnp.where(c == mat, mine, theirs)
            wn, mn, vn = adam(wr[layer, :, cols].astype(F32), om[layer, :, cols], ov[layer, :, cols], g)
            om[layer, :, cols] = mn
            ov[layer, :, cols] = vn
            wsend[v.f, mat, k] = wn

    def w_exchange(v):
        return rcopy(wsend.at[v.f, ONE - c], wrecv.at[v.id], wsm.at[v.f], wrm.at[v.id], other)

    def rs6(v):
        exchange(v).wait_recv()
        if isinstance(v, Short):
            adam_tile(v.w, 0, v, 0)
            for mat in range(TWO):
                for k in range(1, PARTS):
                    wsend[v.f, mat, k] = jnp.zeros((OCT, LANES), F32)
        else:
            layer = jnp.where(v.w < G0, 1, 0)
            for k in range(PARTS):
                adam_tile(layer, LANES + PARTS * LANES * (v.w - jnp.where(v.w < G0, 0, G0)) + LANES * k, v, k)
        exchange(v).wait_send()
        w_exchange(v).start()

    def rs7(v):
        w_exchange(v).wait_recv()
        for k in range(PARTS if isinstance(v, Full) else 1):
            mine, theirs = wsend[v.f, c, k], wrecv[v.id, k]
            fin[v.id, k] = jnp.concatenate([jnp.where(c == 0, mine, theirs), jnp.where(c == 0, theirs, mine)], 0).astype(BF)
        w_exchange(v).wait_send()

    def window(j):
        return div(OWN_ROWS * j, OCT) * OCT

    def to_group(k, layer, src, dst):
        for r in range(1, GROUP):
            j = mod(j_me + r, GROUP)
            rcopy(src(j), dst.at[layer, j_me], dxs.at[k, layer], dxr.at[k, layer], group_dev(j)).start()

    def from_group(k, layer, dst):
        seven = dst.at[layer, pl.ds(0, GROUP - 1)]
        cp = rcopy(seven, seven, dxs.at[k, layer], dxr.at[k, layer], other)
        cp.wait_recv()
        cp.wait_send()

    def dx1(layer):
        def src(j):
            return g_d.at[layer, aligned(window(j), WIN, OCT)]

        to_group(0, layer, src, gx)

        def row(r, _):
            for o, t in ((om_d, md), (ov_d, vd)):
                o[layer, pl.ds(r, 1)] = t[r, pl.ds(layer, 1)]
            return 0

        loop(OWN_ROWS, row)
        gx[layer, j_me] = g_d[layer, aligned(window(j_me), WIN, OCT)]

    def dx2(layer):
        from_group(0, layer, gx)
        shift = mod(OWN_ROWS * j_me, OCT)
        row = lax.broadcasted_iota(jnp.int32, (WIN, LANES), 0)
        valid = (row >= shift) & (row < shift + OWN_ROWS)
        def tile(lt, _):
            cols = aligned(lt * LANES, LANES)
            m, s = (pltpu.roll(t[layer, :, cols], shift, 0) for t in (om_d, ov_d))
            wn, mn, vn = adam(wr_d[layer, :, cols].astype(F32), m, s, gx[layer, TWO * mod(lt, 4) + div(lt, 4)])
            for o, t in ((om_d, mn), (ov_d, vn)):
                o[layer, :, cols] = pltpu.roll(t, mod(WIN - shift, WIN), 0)
            ws_d[layer, lt] = jnp.where(valid, wn, 0.0)
            return 0

        loop(OCT, tile)

        def src(j):
            return ws_d.at[layer, 4 * mod(j, 2) + div(j, 2)]

        to_group(1, layer, src, wx)
        wx[layer, j_me] = ws_d[layer, 4 * c + pos["z"]]

    def dx3(layer):
        from_group(1, layer, wx)
        octets = [None] * (TWO * UNITS + 2)
        for j in range(GROUP):
            for k in range(WIN // OCT):
                o, t = window(j) // OCT + k, wx[layer, j, OCT * k : OCT * k + OCT]
                octets[o] = t if octets[o] is None else octets[o] + t
        octets[-1] = jnp.zeros((OCT, LANES), F32)
        for u in range(UNITS + 1):
            block = jnp.concatenate(octets[TWO * u : TWO * u + 2], 0).astype(BF)
            if u < UNITS:
                fin[jnp.where(layer == 1, D1, D0) + u // PARTS, u % PARTS] = block
            else:
                fin[NW + layer, 1] = block

    def part_of(v):
        return v.ag_ref.at[v.w, c]

    def ag1(v):
        for k, p in enumerate(v.parts):
            src, dst = fin.at[v.id, k], part_of(v).at[k, rot[p]]
            copy(src, dst, agl.at[v.id]).start()
            for dims in near[p]:
                rcopy(src, dst, ags.at[v.id], agr.at[v.id, 0], across[dims]).start()

    def agk(k, v):
        n = 2 ** (k - 2)
        mine = part_of(v)
        first = k == 4
        if first:
            copy(fin.at[v.id, pl.ds(0, len(v.parts))], mine.at[:, 0], agl.at[v.id]).wait()
        came = mine.at[:, pl.ds(0, OCT - 1 if first else n)]
        rcopy(came, came, ags.at[v.id], agr.at[v.id, 0 if first else k - 4], other).wait_recv()
        j = PARTS + ONE - k
        for q, p in enumerate(v.parts):
            if k <= PARTS:
                h = mine.at[q, pl.ds(kept(p, j), TWO * n)]
                rcopy(h, h, ags.at[v.id], agr.at[v.id, k - 3], partners[(p + j - ONE) % PARTS]).start()
            g = mine.at[q, pl.ds(kept(p, j), OCT) if first else pl.ds(kept(p, j) + (ONE - bits[(p + j) % PARTS]) * n, n)]
            rcopy(g, g, dags.at[v.id], dagr.at[v.id], other).start()

    def ag_end(v):
        most = part_of(v).at[:, pl.ds(0, CHIPS - 1)]
        rcopy(most, most, ags.at[v.id], agr.at[v.id, 0], other).wait_send()
        cp = rcopy(part_of(v), part_of(v), dags.at[v.id], dagr.at[v.id], other)
        cp.wait_send()
        cp.wait_recv()

    rs_stages = [rs0, rs1, functools.partial(rsj, 2), functools.partial(rsj, 3), rs4, rs5, rs6, rs7]
    ag_stages = [ag1] + [functools.partial(agk, k) for k in range(4, PARTS + 2)] + [ag_end]

    def find(t, due):
        terms = [jnp.where(t == s, w + 1, 0) for w, s in due]
        while len(terms) > 1:
            terms = [sum(terms[q : q + 2]) for q in range(0, len(terms), 2)]
        return terms[0]

    def within(t, due, fn):
        at = [s for _, s in due]
        pl.when((t >= min(at)) & (t <= max(at)))(fn)

    def run(t, kind, some):
        found = [(fn, find(t, due)) for fn, due in reversed(some)]

        @pl.when(sum(w for _, w in found) > 0)
        def _():
            for fn, w in found:

                @pl.when(w > 0)
                def _():
                    fn(kind(w - 1))

    def stages(fns, t, full, short):
        full = [[(w, at[s]) for w, at in enumerate(full) if not (fn in (rs6, rs7) and is_down(w))] for s, fn in enumerate(fns)]
        short = [[(w, at[s]) for w, at in enumerate(short)] for s in range(len(fns))]

        def full_ones():
            for odd in range(TWO):

                @pl.when(mod(t, 2) == odd)
                def _():
                    run(t, Full, [(fn, due) for fn, due in zip(fns, full) if due[0][1] % TWO == odd])

        within(t, sum(full, []), full_ones)
        within(t, sum(short, []), lambda: run(t, Short, list(zip(fns, short))))

    def moves(t):
        stages(rs_stages, t, RS_TICKS, SHORT_RS_TICKS)
        for q, fn in enumerate((dx1, dx2, dx3)):

            @pl.when((t == DX[0][q]) | (t == DX[1][q]))
            def _():
                fn(jnp.where(t == DX[1][q], 1, 0))

        stages(ag_stages, t, AG_TICKS, SHORT_AG_TICKS)

    loads = [copy(x, acts.at[2], lsem.at[1]), copy(dy, acts.at[0], lsem.at[2])]
    rows_in = [copy(w.at[:, aligned(dp * OCT, OCT)], o, lsem.at[3 + k]) for k, (w, o) in enumerate(((w_gate, wr_g), (w_up, wr_u)))]
    rows_in.append(copy(w_down.at[:, aligned(div(OWN_ROWS * dp, OCT) * OCT, WIN, OCT)], wr_d, lsem.at[5]))
    moments = ((m_g, om_g), (m_u, om_u), (m_d, md), (v_g, ov_g), (v_u, ov_u), (v_d, vd))
    rows_in += [copy(m, o, lsem.at[6 + k]) for k, (m, o) in enumerate(moments)]
    for cp in loads + weights(0, 0, 0) + rows_in:
        cp.start()
    for q in range(OCT):
        da[pl.ds(q * CHIPS, CHIPS)] = jnp.zeros((CHIPS, ROWS, LANES), F32)
    loads[0].wait()
    by_rows(norm_in)
    transpose_in()
    a0t_out.start()
    for cp in rows_in:
        cp.wait()
    pl.semaphore_wait(barrier, GROUP - 1 + len(far))

    def tick(t, _):
        pl.when(t < T_TAIL)(lambda: compute(t))
        moves(t)
        return 0

    loop(TICKS, tick)


def step_call(args):
    B = (ROWS, LANES)
    V, R, S = pltpu.VMEM, pltpu.SemaphoreType.REGULAR, pltpu.SemaphoreType.DMA
    sizes = [HALF, HALF // TWO, OCT, OCT]
    n, ns = NW + NS, len(SHORT)
    own_parts = OWN_SLOTS * PARTS + NS * ns
    E = (PARTS, OCT, LANES)
    scratch = [
        V((3, TOK, D), BF), V((D, TOK), BF), V((4 * TB, *B), F32), V((TWO, D, TWO * TILE), BF), V((TWO, TILE, D), BF),
        V((TWO, TOK, TWO * TILE), BF), V((TOK, TILE), BF), V((TWO, TILE, TOK), BF), V((TWO, PAIR, TOK), BF),
        *[V((LAYERS, OCT, FF), BF)] * TWO, V((LAYERS, WIN, D), BF), *[V((OWN_ROWS, LAYERS, D), F32)] * TWO,
        V((TWO, own_parts, CHIPS, *B), BF), V((NDD, PARTS, CHIPS, *B), BF), V((NRS * PARTS * HALF, *B), F32),
        *[V((NRS, PARTS, k, *B), BF) for k in sizes * TWO],
        V((NS, ns, CHIPS, *B), BF), V((NS * ns * HALF, *B), F32),
        *[V((NS, ns, k, *B), BF) for k in sizes * TWO],
        V((NX + NS, TWO, *E), F32), V((n, *E), F32), V((NX + NS, TWO, *E), F32), V((n, *E), F32), V((n, PARTS, *B), BF),
        V((LAYERS, ROWS * (UNITS + 1), LANES), F32), *[V((LAYERS, GROUP, WIN, LANES), F32)] * 3,
        S((12,)), S((TWO, 3)), S((TWO,)), S((TWO,)), S((TWO, 2)), S((TWO,)), S((NDD + NS,)), S((NDD + NS,)), S((NRS + NS, PARTS)), S((NRS + NS, PARTS)),
        S((NX + NS,)), S((n,)), S((NX + NS,)), S((n,)), S((n,)), S((n,)), S((n, PARTS)), S((n,)), S((n,)), S((TWO, LAYERS)), S((TWO, LAYERS)),
        R((NDD,)), R((NRS,)),
    ]
    hbm, vmem = pl.BlockSpec(memory_space=pl.ANY), pl.BlockSpec(memory_space=pltpu.VMEM)
    out = [((NW, TWO, PARTS, CHIPS, *B), BF), ((NS, 2, ns, CHIPS, *B), BF), ((LAYERS, FF, TOK), BF), ((D, TOK), BF), ((TILES, TWO * TB, *B), F32), ((TILES, TOK, TWO * TILE), BF)]
    out += [(s, F32) for s in ((LAYERS, OCT, FF), (LAYERS, OCT, FF), (LAYERS, WIN, D))] * TWO
    return pl.pallas_call(
        step_kernel,
        out_shape=[jax.ShapeDtypeStruct(*o) for o in out],
        in_specs=[hbm] * 11,
        out_specs=[hbm] * 6 + [vmem] * 6,
        scratch_shapes=scratch,
        compiler_params=pltpu.CompilerParams(collective_id=0, has_side_effects=True, vmem_limit_bytes=67043328),
        name="step",
    )(*args)


def place_kernel(
    ag, agm, om_g, om_u, om_d, ov_g, ov_u, ov_d, gate, up, down, pm_g, pm_u, pm_d, pv_g, pv_u, pv_d, buf, dbuf, mbuf, stage, mstage, dstage,
    isem, dsem, msem, osem, mosem, dosem,
):
    copy = pltpu.make_async_copy
    jobs = G0
    outs = (gate, up)

    def load(k):
        return copy(ag.at[jnp.where(k < D1, k, k + D1)], buf.at[mod(k, DEEP)], isem.at[mod(k, DEEP)])

    def stores(k):
        cols = aligned(LANES + PARTS * LANES * mod(k, 4), PARTS * LANES, LANES)
        return [copy(stage.at[mod(k, 2), m], o.at[jnp.where(k < D1, 1, 0), :, cols], osem.at[mod(k, 2), m]) for m, o in enumerate(outs)]

    def load_down(layer):
        return copy(ag.at[pl.ds(pick(layer, (D0, D1)), 2)], dbuf.at[layer], dsem.at[layer])

    def store_down(k):
        rows = aligned(mod(k, 4) * TWO * PAIR, TWO * PAIR, ROWS)
        return copy(dstage.at[mod(k, 2)], down.at[jnp.where(k < D1, 1, 0), rows], dosem.at[mod(k, 2)])

    def store_short(layer, m):
        return copy(mstage.at[layer, m], outs[m].at[layer, :, lanes(0)], mosem.at[layer, m])

    mini = copy(agm, mbuf, msem.at[0])
    for cp in (load(0), load(1), load_down(1), mini, load(2), load_down(0)):
        cp.start()

    def by_chip(dst, cols, src, p):
        for u in range(CHIPS):
            n = CHIP_AT[u]
            dst[ROWS * n : ROWS * n + ROWS, cols] = src[rotl(u, p)]

    def body(k, _):
        @pl.when(k < jobs)
        def _():
            load(k).wait()

            @pl.when(k >= 2)
            def _():
                for cp in stores(k - 2):
                    cp.wait()

            for m in range(TWO):
                for p in range(PARTS):
                    by_chip(stage.at[mod(k, 2), m], lanes(p), buf.at[mod(k, DEEP), m, p], p)
            for cp in stores(k):
                cp.start()

            @pl.when(k + DEEP < jobs)
            def _():
                load(k + DEEP).start()

        @pl.when(k >= 1)
        def _():
            down_job(k - ONE)

        return 0

    def down_job(k):
        layer = jnp.where(k < D1, 1, 0)

        @pl.when(k == 0)
        def _():
            mini.wait()
            for layer in range(LAYERS):
                for m in range(TWO):
                    by_chip(mstage.at[layer, m], lanes(0), mbuf.at[layer, m, 0], SHORT[0])
                    store_short(layer, m).start()

        @pl.when(mod(k, 4) == 0)
        def _():
            load_down(layer).wait()

        @pl.when(k >= 2)
        def _():
            store_down(k - 2).wait()

        def pair(q, _):
            for lt in range(OCT):
                h = lt // 4
                octets = []
                for gg in range(TWO):
                    g = (mod(k, 4) * TWO + q) * TWO + gg
                    spot = base_of(div(g, 4), mod(g, 4), 0) + base_of(0, 0, lt % 4)
                    for u in range(UNITS + 1):
                        if u < UNITS:
                            t = dbuf[layer, u // PARTS, h, u % PARTS, rotl(spot, u % PARTS)].astype(F32)
                        else:
                            t = mbuf[layer, h, 1, rotl(spot, SHORT[1])].astype(F32)[:OCT]
                        octets.append(t)
                dstage[mod(k, 2), aligned(PAIR * q, PAIR, ROWS), lanes(lt)] = jnp.concatenate(octets, 0).astype(BF)
            return 0

        loop(2, pair)
        store_down(k).start()

        @pl.when(k == jobs - 1)
        def _():
            for o, t in ((pm_g, om_g), (pm_u, om_u), (pv_g, ov_g), (pv_u, ov_u)):
                o[...] = t[...]
            for o, t in ((pm_d, om_d), (pv_d, ov_d)):
                for layer in range(LAYERS):
                    for r in range(OWN_ROWS):
                        o[r, layer : layer + 1] = t[layer, r : r + 1]

    loop(jobs + 1, body)
    for k in (jobs - 2, jobs - 1):
        for cp in stores(k) + [store_down(k)]:
            cp.wait()
    for layer in range(LAYERS):
        for m in range(TWO):
            store_short(layer, m).wait()


def place_call(args):
    hbm, vmem = pl.BlockSpec(memory_space=pl.ANY), pl.BlockSpec(memory_space=pltpu.VMEM)
    V, S = pltpu.VMEM, pltpu.SemaphoreType.DMA
    whole = (TWO, PARTS, CHIPS, ROWS, LANES)
    out = [(s, BF) for s in ((LAYERS, D, FF), (LAYERS, D, FF), (LAYERS, FF, D))]
    out += [(s, F32) for s in ((LAYERS, OCT, FF), (LAYERS, OCT, FF), (OWN_ROWS, LAYERS, D))] * TWO
    return pl.pallas_call(
        place_kernel,
        out_shape=[jax.ShapeDtypeStruct(*o) for o in out],
        in_specs=[hbm] * TWO + [vmem] * 6,
        out_specs=[hbm] * 3 + [vmem] * 6,
        scratch_shapes=[
            V((DEEP, *whole), BF), V((LAYERS, TWO, *whole), BF), V((NS, 2, len(SHORT), CHIPS, ROWS, LANES), BF),
            V((TWO, TWO, D, PARTS * LANES), BF), V((LAYERS, TWO, D, LANES), BF), V((TWO, TWO * PAIR, D), BF),
            S((DEEP,)), S((TWO,)), S((1,)), S((TWO, 2)), S((TWO, 2)), S((TWO,)),
        ],
        compiler_params=pltpu.CompilerParams(vmem_limit_bytes=60 * TWO**20),
        name="place",
    )(*args)


def local_step(x, dy, w_gate, w_up, w_down, m_g, m_u, m_d, v_g, v_u, v_d):
    m_d, v_d = (jnp.transpose(t, (1, 0, 2)) for t in (m_d, v_d))
    ag, agm, _, _, _, _, *moments = step_call((x[0], dy[0], w_gate, w_up, w_down, m_g, m_u, m_d, v_g, v_u, v_d))
    gate, up, down, om_g, om_u, om_d, ov_g, ov_u, ov_d = place_call((ag, agm, *moments))
    om_d, ov_d = (jnp.transpose(t, (1, 0, 2)) for t in (om_d, ov_d))
    return gate, up, down, om_g, om_u, om_d, ov_g, ov_u, ov_d


def solution(mesh):
    moment = P(None, "dp", None)
    return jax.shard_map(
        local_step,
        mesh=mesh,
        in_specs=(P(("rep", "dp")), P(("rep", "dp")), P(), P(), P(), *[moment] * 6),
        out_specs=(P("rep"), P("rep"), P("rep"), *[P("rep", "dp", None)] * 6),
        check_vma=False,
    )
```

```python
import functools
from itertools import accumulate

import jax
import jax.numpy as jnp
from jax import lax
from jax.experimental import pallas as pl
from jax.experimental.pallas import tpu as pltpu
from jax.sharding import PartitionSpec as P

MESH = pl.DeviceIdType.MESH
ONE, TWO = 1, 2
BF, F32 = jnp.bfloat16, jnp.float32
LAYERS, D, FF, TOK = 2, 1024, 3200, 1024
LANES, ROWS, OCT = 128, 16, 8
PARTS, CHIPS, HALF = 6, 64, 32
TILE, TILES = 256, 13
TB = 2 * CHIPS
ORDER = ("x1", "y1", "z1", "x0", "y0", "z0")
GROUP, GROUPS, ROWS_GROUP = 8, 16, 200
PAIR = 2 * ROWS_GROUP
UNITS = ROWS_GROUP // ROWS
OWN_ROWS = ROWS_GROUP // GROUP
WIN = 32
RUN = 32
DEEP = 3

G1, D1, D0, G0, NW = 0, 4, 6, 8, 12
SHORT = (0, 3)
NS = 2
OWN_SLOT = (0, 1, 2, 0, 1, 2, 0, 3, 2, 0, 1, 2)
OWN_SLOTS = 4
NRS, NDD, NX = 3, 2, 4

T_F, T_FN, T_L1, T_DOWN1, T_DA, T_NORM, T_DOWN0, T_B0, T_TAIL = 0, 13, 14, 40, 44, 51, 52, 56, 69


def ticks(codes):
    return tuple(tuple(accumulate((ord(ch) - ord("0") for ch in code), initial=18))[1:] for code in codes)


RS_TICKS = ticks(('34322411', '94322211', '?4322211', 'E2322411', 'I2322211', 'K2322211', 'U2322211', 'W2322211', 'Y2324411', ']4344211', '_4542411', 'c6342411'))
SHORT_RS_TICKS = ticks(('V2321211', 'I2322212'))
AG_TICKS = ticks(('D23234', 'H23432', 'N43254', 'T23432', '\\23452', '^45634', 'n47674', 'l43652', 'j43454', 'p43654', 't45654', 'x45454'))
SHORT_AG_TICKS = ticks(('l23441', ']25551'))
DX = ticks(('b64', 'V33'))
TICKS = max(max(t) for t in AG_TICKS + SHORT_AG_TICKS) + 1


def div(a, b):
    return a // b if isinstance(a, int) else lax.div(a, jnp.int32(b))


def mod(a, b):
    return a % b if isinstance(a, int) else lax.rem(a, jnp.int32(b))


def loop(n, fn):
    lax.fori_loop(0, n, fn, 0)


def base_of(x, y, z):
    r = 0
    for d in ORDER:
        v = {"x": x, "y": y, "z": z}[d[0]]
        r = TWO * r + gray(v, d)
    return r


def gray(v, d):
    h, l = div(v, 2), mod(v, 2)
    return h if d.endswith("1") else h + l - TWO * h * l


CHIP_AT = [None] * CHIPS
for _n in range(CHIPS):
    CHIP_AT[base_of(_n // 16, _n // 4 % 4, _n % 4)] = _n


def rotl(u, p):
    return mod(u * TWO**p, CHIPS) + div(u * TWO**p, CHIPS)


def rotr(u, p):
    return rotl(u, (PARTS - p) % PARTS)


def _flips(p):
    dims = [ORDER[(p + j) % PARTS] for j in (3, 4, 5)]
    return [tuple(d for d, bit in zip(dims, (4, 2, 1)) if e & bit) for e in range(1, OCT)]


def off_of(i):
    return pl.multiple_of(jnp.maximum(TILE * i - LANES, 0), LANES)


def aligned(start, size, to=None):
    return pl.ds(pl.multiple_of(start, to or size), size)


def dot(a, b, cb=0):
    return lax.dot_general(a, b, (((1,), (cb,)), ((), ())), preferred_element_type=F32)


def pick(w, values):
    r = values[0]
    for q, v in enumerate(values):
        if q:
            r = jnp.where(w == q, v, r)
    return r


def adam(w, m, v, g):
    m = 0.9 * m + 0.1 * g
    v = 0.95 * v + 0.05 * g * g
    step = m * lax.rsqrt(v + 1e-8) + 0.1 * w
    return (w - 0.02 * step).astype(BF).astype(F32), m, v


def rms_scale(squares):
    return lax.rsqrt(squares * (1.0 / D) + 1e-6)


def lanes(q):
    return slice(LANES * q, LANES * q + LANES)


def step_kernel(
    x, dy, w_gate, w_up, w_down, m_g, m_u, m_d, v_g, v_u, v_d,
    ag, agm, hidt, a0t, gu0, dgh, om_g, om_u, om_d, ov_g, ov_u, ov_d,
    acts, at, da, wgu, wdb, dgu, hidb, hts, htb, wr_g, wr_u, wr_d, md, vd,
    own, d2d, acc, r1, r2, r3, r4, s1, s2, s3, s4,
    d2dm, accm, q1, q2, q3, q4, t1, t2, t3, t4,
    gfin, xg, wsend, wrecv, fin, g_d, gx, ws_d, wx,
    lsem, wsem, gsem, dsem, hsem, htsem, d2s, d2r, ssem, rsem, xs, xr, wsm, wrm, agl, ags, agr, dags, dagr, dxs, dxr, d2c, rcred,
):
    dp = lax.axis_index("dp")
    c = mod(dp, 2)
    pos = {"x": div(dp, 32), "y": mod(div(dp, 8), 4), "z": mod(div(dp, 2), 4)}
    other = dp + 1 - TWO * c
    j_me = pos["z"] * TWO + c

    def device(x, y, z, core):
        return ((x * 4 + y) * 4 + z) * TWO + core

    def flipped(*dims):
        at = dict(pos)
        for d in dims:
            o = pos[d[0]]
            at[d[0]] = 3 - o if d.endswith("1") else o + 1 - TWO * mod(o, 2)
        return device(**at, core=c)

    bits = [gray(pos[d[0]], d) for d in ORDER]
    partners = [flipped(d) for d in ORDER]
    near = [_flips(p) for p in range(PARTS)]
    across = {dims: flipped(*dims) for dims in dict.fromkeys(d for ds in near for d in ds)}
    rot = [rotl(base_of(**pos), p) for p in range(PARTS)]

    def group_dev(j):
        return device(pos["x"], pos["y"], div(j, 2), mod(j, 2))

    def rcopy(src, dst, ss, rs, dev):
        return pltpu.make_async_remote_copy(src_ref=src, dst_ref=dst, send_sem=ss, recv_sem=rs, device_id={"dp": dev}, device_id_type=MESH)

    def signal(sem, dev):
        pl.semaphore_signal(sem, inc=1, device_id={"dp": dev}, device_id_type=MESH)

    copy = pltpu.make_async_copy

    barrier = pltpu.get_barrier_semaphore()
    for r in range(1, GROUP):
        signal(barrier, group_dev(mod(j_me + r, GROUP)))
    far = [q for dims, q in across.items() if dims not in (("z1",), ("z0",))]
    for q in far:
        signal(barrier, q)

    def weights(layer, i, b, gate_up=True, down=True):
        o = pl.ds(off_of(i), TILE)
        some = [copy(w_down.at[layer, o], wdb.at[b], wsem.at[b, 2])] if down else []
        if not gate_up:
            return some
        return some + [copy(w.at[layer, :, o], wgu.at[b, :, pl.ds(TILE * k, TILE)], wsem.at[b, k]) for k, w in enumerate((w_gate, w_up))]

    def saved(i, b):
        return weights(0, i, b, False) + [copy(gu0.at[i], da.at[pl.ds(b * TWO * TB, TWO * TB)], gsem.at[b])]

    def stream(make, i, b):
        for cp in make(i, b):
            cp.wait()

        @pl.when(i + 1 < TILES)
        def _():
            for cp in make(i + 1, ONE - b):
                cp.start()

    def as_blocks(v):
        return v.reshape(v.shape[0] // ROWS, ROWS, LANES)

    def get_da(q, rows, n):
        at_row = rows // ROWS if isinstance(rows, int) else div(rows, ROWS)
        return da[pl.ds(q * CHIPS + at_row, n // ROWS)].reshape(n, LANES)

    def sigmoid(v):
        return 1.0 / (1.0 + jnp.exp(-v))

    def through_act(gate, up, dhid):
        sg = sigmoid(gate)
        s = gate * sg
        return s, dhid * up * (sg * (1.0 + gate * (1.0 - sg))), dhid * s

    def counts(i):
        return (lax.broadcasted_iota(jnp.int32, (TOK, TILE), 1) < LANES) | (i > 0)

    def add_product(t):
        for q in range(OCT):
            o = pl.ds(q * CHIPS, CHIPS)
            da[o] = da[o] + as_blocks(t[:, lanes(q)])

    def hid_write(layer, i, b, q):
        o = pl.multiple_of(off_of(i) + LANES * q, LANES)
        return copy(hts.at[b, lanes(q)], hidt.at[layer, pl.ds(o, LANES)], hsem.at[b, q])

    def put_hidden(layer, i, b):
        for q in range(TWO):

            @pl.when(i >= 2 + q)
            def _():
                hid_write(layer, i - 2, b, q).wait()

        hts[b] = hidb[...].T
        for q in range(TWO):

            @pl.when(i >= q)
            def _():
                hid_write(layer, i, b, q).start()

    def hidden_out(layer):
        for i in (TILES - 2, TILES - 1):
            for q in range(TWO):
                hid_write(layer, i, i % TWO, q).wait()

    def gu_out(i, b):
        return copy(acc.at[pl.ds(b * TWO * TB, TWO * TB)], gu0.at[i], gsem.at[b])

    def tick_f(i):
        b = mod(i, 2)
        stream(functools.partial(weights, 0), i, b)

        @pl.when(i >= 2)
        def _():
            gu_out(i - 2, b).wait()

        gu = dot(acts[1], wgu[b])
        gate, up = gu[:, :TILE], gu[:, TILE:]
        hidb[...] = jnp.where(counts(i), gate * sigmoid(gate) * up, 0.0).astype(BF)
        for q in range(4):
            acc[pl.ds(TWO * b * TB + q * CHIPS, CHIPS)] = as_blocks(gu[:, lanes(q)])
        gu_out(i, b).start()
        add_product(dot(hidb[...], wdb[b]))
        put_hidden(0, i, b)

    def transpose_in():
        def part(k, _):
            t = acts[1, :, aligned(k * LANES, LANES)].T
            for q in range(OCT):
                n = k * OCT + q
                at[aligned(base_of(div(n, 16), mod(div(n, 4), 4), mod(n, 4)) * ROWS, ROWS)] = t[q * ROWS : (q + 1) * ROWS]
            return 0

        loop(D // LANES, part)

    def by_rows(fn):
        def chunk(k, _):
            fn(k * TILE, aligned(k * TILE, TILE))
            return 0

        loop(TOK // TILE, chunk)

    def norm_in(_, rows):
        h = acts[2, rows].astype(F32)
        acts[1, rows] = (h * rms_scale(jnp.sum(h * h, -1, keepdims=True))).astype(BF)

    def tick_fn():
        for b in range(TWO):
            gu_out(TILES - 2 + (b + TILES) % TWO, b).wait()

        def chunk(r, rows):
            o = jnp.concatenate([get_da(q, r, TILE) for q in range(OCT)], 1).astype(BF).astype(F32)
            acts[2, rows] = (acts[2, rows].astype(F32) + o).astype(BF)
            for q in range(OCT):
                da[pl.ds(q * CHIPS + div(r, ROWS), ROWS)] = jnp.zeros((ROWS, ROWS, LANES), F32)
            norm_in(r, rows)

        by_rows(chunk)
        a0t_out.wait()
        transpose_in()
        hidden_out(0)

    def dgu_out(i, b):
        return copy(dgu.at[b], dgh.at[i], dsem.at[b])

    def tick_a(i):
        b = mod(i, 2)
        stream(functools.partial(weights, 1), i, b)

        @pl.when(i >= 2)
        def _():
            dgu_out(i - 2, b).wait()


        gu = dot(acts[1], wgu[b])
        gate, up = gu[:, :TILE], gu[:, TILE:]
        dhid = dot(acts[0], wdb[b], 1).astype(BF).astype(F32)
        s, dgate, dup = through_act(gate, up, dhid)
        hidb[...] = (s * up).astype(BF)
        dgu[b, :, :TILE] = jnp.where(counts(i), dgate, 0.0).astype(BF)
        dgu[b, :, TILE:] = jnp.where(counts(i), dup, 0.0).astype(BF)

    def grads_gate_up(i, slot, layer, cuts):
        first = i == 0
        part = slot * PARTS + TWO * mod(i + 2, 3)
        pa = jnp.where(first, OWN_SLOTS * PARTS + TWO * layer, part)
        pb = jnp.where(first, slot * PARTS, part + 1)
        n = D // cuts

        def chunk(k, _):
            r = dot(at[aligned(k * n, n)], dgu[mod(i, 2)]).astype(BF)
            for q in range(4):
                own[q // TWO, pb if q % TWO else pa, pl.ds(k * (n // ROWS), n // ROWS)] = as_blocks(r[:, lanes(q)])
            return 0

        if cuts == 1:
            chunk(0, 0)
        else:
            loop(cuts, chunk)

    def wave_in_layer(i):
        return div(jnp.maximum(i - 1, 0), 3)

    def tick_b(i):
        b = mod(i, 2)
        grads_gate_up(i, mod(wave_in_layer(i), 3), 1, 1)
        dgu_out(i, b).start()
        put_hidden(1, i, b)

    def da_loads(i, b):
        return weights(1, i, b, down=False) + [copy(dgh.at[i], dgu.at[b], dsem.at[b])]

    def tick_da(k):
        def iteration(i, _):
            b = mod(i, 2)
            stream(da_loads, i, b)
            add_product(dot(dgu[b], wgu[b], 1))
            return 0

        lax.fori_loop(TWO * k, jnp.minimum(TWO * k + 2, TILES), iteration, 0)

    def hid_load(layer, r):
        return copy(hidt.at[layer, aligned(PAIR * r, PAIR, ROWS)], htb.at[mod(r, 2)], htsem.at[mod(r, 2)])

    def tick_down(k, layer):
        def iteration(r, _):
            hid_load(layer, r).wait()

            @pl.when(r + 1 < OCT)
            def _():
                hid_load(layer, r + 1).start()

            slots = [jnp.where(layer == 1, OWN_SLOT[D1 + q], OWN_SLOT[D0 + q]) * PARTS for q in range(TWO)]
            res = dot(htb[mod(r, 2)], acts[ONE - layer])
            for gg in range(TWO):
                g = TWO * r + gg
                at_xy = base_of(div(g, 4), mod(g, 4), 0)
                for lt in range(OCT):
                    place = at_xy + base_of(0, 0, lt % 4)
                    mine = res[gg * ROWS_GROUP : (gg + 1) * ROWS_GROUP, lanes(lt)]
                    for u in range(UNITS):
                        own[lt // 4, slots[u // PARTS] + u % PARTS, place] = mine[ROWS * u : ROWS * u + ROWS].astype(BF)
                    last = jnp.concatenate([mine[ROWS * UNITS :], jnp.zeros((OCT, LANES), F32)], 0)
                    own[lt // 4, OWN_SLOTS * PARTS + TWO * layer + 1, place] = last.astype(BF)
            return 0

        lax.fori_loop(TWO * k, TWO * k + 2, iteration, 0)

    def tick_norm():
        def chunk(r, rows):
            h = acts[2, rows].astype(F32)
            g = jnp.concatenate([get_da(q, r, TILE) for q in range(OCT)], 1).astype(BF).astype(F32)
            scale = rms_scale(jnp.sum(h * h, -1, keepdims=True))
            back = scale * scale * scale * jnp.sum(h * g, -1, keepdims=True) * (1.0 / D)
            dh = (g * scale - h * back).astype(BF).astype(F32)
            acts[1, rows] = (acts[0, rows].astype(F32) + dh).astype(BF)

        by_rows(chunk)

    def tick_back0(i):
        b = mod(i, 2)
        stream(saved, i, b)

        def chunk(k, _):
            n = TOK // TWO
            rows = aligned(k * n, n)
            dhid = dot(acts[1, rows], wdb[b], 1).astype(BF).astype(F32)
            gate, up = (jnp.concatenate([get_da(4 * b + TWO * m + q, k * n, n) for q in range(TWO)], 1) for m in range(TWO))
            _, dgate, dup = through_act(gate, up, dhid)
            dgu[b, rows, :TILE] = dgate.astype(BF)
            dgu[b, rows, TILE:] = dup.astype(BF)
            return 0

        loop(2, chunk)
        grads_gate_up(i, pick(wave_in_layer(i), OWN_SLOT[G0:]), 0, 2)

    a0t_out = copy(at, a0t, lsem.at[0])
    a0t_in = copy(a0t, at, lsem.at[0])

    def compute(t):
        def between(lo, hi, fn):
            @pl.when((t >= lo) & (t < hi))
            def _():
                fn(t - lo)

        between(T_F, T_FN, tick_f)

        @pl.when(t == T_FN)
        def _():
            for cp in weights(1, 0, 0):
                cp.start()
            tick_fn()
            for cp in [loads[1], *rows_in]:
                cp.wait()

        @pl.when((t >= T_L1) & (t < T_DOWN1) & (mod(t, 2) == T_L1 % TWO))
        def _():
            tick_a(div(t - T_L1, 2))

        @pl.when((t >= T_L1) & (t < T_DOWN1) & (mod(t, 2) != T_L1 % TWO))
        def _():
            tick_b(div(t - T_L1, 2))

        @pl.when(t == T_DOWN1 - 1)
        def _():
            hid_load(1, 0).start()
            a0t_in.start()

        @pl.when(t == T_DOWN1)
        def _():
            hidden_out(1)
            for i in (TILES - 2, TILES - 1):
                dgu_out(i, i % TWO).wait()
            for cp in da_loads(0, 0):
                cp.start()

        @pl.when(((t >= T_DOWN1) & (t < T_DA)) | ((t >= T_DOWN0) & (t < T_B0)))
        def _():
            layer = jnp.where(t < T_NORM, 1, 0)
            tick_down(t - jnp.where(t < T_NORM, T_DOWN1, T_DOWN0), layer)

        between(T_DA, T_NORM, tick_da)

        @pl.when(t == T_NORM)
        def _():
            hid_load(0, 0).start()
            tick_norm()
            for cp in saved(0, 0):
                cp.start()
            a0t_in.wait()

        between(T_B0, T_TAIL, tick_back0)

    def L(j):
        return 2 ** (PARTS - j)

    starts = [[div(r, L(j)) * L(j) for j in range(PARTS + 1)] for r in rot]

    def kept(p, j):
        return starts[p][j]

    def lag_start(makers):
        last = None
        for make in makers:
            cp = make()
            if last is not None:
                last.start()
            last = cp
        last.start()

    class Full:
        parts = tuple(range(PARTS))
        accumulated, received, sent, crossed, ag_ref = acc, (None, r1, r2, r3, r4), (None, s1, s2, s3, s4), d2d, ag

        def __init__(self, w):
            self.w, self.id, self.r, self.s, self.f = w, w, mod(w, NRS), mod(w, NDD), mod(w, NX)
            self.own = pick(w, OWN_SLOT) * PARTS

    class Short:
        parts = SHORT
        accumulated, received, sent, crossed, ag_ref = accm, (None, q1, q2, q3, q4), (None, t1, t2, t3, t4), d2dm, agm

        def __init__(self, w):
            self.w, self.id, self.r, self.s, self.f = w, NW + w, w, w, NX + w
            self.own = OWN_SLOTS * PARTS + TWO * w

    def sems(v):
        return (v.r, v.s) if isinstance(v, Full) else (NRS + v.r, NDD + v.s)

    def crossing(v):
        s = sems(v)[1]
        return rcopy(own.at[ONE - c, pl.ds(v.own, len(v.parts))], v.crossed.at[v.s], d2s.at[s], d2r.at[s], other)

    def stage_all(v, j):
        s = sems(v)[0]
        return rcopy(v.sent[j].at[v.r], v.received[j].at[v.r], ssem.at[s, j - ONE], rsem.at[s, j - ONE], other)

    def stage_one(v, j, k):
        s = sems(v)[0]
        to = partners[(v.parts[k] + j - ONE) % PARTS]
        return rcopy(v.sent[j].at[v.r, k], v.received[j].at[v.r, k], ssem.at[s, j - ONE], rsem.at[s, j - ONE], to)

    def acc_at(v, k):
        return (v.r * len(v.parts) + k) * HALF

    def rs0(v):
        if isinstance(v, Full):

            @pl.when(v.w >= NDD)
            def _():
                pl.semaphore_wait(d2c.at[v.s], 1)

        crossing(v).start()

    def rs1(v):
        crossing(v).wait_recv()
        if isinstance(v, Full):

            @pl.when(v.w >= NRS)
            def _():
                pl.semaphore_wait(rcred.at[v.r], len(partners))

        def make(k):
            p = v.parts[k]
            b = bits[p]
            lv, kp = (ONE - b) * TWO ** (PARTS - ONE - p), b * TWO ** (PARTS - ONE - p)
            def some(g, _):
                at_g = rotr(g * RUN, p)
                for i in range(RUN):
                    u = at_g + rotr(i, p)
                    both = [own[c, v.own + k, o + u].astype(F32) + v.crossed[v.s, k, o + u].astype(F32) for o in (lv, kp)]
                    v.sent[1][v.r, k, g * RUN + i] = both[0].astype(BF)
                    v.accumulated[acc_at(v, k) + g * RUN + i] = both[1]
                return 0

            some(0, None)
            return stage_one(v, 1, k)

        lag_start([functools.partial(make, k) for k in range(len(v.parts))])
        crossing(v).wait_send()
        if isinstance(v, Full):

            @pl.when(v.w + NDD < NW)
            def _():
                signal(d2c.at[v.s], other)

    def peer_block(p, e):
        r = 0
        for j, bit in zip((3, 4, 5), (4, 2, 1)):
            own_bit = bits[(p + j) % PARTS]
            r = TWO * r + (ONE - own_bit if e & bit else own_bit)
        return r

    def seven(v, ref):
        s = sems(v)[0]
        view = ref.at[v.r, :, pl.ds(0, OCT - 1)]
        return rcopy(view, view, ssem.at[s, 3], rsem.at[s, 3], other)

    def rs4(v):
        stage_all(v, 3).wait_recv()

        def make(k):
            p = v.parts[k]
            o = pl.ds(acc_at(v, k) + kept(p, 3) - kept(p, 1), OCT)
            total = v.accumulated[o] + v.received[3][v.r, k].astype(F32)
            v.accumulated[o] = total
            v.sent[4][v.r, k] = total.astype(BF)
            s = sems(v)[0]
            return [
                rcopy(v.sent[4].at[v.r, k, peer_block(p, e)], v.received[4].at[v.r, k, e - 1], ssem.at[s, 3], rsem.at[s, 3], across[near[p][e - 1]])
                for e in range(1, OCT)
            ]

        last = []
        for k in range(len(v.parts) + 1):
            made = make(k) if k < len(v.parts) else []
            for cp in last:
                cp.start()
            last = made

    def rsj(j, v):
        stage_all(v, j - ONE).wait_recv()
        n = L(j)
        ch = min(n, OCT)

        def make(k):
            p = v.parts[k]
            b = bits[(p + j - ONE) % PARTS]
            o = acc_at(v, k) + kept(p, j - ONE) - kept(p, 1)
            for i in range(0, n, ch):
                lv, kp = (ONE - b) * n + i, b * n + i
                both = [v.accumulated[pl.ds(o + h, ch)] + v.received[j - ONE][v.r, k, pl.ds(h, ch)].astype(F32) for h in (lv, kp)]
                v.sent[j][v.r, k, pl.ds(i, ch)] = both[0].astype(BF)
                v.accumulated[pl.ds(o + kp, ch)] = both[1]
            return stage_one(v, j, k)

        lag_start([functools.partial(make, k) for k in range(len(v.parts))])

    def is_down(w):
        return (w >= D1) & (w < G0)

    def exchange(v):
        return rcopy(gfin.at[v.f, ONE - c], xg.at[v.id], xs.at[v.f], xr.at[v.id], other)

    def rs5(v):
        seven(v, v.received[4]).wait_recv()
        for k, p in enumerate(v.parts):
            g = v.accumulated[acc_at(v, k) + rot[p] - kept(p, 1)]
            for e in range(OCT - 1):
                g = g + v.received[4][v.r, k, e].astype(F32)
            g = g.astype(BF).astype(F32)
            for h in range(TWO):
                gfin[v.f, h, k] = g[OCT * h : OCT * h + OCT]
        for j in range(1, 4):
            stage_all(v, j).wait_send()
        seven(v, v.sent[4]).wait_send()
        if isinstance(v, Short):
            g_d[v.w, ROWS * UNITS : ROWS * UNITS + OCT] = gfin[v.f, 0, 1]
            exchange(v).start()
            return

        @pl.when(v.w + NRS < NW)
        def _():
            for q in partners:
                signal(rcred.at[v.r], q)

        @pl.when(is_down(v.w))
        def _():
            for p in range(PARTS):
                for h in range(TWO):
                    g_d[jnp.where(v.w < D0, 1, 0), aligned((mod(v.w, 2) * PARTS + p) * ROWS + OCT * h, OCT)] = gfin[v.f, h, p]

        @pl.when(~is_down(v.w))
        def _():
            exchange(v).start()

    def adam_tile(layer, col, v, k):
        cols = aligned(col, LANES)
        mine, theirs = gfin[v.f, c, k], xg[v.id, k]
        for mat, (wr, om, ov) in enumerate(((wr_g, om_g, ov_g), (wr_u, om_u, ov_u))):
            g = jnp.where(c == mat, mine, theirs)
            wn, mn, vn = adam(wr[layer, :, cols].astype(F32), om[layer, :, cols], ov[layer, :, cols], g)
            om[layer, :, cols] = mn
            ov[layer, :, cols] = vn
            wsend[v.f, mat, k] = wn

    def w_exchange(v):
        return rcopy(wsend.at[v.f, ONE - c], wrecv.at[v.id], wsm.at[v.f], wrm.at[v.id], other)

    def rs6(v):
        exchange(v).wait_recv()
        if isinstance(v, Short):
            adam_tile(v.w, 0, v, 0)
            for mat in range(TWO):
                for k in range(1, PARTS):
                    wsend[v.f, mat, k] = jnp.zeros((OCT, LANES), F32)
        else:
            layer = jnp.where(v.w < G0, 1, 0)
            for k in range(PARTS):
                adam_tile(layer, LANES + PARTS * LANES * (v.w - jnp.where(v.w < G0, 0, G0)) + LANES * k, v, k)
        exchange(v).wait_send()
        w_exchange(v).start()

    def rs7(v):
        w_exchange(v).wait_recv()
        for k in range(PARTS if isinstance(v, Full) else 1):
            mine, theirs = wsend[v.f, c, k], wrecv[v.id, k]
            fin[v.id, k] = jnp.concatenate([jnp.where(c == 0, mine, theirs), jnp.where(c == 0, theirs, mine)], 0).astype(BF)
        w_exchange(v).wait_send()

    def window(j):
        return div(OWN_ROWS * j, OCT) * OCT

    def to_group(k, layer, src, dst):
        for r in range(1, GROUP):
            j = mod(j_me + r, GROUP)
            rcopy(src(j), dst.at[layer, j_me], dxs.at[k, layer], dxr.at[k, layer], group_dev(j)).start()

    def from_group(k, layer, dst):
        seven = dst.at[layer, pl.ds(0, GROUP - 1)]
        cp = rcopy(seven, seven, dxs.at[k, layer], dxr.at[k, layer], other)
        cp.wait_recv()
        cp.wait_send()

    def dx1(layer):
        def src(j):
            return g_d.at[layer, aligned(window(j), WIN, OCT)]

        to_group(0, layer, src, gx)

        def row(r, _):
            for o, t in ((om_d, md), (ov_d, vd)):
                o[layer, pl.ds(r, 1)] = t[r, pl.ds(layer, 1)]
            return 0

        loop(OWN_ROWS, row)
        gx[layer, j_me] = g_d[layer, aligned(window(j_me), WIN, OCT)]

    def dx2(layer):
        from_group(0, layer, gx)
        shift = mod(OWN_ROWS * j_me, OCT)
        row = lax.broadcasted_iota(jnp.int32, (WIN, LANES), 0)
        valid = (row >= shift) & (row < shift + OWN_ROWS)
        def tile(lt, _):
            cols = aligned(lt * LANES, LANES)
            m, s = (pltpu.roll(t[layer, :, cols], shift, 0) for t in (om_d, ov_d))
            wn, mn, vn = adam(wr_d[layer, :, cols].astype(F32), m, s, gx[layer, TWO * mod(lt, 4) + div(lt, 4)])
            for o, t in ((om_d, mn), (ov_d, vn)):
                o[layer, :, cols] = pltpu.roll(t, mod(WIN - shift, WIN), 0)
            ws_d[layer, lt] = jnp.where(valid, wn, 0.0)
            return 0

        loop(OCT, tile)

        def src(j):
            return ws_d.at[layer, 4 * mod(j, 2) + div(j, 2)]

        to_group(1, layer, src, wx)
        wx[layer, j_me] = ws_d[layer, 4 * c + pos["z"]]

    def dx3(layer):
        from_group(1, layer, wx)
        octets = [None] * (TWO * UNITS + 2)
        for j in range(GROUP):
            for k in range(WIN // OCT):
                o, t = window(j) // OCT + k, wx[layer, j, OCT * k : OCT * k + OCT]
                octets[o] = t if octets[o] is None else octets[o] + t
        octets[-1] = jnp.zeros((OCT, LANES), F32)
        for u in range(UNITS + 1):
            block = jnp.concatenate(octets[TWO * u : TWO * u + 2], 0).astype(BF)
            if u < UNITS:
                fin[jnp.where(layer == 1, D1, D0) + u // PARTS, u % PARTS] = block
            else:
                fin[NW + layer, 1] = block

    def part_of(v):
        return v.ag_ref.at[v.w, c]

    def ag1(v):
        for k, p in enumerate(v.parts):
            src, dst = fin.at[v.id, k], part_of(v).at[k, rot[p]]
            copy(src, dst, agl.at[v.id]).start()
            for dims in near[p]:
                rcopy(src, dst, ags.at[v.id], agr.at[v.id, 0], across[dims]).start()

    def agk(k, v):
        n = 2 ** (k - 2)
        mine = part_of(v)
        first = k == 4
        if first:
            copy(fin.at[v.id, pl.ds(0, len(v.parts))], mine.at[:, 0], agl.at[v.id]).wait()
        came = mine.at[:, pl.ds(0, OCT - 1 if first else n)]
        rcopy(came, came, ags.at[v.id], agr.at[v.id, 0 if first else k - 4], other).wait_recv()
        j = PARTS + ONE - k
        for q, p in enumerate(v.parts):
            if k <= PARTS:
                h = mine.at[q, pl.ds(kept(p, j), TWO * n)]
                rcopy(h, h, ags.at[v.id], agr.at[v.id, k - 3], partners[(p + j - ONE) % PARTS]).start()
            g = mine.at[q, pl.ds(kept(p, j), OCT) if first else pl.ds(kept(p, j) + (ONE - bits[(p + j) % PARTS]) * n, n)]
            rcopy(g, g, dags.at[v.id], dagr.at[v.id], other).start()

    def ag_end(v):
        most = part_of(v).at[:, pl.ds(0, CHIPS - 1)]
        rcopy(most, most, ags.at[v.id], agr.at[v.id, 0], other).wait_send()
        cp = rcopy(part_of(v), part_of(v), dags.at[v.id], dagr.at[v.id], other)
        cp.wait_send()
        cp.wait_recv()

    rs_stages = [rs0, rs1, functools.partial(rsj, 2), functools.partial(rsj, 3), rs4, rs5, rs6, rs7]
    ag_stages = [ag1] + [functools.partial(agk, k) for k in range(4, PARTS + 2)] + [ag_end]

    def find(t, due):
        terms = [jnp.where(t == s, w + 1, 0) for w, s in due]
        while len(terms) > 1:
            terms = [sum(terms[q : q + 2]) for q in range(0, len(terms), 2)]
        return terms[0]

    def within(t, due, fn):
        at = [s for _, s in due]
        pl.when((t >= min(at)) & (t <= max(at)))(fn)

    def run(t, kind, some):
        found = [(fn, find(t, due)) for fn, due in reversed(some)]

        @pl.when(sum(w for _, w in found) > 0)
        def _():
            for fn, w in found:

                @pl.when(w > 0)
                def _():
                    fn(kind(w - 1))

    def stages(fns, t, full, short):
        full = [[(w, at[s]) for w, at in enumerate(full) if not (fn in (rs6, rs7) and is_down(w))] for s, fn in enumerate(fns)]
        short = [[(w, at[s]) for w, at in enumerate(short)] for s in range(len(fns))]

        def full_ones():
            for odd in range(TWO):

                @pl.when(mod(t, 2) == odd)
                def _():
                    run(t, Full, [(fn, due) for fn, due in zip(fns, full) if due[0][1] % TWO == odd])

        within(t, sum(full, []), full_ones)
        within(t, sum(short, []), lambda: run(t, Short, list(zip(fns, short))))

    def moves(t):
        stages(rs_stages, t, RS_TICKS, SHORT_RS_TICKS)
        for q, fn in enumerate((dx1, dx2, dx3)):

            @pl.when((t == DX[0][q]) | (t == DX[1][q]))
            def _():
                fn(jnp.where(t == DX[1][q], 1, 0))

        stages(ag_stages, t, AG_TICKS, SHORT_AG_TICKS)

    loads = [copy(x, acts.at[2], lsem.at[1]), copy(dy, acts.at[0], lsem.at[2])]
    rows_in = [copy(w.at[:, aligned(dp * OCT, OCT)], o, lsem.at[3 + k]) for k, (w, o) in enumerate(((w_gate, wr_g), (w_up, wr_u)))]
    rows_in.append(copy(w_down.at[:, aligned(div(OWN_ROWS * dp, OCT) * OCT, WIN, OCT)], wr_d, lsem.at[5]))
    moments = ((m_g, om_g), (m_u, om_u), (m_d, md), (v_g, ov_g), (v_u, ov_u), (v_d, vd))
    rows_in += [copy(m, o, lsem.at[6 + k]) for k, (m, o) in enumerate(moments)]
    for cp in [loads[0], *weights(0, 0, 0)]:
        cp.start()
    for q in range(OCT):
        da[pl.ds(q * CHIPS, CHIPS)] = jnp.zeros((CHIPS, ROWS, LANES), F32)
    loads[0].wait()
    for cp in [loads[1], *rows_in]:
        cp.start()
    by_rows(norm_in)
    transpose_in()
    a0t_out.start()
    pl.semaphore_wait(barrier, GROUP - 1 + len(far))

    def tick(t, _):
        pl.when(t < T_TAIL)(lambda: compute(t))
        moves(t)
        return 0

    loop(TICKS, tick)


def step_call(args):
    B = (ROWS, LANES)
    V, R, S = pltpu.VMEM, pltpu.SemaphoreType.REGULAR, pltpu.SemaphoreType.DMA
    sizes = [HALF, HALF // TWO, OCT, OCT]
    n, ns = NW + NS, len(SHORT)
    own_parts = OWN_SLOTS * PARTS + NS * ns
    E = (PARTS, OCT, LANES)
    scratch = [
        V((3, TOK, D), BF), V((D, TOK), BF), V((4 * TB, *B), F32), V((TWO, D, TWO * TILE), BF), V((TWO, TILE, D), BF),
        V((TWO, TOK, TWO * TILE), BF), V((TOK, TILE), BF), V((TWO, TILE, TOK), BF), V((TWO, PAIR, TOK), BF),
        *[V((LAYERS, OCT, FF), BF)] * TWO, V((LAYERS, WIN, D), BF), *[V((OWN_ROWS, LAYERS, D), F32)] * TWO,
        V((TWO, own_parts, CHIPS, *B), BF), V((NDD, PARTS, CHIPS, *B), BF), V((NRS * PARTS * HALF, *B), F32),
        *[V((NRS, PARTS, k, *B), BF) for k in sizes * TWO],
        V((NS, ns, CHIPS, *B), BF), V((NS * ns * HALF, *B), F32),
        *[V((NS, ns, k, *B), BF) for k in sizes * TWO],
        V((NX + NS, TWO, *E), F32), V((n, *E), F32), V((NX + NS, TWO, *E), F32), V((n, *E), F32), V((n, PARTS, *B), BF),
        V((LAYERS, ROWS * (UNITS + 1), LANES), F32), *[V((LAYERS, GROUP, WIN, LANES), F32)] * 3,
        S((12,)), S((TWO, 3)), S((TWO,)), S((TWO,)), S((TWO, 2)), S((TWO,)), S((NDD + NS,)), S((NDD + NS,)), S((NRS + NS, PARTS)), S((NRS + NS, PARTS)),
        S((NX + NS,)), S((n,)), S((NX + NS,)), S((n,)), S((n,)), S((n,)), S((n, PARTS)), S((n,)), S((n,)), S((TWO, LAYERS)), S((TWO, LAYERS)),
        R((NDD,)), R((NRS,)),
    ]
    hbm, vmem = pl.BlockSpec(memory_space=pl.ANY), pl.BlockSpec(memory_space=pltpu.VMEM)
    out = [((NW, TWO, PARTS, CHIPS, *B), BF), ((NS, 2, ns, CHIPS, *B), BF), ((LAYERS, FF, TOK), BF), ((D, TOK), BF), ((TILES, TWO * TB, *B), F32), ((TILES, TOK, TWO * TILE), BF)]
    out += [(s, F32) for s in ((LAYERS, OCT, FF), (LAYERS, OCT, FF), (LAYERS, WIN, D))] * TWO
    return pl.pallas_call(
        step_kernel,
        out_shape=[jax.ShapeDtypeStruct(*o) for o in out],
        in_specs=[hbm] * 11,
        out_specs=[hbm] * 6 + [vmem] * 6,
        scratch_shapes=scratch,
        compiler_params=pltpu.CompilerParams(collective_id=0, has_side_effects=True, vmem_limit_bytes=67043328),
        name="step",
    )(*args)


def place_kernel(
    ag, agm, om_g, om_u, om_d, ov_g, ov_u, ov_d, gate, up, down, pm_g, pm_u, pm_d, pv_g, pv_u, pv_d, buf, dbuf, mbuf, stage, mstage, dstage,
    isem, dsem, msem, osem, mosem, dosem,
):
    copy = pltpu.make_async_copy
    jobs = G0
    outs = (gate, up)

    def load(k):
        return copy(ag.at[jnp.where(k < D1, k, k + D1)], buf.at[mod(k, DEEP)], isem.at[mod(k, DEEP)])

    def stores(k):
        cols = aligned(LANES + PARTS * LANES * mod(k, 4), PARTS * LANES, LANES)
        return [copy(stage.at[mod(k, 2), m], o.at[jnp.where(k < D1, 1, 0), :, cols], osem.at[mod(k, 2), m]) for m, o in enumerate(outs)]

    def load_down(layer):
        return copy(ag.at[pl.ds(pick(layer, (D0, D1)), 2)], dbuf.at[layer], dsem.at[layer])

    def store_down(k):
        rows = aligned(mod(k, 4) * TWO * PAIR, TWO * PAIR, ROWS)
        return copy(dstage.at[mod(k, 2)], down.at[jnp.where(k < D1, 1, 0), rows], dosem.at[mod(k, 2)])

    def store_short(layer, m):
        return copy(mstage.at[layer, m], outs[m].at[layer, :, lanes(0)], mosem.at[layer, m])

    mini = copy(agm, mbuf, msem.at[0])
    for cp in (load(0), load(1), load_down(1), mini, load(2), load_down(0)):
        cp.start()

    def by_chip(dst, cols, src, p):
        for u in range(CHIPS):
            n = CHIP_AT[u]
            dst[ROWS * n : ROWS * n + ROWS, cols] = src[rotl(u, p)]

    def body(k, _):
        @pl.when(k < jobs)
        def _():
            load(k).wait()

            @pl.when(k >= 2)
            def _():
                for cp in stores(k - 2):
                    cp.wait()

            for m in range(TWO):
                for p in range(PARTS):
                    by_chip(stage.at[mod(k, 2), m], lanes(p), buf.at[mod(k, DEEP), m, p], p)
            for cp in stores(k):
                cp.start()

            @pl.when(k + DEEP < jobs)
            def _():
                load(k + DEEP).start()

        @pl.when(k >= 1)
        def _():
            down_job(k - ONE)

        return 0

    def down_job(k):
        layer = jnp.where(k < D1, 1, 0)

        @pl.when(k == 0)
        def _():
            mini.wait()
            for layer in range(LAYERS):
                for m in range(TWO):
                    by_chip(mstage.at[layer, m], lanes(0), mbuf.at[layer, m, 0], SHORT[0])
                    store_short(layer, m).start()

        @pl.when(mod(k, 4) == 0)
        def _():
            load_down(layer).wait()

        @pl.when(k >= 2)
        def _():
            store_down(k - 2).wait()

        def pair(q, _):
            for lt in range(OCT):
                h = lt // 4
                octets = []
                for gg in range(TWO):
                    g = (mod(k, 4) * TWO + q) * TWO + gg
                    spot = base_of(div(g, 4), mod(g, 4), 0) + base_of(0, 0, lt % 4)
                    for u in range(UNITS + 1):
                        if u < UNITS:
                            t = dbuf[layer, u // PARTS, h, u % PARTS, rotl(spot, u % PARTS)].astype(F32)
                        else:
                            t = mbuf[layer, h, 1, rotl(spot, SHORT[1])].astype(F32)[:OCT]
                        octets.append(t)
                dstage[mod(k, 2), aligned(PAIR * q, PAIR, ROWS), lanes(lt)] = jnp.concatenate(octets, 0).astype(BF)
            return 0

        loop(2, pair)
        store_down(k).start()

        @pl.when(k == jobs - 1)
        def _():
            for o, t in ((pm_g, om_g), (pm_u, om_u), (pv_g, ov_g), (pv_u, ov_u)):
                o[...] = t[...]
            for o, t in ((pm_d, om_d), (pv_d, ov_d)):
                for layer in range(LAYERS):
                    for r in range(OWN_ROWS):
                        o[r, layer : layer + 1] = t[layer, r : r + 1]

    loop(jobs + 1, body)
    for k in (jobs - 2, jobs - 1):
        for cp in stores(k) + [store_down(k)]:
            cp.wait()
    for layer in range(LAYERS):
        for m in range(TWO):
            store_short(layer, m).wait()


def place_call(args):
    hbm, vmem = pl.BlockSpec(memory_space=pl.ANY), pl.BlockSpec(memory_space=pltpu.VMEM)
    V, S = pltpu.VMEM, pltpu.SemaphoreType.DMA
    whole = (TWO, PARTS, CHIPS, ROWS, LANES)
    out = [(s, BF) for s in ((LAYERS, D, FF), (LAYERS, D, FF), (LAYERS, FF, D))]
    out += [(s, F32) for s in ((LAYERS, OCT, FF), (LAYERS, OCT, FF), (OWN_ROWS, LAYERS, D))] * TWO
    return pl.pallas_call(
        place_kernel,
        out_shape=[jax.ShapeDtypeStruct(*o) for o in out],
        in_specs=[hbm] * TWO + [vmem] * 6,
        out_specs=[hbm] * 3 + [vmem] * 6,
        scratch_shapes=[
            V((DEEP, *whole), BF), V((LAYERS, TWO, *whole), BF), V((NS, 2, len(SHORT), CHIPS, ROWS, LANES), BF),
            V((TWO, TWO, D, PARTS * LANES), BF), V((LAYERS, TWO, D, LANES), BF), V((TWO, TWO * PAIR, D), BF),
            S((DEEP,)), S((TWO,)), S((1,)), S((TWO, 2)), S((TWO, 2)), S((TWO,)),
        ],
        compiler_params=pltpu.CompilerParams(vmem_limit_bytes=60 * TWO**20),
        name="place",
    )(*args)


def local_step(x, dy, w_gate, w_up, w_down, m_g, m_u, m_d, v_g, v_u, v_d):
    m_d, v_d = (jnp.transpose(t, (1, 0, 2)) for t in (m_d, v_d))
    ag, agm, _, _, _, _, *moments = step_call((x[0], dy[0], w_gate, w_up, w_down, m_g, m_u, m_d, v_g, v_u, v_d))
    gate, up, down, om_g, om_u, om_d, ov_g, ov_u, ov_d = place_call((ag, agm, *moments))
    om_d, ov_d = (jnp.transpose(t, (1, 0, 2)) for t in (om_d, ov_d))
    return gate, up, down, om_g, om_u, om_d, ov_g, ov_u, ov_d


def solution(mesh):
    moment = P(None, "dp", None)
    return jax.shard_map(
        local_step,
        mesh=mesh,
        in_specs=(P(("rep", "dp")), P(("rep", "dp")), P(), P(), P(), *[moment] * 6),
        out_specs=(P("rep"), P("rep"), P("rep"), *[P("rep", "dp", None)] * 6),
        check_vma=False,
    )
```
